128 devices in a mesh: az: 8 (over y, core), rg: 16 (over z, x).
Axes of the slice: x: 4, y: 4, z: 4, core: 2. Of those that a mesh axis runs over, the one named last changes fastest.
Arguments:
- master_raw: float32 [2, 2048, 20000], P(None, 'az', 'rg'), may hold values from -6 to 6
- slave_raw: float32 [2, 2048, 20000], P(None, 'az', 'rg'), may hold values from -6 to 6
- range_ref: float32 [2, 20000], replicated, may hold values from -4 to 4
- az_ref: float32 [2, 2048], replicated, may hold values from -4 to 4
- az_shift: int32 [4, 256], P(None, ('az', 'rg')), may hold values from -32 to 32, as said below
- rg_shift: int32 [4, 256], P(None, ('az', 'rg')), may hold values from -64 to 64, as said below
- valid_lines: int32 [256], replicated, may hold values from 1024 to 2048, as said below
Outputs:
- interferogram: float32 [2, 256, 2048], P(None, None, ('az', 'rg'))
The draws below stay inside these ranges and needn't reach their ends.
Inputs may be any that keep to these rules, and one draw needn't show every extreme that they name: `az_shift`: azimuth offset of the slave in lines for each block of 512 lines and 64 samples. `rg_shift`: range offset of the slave in samples for each block of 512 lines and 64 samples. Lines 0 to valid_lines[t] - 1 of range tile t are valid.
All inputs are finite; a program needn't handle non-finite values.
Results may differ from the reference program's by a relative error of at most 0.0003.
Values sent between devices are 32-bit elements; how exact they have to be, the bound alone decides.
No kernel may reach another device: no remote copies, remote signals or barrier semaphores. Data moves between devices by JAX's collectives and lax.ppermute only.
A program may use at most 256 MiB of HBM per device.

```python
import jax
import jax.numpy as jnp
from jax import lax

LINES = 2048
RANGE = 20000
RV = 16384
LOOK = 8
BA = 512
BR = 64
ASH = 32
RSH = 64
NBA = 4
NBR = 256


def forced_table(key, count, lowest, highest):
    key_values, key_first, key_second = jax.random.split(key, 3)
    values = jax.random.randint(key_values, (count,), lowest, highest + 1)
    index_first = jax.random.randint(key_first, (), 0, count)
    index_second = (index_first + 1 + jax.random.randint(key_second, (), 0, count - 1)) % count
    return values.at[index_first].set(highest).at[index_second].set(lowest).astype(jnp.int32)


def draw_az_shift(key, part):
    return forced_table(jax.random.fold_in(key, 101), NBA * NBR, -ASH, ASH).reshape(NBA, NBR)


def draw_rg_shift(key, part):
    return forced_table(jax.random.fold_in(key, 202), NBA * NBR, -RSH, RSH).reshape(NBA, NBR)


def draw_valid_lines(key, part):
    return forced_table(jax.random.fold_in(key, 303), NBR, LINES // 2, LINES)


def level_of(rng, dims, cuts, smallest, high):
    gain = 1.0
    for axis_at, shards_of in cuts:
        draws = jax.random.uniform(jax.random.fold_in(jax.random.fold_in(rng, 6), axis_at), (shards_of,), jnp.float32, smallest / len(cuts), high / len(cuts))
        gain = gain * jnp.repeat(jnp.exp(draws), dims[axis_at] // shards_of).reshape((-1,) + (1,) * (len(dims) - 1 - axis_at))
    return gain


def bell_draw(own_key, extent, width, limit, cuts=(), kind=jnp.bfloat16):
    loudness = level_of(own_key, extent, cuts, -0.22, 0.18) if cuts else 1.0
    values = jax.random.normal(own_key, extent, jnp.float32) * width * loudness
    return jnp.minimum(jnp.maximum(values, -limit), limit).astype(kind)


def setup_inputs(seed: int = 0) -> dict:
    streams_of = jax.random.split(jax.random.key(seed), 8)
    master_raw = bell_draw(streams_of[0], (2, LINES, RANGE), 1.0, 6.0, ((1, 8), (2, 16)), jnp.float32)
    slave_raw = bell_draw(streams_of[1], (2, LINES, RANGE), 1.0, 6.0, ((1, 8), (2, 16)), jnp.float32)
    range_ref = bell_draw(streams_of[2], (2, RANGE), 0.6, 4.0, (), jnp.float32)
    az_ref = bell_draw(streams_of[3], (2, LINES), 0.6, 4.0, (), jnp.float32)
    az_shift = draw_az_shift(jax.random.fold_in(streams_of[7], 71), 0)
    rg_shift = draw_rg_shift(jax.random.fold_in(streams_of[7], 71), 0)
    valid_lines = draw_valid_lines(jax.random.fold_in(streams_of[7], 71), 0)
    return dict(master_raw=master_raw, slave_raw=slave_raw, range_ref=range_ref, az_ref=az_ref, az_shift=az_shift, rg_shift=rg_shift, valid_lines=valid_lines)


def focus_image(raw_data, range_ref, az_ref):
    range_filter = range_ref[0] + 1j * range_ref[1]

    def range_block(block_index):
        line_start = (block_index * BA).astype(jnp.int32)
        block_data = lax.dynamic_slice_in_dim(raw_data, line_start, BA, 1)
        signal = block_data[0] + 1j * block_data[1]
        spectrum = jnp.fft.fft(signal, axis=1) * range_filter[None, :]
        return jnp.fft.ifft(spectrum, axis=1)[:, :RV]
    ranged = lax.map(range_block, jnp.arange(LINES // BA, dtype=jnp.int32)).reshape(LINES, RV)
    spectrum = jnp.fft.fft(ranged, axis=0) * (az_ref[0] + 1j * az_ref[1])[:, None]
    focused = jnp.fft.ifft(spectrum, axis=0)
    return (jnp.real(focused), jnp.imag(focused))

def resample(slave_field, az_shift, rg_shift):
    padded = jnp.pad(slave_field, ((0, 0), (ASH, ASH), (RSH, RSH)))
    row_start = (lax.broadcasted_iota(jnp.int32, (NBA, NBR), 0) * BA + ASH + az_shift).astype(jnp.int32)
    col_start = (lax.broadcasted_iota(jnp.int32, (NBA, NBR), 1) * BR + RSH + rg_shift).astype(jnp.int32)

    def cutout(row_begin, col_begin):
        return lax.dynamic_slice(padded, (jnp.int32(0), row_begin, col_begin), (2, BA, BR))
    pieces = jax.vmap(jax.vmap(cutout))(row_start, col_start)
    return pieces.transpose(2, 0, 3, 1, 4).reshape(2, LINES, RV)

def box_filter(padded_grid, rows_out, cols_out):
    total = padded_grid[..., 0:rows_out, 0:cols_out]
    for row_step in range(3):
        for col_step in range(3):
            if row_step + col_step > 0:
                total = total + padded_grid[..., row_step:row_step + rows_out, col_step:col_step + cols_out]
    return total

def reference(master_raw, slave_raw, range_ref, az_ref, az_shift, rg_shift, valid_lines):
    master_real, master_imag = focus_image(master_raw, range_ref, az_ref)
    slave_real, slave_imag = focus_image(slave_raw, range_ref, az_ref)
    moved = resample(jnp.stack([slave_real, slave_imag]), az_shift, rg_shift)
    col_counts = jnp.repeat(valid_lines, BR)
    valid_mask = (lax.broadcasted_iota(jnp.int32, (LINES, RV), 0) < col_counts[None, :]).astype(master_real.dtype)
    cross_real = (master_real * moved[0] + master_imag * moved[1]) * valid_mask
    cross_imag = (master_imag * moved[0] - master_real * moved[1]) * valid_mask
    rows_out = LINES // LOOK
    cols_out = RV // LOOK
    looks = jnp.stack([cross_real, cross_imag]).reshape(2, rows_out, LOOK, cols_out, LOOK).sum(axis=(2, 4))
    groups = lax.broadcasted_iota(jnp.int32, (rows_out, cols_out), 0)
    look_counts = jnp.repeat(valid_lines, BR // LOOK)
    pixels = (jnp.clip(look_counts[None, :] - LOOK * groups, 0, LOOK) * LOOK).astype(master_real.dtype)
    box = box_filter(jnp.pad(looks, ((0, 0), (1, 1), (1, 1))), rows_out, cols_out)
    box_pixels = box_filter(jnp.pad(pixels, ((1, 1), (1, 1))), rows_out, cols_out)
    return box / jnp.sqrt(jnp.maximum(box_pixels, 1.0))[None]
```

```python
import math

import jax
import jax.numpy as jnp
import numpy as np
from jax import lax
from jax.experimental import pallas as pl
from jax.experimental.pallas import tpu as pltpu
from jax.sharding import PartitionSpec as P

LINES = 2048
RANGE = 20000
RV = 16384
LOOK = 8
BA = 512
BR = 64
ASH = 32
RSH = 64
NBA = 4
ALL = ("az", "rg")
NP = 16
NQ = 10
NS = 125
RPAD = 1280
F32 = jnp.float32
BF16 = jnp.bfloat16


def _rot(v, angle):
    c, s = math.cos(angle), math.sin(angle)
    turns = angle / (math.pi / 4)
    eighth = round(turns)
    x, y = v
    if abs(turns - eighth) < 1e-9:
        e = eighth % 8
        if e == 0:
            return v
        if e == 2:
            return (-y, x)
        if e == 4:
            return (-x, -y)
        if e == 6:
            return (y, -x)
        h = math.sqrt(0.5)
        if e == 1:
            return ((x - y) * h, (x + y) * h)
        if e == 3:
            return (-(x + y) * h, (x - y) * h)
        if e == 5:
            return ((y - x) * h, -(x + y) * h)
        return ((x + y) * h, (y - x) * h)
    return (x * c - y * s, x * s + y * c)


def _add(a, b):
    return (a[0] + b[0], a[1] + b[1])


def _sub(a, b):
    return (a[0] - b[0], a[1] - b[1])


def _dft2(v, sign):
    return [_add(v[0], v[1]), _sub(v[0], v[1])]


def _dft4(v, sign):
    a, b = _add(v[0], v[2]), _sub(v[0], v[2])
    c, d = _add(v[1], v[3]), _sub(v[1], v[3])
    if sign < 0:
        return [_add(a, c), (b[0] + d[1], b[1] - d[0]), _sub(a, c), (b[0] - d[1], b[1] + d[0])]
    return [_add(a, c), (b[0] - d[1], b[1] + d[0]), _sub(a, c), (b[0] + d[1], b[1] - d[0])]


def _dft5(v, sign):
    c1, c2 = math.cos(2 * math.pi / 5), math.cos(4 * math.pi / 5)
    s1, s2 = sign * math.sin(2 * math.pi / 5), sign * math.sin(4 * math.pi / 5)
    a1, b1 = _add(v[1], v[4]), _sub(v[1], v[4])
    a2, b2 = _add(v[2], v[3]), _sub(v[2], v[3])
    x0 = v[0]
    y0 = (x0[0] + a1[0] + a2[0], x0[1] + a1[1] + a2[1])
    p1 = tuple(x0[i] + c1 * a1[i] + c2 * a2[i] for i in range(2))
    p2 = tuple(x0[i] + c2 * a1[i] + c1 * a2[i] for i in range(2))
    q1 = tuple(s1 * b1[i] + s2 * b2[i] for i in range(2))
    q2 = tuple(s2 * b1[i] - s1 * b2[i] for i in range(2))
    return [
        y0,
        (p1[0] - q1[1], p1[1] + q1[0]),
        (p2[0] - q2[1], p2[1] + q2[0]),
        (p2[0] + q2[1], p2[1] - q2[0]),
        (p1[0] + q1[1], p1[1] - q1[0]),
    ]


def _dft_two(v, n1, n2, first, second, sign):
    n = n1 * n2
    out = [None] * n
    mid = []
    for b in range(n2):
        col = first([v[n2 * a + b] for a in range(n1)], sign)
        mid.append([_rot(col[k], sign * 2 * math.pi * ((b * k) % n) / n) for k in range(n1)])
    for k1 in range(n1):
        row = second([mid[b][k1] for b in range(n2)], sign)
        for k2 in range(n2):
            out[k1 + n1 * k2] = row[k2]
    return out


def dft16(v, sign):
    return _dft_two(v, 4, 4, _dft4, _dft4, sign)


def dft10(v, sign):
    return _dft_two(v, 2, 5, _dft2, _dft5, sign)


def cmul(a, b):
    return (a[0] * b[0] - a[1] * b[1], a[0] * b[1] + a[1] * b[0])


def split(x):
    hi = x.astype(BF16)
    return hi, (x - hi.astype(F32)).astype(BF16)


def dot(a, b):
    return jnp.dot(a, b, preferred_element_type=F32)


def _np_split(x):
    x = np.asarray(x, np.float32)
    hi = x.astype(BF16)
    return hi, (x - hi.astype(np.float32)).astype(BF16)


def _tables():
    t = {}
    two = 2 * np.pi
    q = np.arange(RPAD)
    ang = -two * ((np.arange(NP)[:, None] * q[None, :]) % RANGE) / RANGE
    t["twa"] = np.stack([np.cos(ang), np.sin(ang)], 1).astype(np.float32)
    q2 = np.arange(128)
    keep = (q2 < NS)[None, :]
    ang = -two * ((np.arange(NQ)[:, None] * q2[None, :]) % 1250) / 1250
    t["twb"] = np.stack([np.cos(ang) * keep, np.sin(ang) * keep], 1).astype(np.float32)
    n = np.arange(NQ)[None, :, None] * NS + q2[None, None, :]
    ang = two * ((np.arange(NP)[:, None, None] * n) % RANGE) / RANGE
    t["twc"] = (
        (np.stack([np.cos(ang), np.sin(ang)], 2) / RANGE)
        .reshape(NP * NQ, 2, 128)
        .astype(np.float32)
    )
    ang = two * ((q2[:, None] * q2[None, :]) % NS) / NS
    both = keep & keep.T
    c, s = np.cos(ang) * both, np.sin(ang) * both
    t["fh"], t["fl"] = _np_split(np.block([[c, -s], [s, c]]))
    t["gh"], t["gl"] = _np_split(np.block([[c, s], [-s, c]]))
    k2 = np.arange(128)
    l2 = np.arange(128)
    ang = -two * ((l2[:, None] * k2[None, :]) % 128) / 128
    pr, pi = np.cos(ang), np.sin(ang)
    ang = np.broadcast_to(-two * l2[:, None] / LINES, (128, 128))
    wr, wi = np.cos(ang), np.sin(ang)
    t["p"] = np.stack([pr, pi]).astype(np.float32)
    t["w"] = np.stack([wr, wi]).astype(np.float32)
    kk = np.arange(256)
    part, line = (kk // 16) % 2, (kk // 32) * 16 + kk % 16
    sel = (part == 0)[:, None]
    t["q"] = np.stack(
        [np.where(sel, pr[line], -pi[line]), np.where(sel, -pi[line], -pr[line])]
    ).astype(np.float32)
    t["v"] = np.stack([wr[line], wi[line]]).astype(np.float32)
    lane = np.arange(128)
    band = np.zeros((128, 128), np.float32)
    for o in range(16):
        band[:, o] = np.abs(lane // LOOK - o) <= 1
    t["band"] = band
    edge = np.zeros((4, 8, 128), np.float32)
    for part in range(2):
        edge[part, part] = lane < LOOK
        edge[2 + part, part] = lane >= 128 - LOOK
    t["edge"] = edge
    return t


TABLES = _tables()


def _pre_kernel(x_ref, o_ref):
    for part in range(2):
        o_ref[0, part, :, 0:1152] = x_ref[part, :, 0:1152]
        tail = x_ref[part, :, 1152:1250]
        o_ref[0, part, :, 1152:1280] = jnp.concatenate([tail, jnp.zeros((16, 30), F32)], axis=1)


def pre(raw):
    return pl.pallas_call(
        _pre_kernel,
        grid=(NP,),
        in_specs=[pl.BlockSpec((2, 16, 1250), lambda i: (0, i, 0))],
        out_specs=pl.BlockSpec((1, 2, 16, RPAD), lambda i: (i, 0, 0, 0)),
        out_shape=jax.ShapeDtypeStruct((NP, 2, 16, RPAD), F32),
        cost_estimate=pl.CostEstimate(flops=10**8, bytes_accessed=5 * 10**6, transcendentals=0),
        name="pre",
    )(raw)


def _range_kernel(x_ref, twa_ref, twb_ref, hf_ref, fh_ref, fl_ref, gh_ref, gl_ref, twc_ref, o_ref, b_ref, d_ref):
    lane = lax.broadcasted_iota(jnp.int32, (16, 128), 1)

    def outer(j, carry):
        lanes = pl.ds(pl.multiple_of(j * 128, 128), 128)
        for g in range(2):
            rows = slice(8 * g, 8 * g + 8)
            v = [(x_ref[p, 0, rows, lanes], x_ref[p, 1, rows, lanes]) for p in range(NP)]
            v = dft16(v, -1)
            for k in range(NP):
                tw = (twa_ref[k, 0:1, lanes], twa_ref[k, 1:2, lanes])
                r, i = cmul(v[k], tw)
                b_ref[k, 0, rows, lanes] = r
                b_ref[k, 1, rows, lanes] = i
        return carry

    lax.fori_loop(0, RPAD // 128, outer, 0)

    def middle(kp, carry):
        chunks = []
        for q in range(NQ):
            pair = []
            for c in range(2):
                here = b_ref[kp, c, :, 128 * q : 128 * q + 128]
                if q:
                    prev = b_ref[kp, c, :, 128 * q - 128 : 128 * q]
                    here = jnp.where(
                        lane < 3 * q, pltpu.roll(prev, 3 * q, 1), pltpu.roll(here, 3 * q, 1)
                    )
                pair.append(here)
            chunks.append(tuple(pair))
        v = dft10(chunks, -1)
        rows = []
        for k in range(NQ):
            r, i = cmul(v[k], (twb_ref[k, 0:1, :], twb_ref[k, 1:2, :]))
            rows.append(jnp.concatenate([r, i], axis=1))
        hi, lo = split(jnp.concatenate(rows, axis=0))
        y = dot(hi, fh_ref[...]) + dot(lo, fh_ref[...]) + dot(hi, fl_ref[...])
        rows = []
        for k in range(NQ):
            val = (y[16 * k : 16 * k + 16, :128], y[16 * k : 16 * k + 16, 128:])
            r, i = cmul(val, (hf_ref[kp * NQ + k, 0:1, :], hf_ref[kp * NQ + k, 1:2, :]))
            rows.append(jnp.concatenate([r, i], axis=1))
        hi, lo = split(jnp.concatenate(rows, axis=0))
        y = dot(hi, gh_ref[...]) + dot(lo, gh_ref[...]) + dot(hi, gl_ref[...])
        v = []
        for k in range(NQ):
            val = (y[16 * k : 16 * k + 16, :128], y[16 * k : 16 * k + 16, 128:])
            v.append(cmul(val, (twb_ref[k, 0:1, :], -twb_ref[k, 1:2, :])))
        v = dft10(v, 1)
        for q in range(NQ):
            tw = (twc_ref[kp * NQ + q, 0:1, :], twc_ref[kp * NQ + q, 1:2, :])
            r, i = cmul(v[q], tw)
            d_ref[kp * NQ + q, 0] = r
            d_ref[kp * NQ + q, 1] = i
        return carry

    lax.fori_loop(0, NP, middle, 0)

    def inner(q, carry):
        for g in range(2):
            rows = slice(8 * g, 8 * g + 8)
            v = [(d_ref[k * NQ + q, 0, rows, :], d_ref[k * NQ + q, 1, rows, :]) for k in range(NP)]
            v = dft16(v, 1)
            for p in range(14):
                d_ref[p * NQ + q, 0, rows, :] = v[p][0]
                d_ref[p * NQ + q, 1, rows, :] = v[p][1]
        return carry

    lax.fori_loop(0, NQ, inner, 0)

    for d in range(128):
        n, a = divmod(128 * d, NS)
        for c in range(2):
            val = d_ref[n, c]
            if a:
                val = pltpu.roll(val, 128 - a, 1)
            start = NS - a
            while start < 128:
                n2 = (128 * d + start) // NS
                nxt = d_ref[n2, c]
                nxt = pltpu.roll(nxt, start % 128, 1)
                val = jnp.where(lane < start, val, nxt)
                start += NS
            o_ref[d, c] = val


def range_compress(x, hf):
    t = TABLES
    return pl.pallas_call(
        _range_kernel,
        out_shape=jax.ShapeDtypeStruct((128, 2, 16, 128), F32),
        scratch_shapes=[
            pltpu.VMEM((NP, 2, 16, RPAD), F32),
            pltpu.VMEM((NP * NQ, 2, 16, 128), F32),
        ],
        cost_estimate=pl.CostEstimate(flops=10**10, bytes_accessed=6 * 10**6, transcendentals=0),
        name="range",
    )(x, t["twa"], t["twb"], hf, t["fh"], t["fl"], t["gh"], t["gl"], t["twc"])


def _dot_t(a, b):
    return lax.dot_general(
        a, b, (((1,), (1,)), ((), ())), precision=lax.Precision.HIGHEST, preferred_element_type=F32
    )


def _prep_kernel(h_ref, p0_ref, w_ref, q0_ref, v_ref, ah_ref, al_ref, p_ref, q_ref):
    p_ref[...] = p0_ref[...]
    q_ref[...] = q0_ref[...]

    def body(k, carry):
        pr, pi = p_ref[0], p_ref[1]
        q1, q2 = q_ref[0], q_ref[1]
        hr, hi = h_ref[k, 0:1, :], h_ref[k, 1:2, :]
        vr, vi = cmul((pr, -pi), (hr, hi))
        top = _dot_t(vr, q1) + _dot_t(vi, q2)
        bottom = _dot_t(vi, q1) - _dot_t(vr, q2)
        high, low = split(top)
        ah_ref[k, 0:128, :] = high
        al_ref[k, 0:128, :] = low
        high, low = split(bottom)
        ah_ref[k, 128:256, :] = high
        al_ref[k, 128:256, :] = low
        pr, pi = cmul((pr, pi), (w_ref[0], w_ref[1]))
        p_ref[0] = pr
        p_ref[1] = pi
        wr, wi = v_ref[0], v_ref[1]
        q_ref[0] = q1 * wr + q2 * wi
        q_ref[1] = q2 * wr - q1 * wi
        return carry

    lax.fori_loop(0, 16, body, 0)


def prep(h):
    t = TABLES
    shape = jax.ShapeDtypeStruct((16, 256, 256), BF16)
    return pl.pallas_call(
        _prep_kernel,
        out_shape=(shape, shape),
        scratch_shapes=[pltpu.VMEM((2, 128, 128), F32), pltpu.VMEM((2, 256, 128), F32)],
        cost_estimate=pl.CostEstimate(flops=5 * 10**9, bytes_accessed=5 * 10**6, transcendentals=0),
        name="prep",
    )(h, t["p"], t["w"], t["q"], t["v"])


def _azimuth_front(x_ref, ah_ref, al_ref, e_ref):
    def first(s, carry):
        for g in range(2):
            rows = slice(8 * g, 8 * g + 8)
            v = [(x_ref[8 * a + s, 0, rows, :], x_ref[8 * a + s, 1, rows, :]) for a in range(16)]
            v = dft16(v, -1)
            for k in range(16):
                for c in range(2):
                    at = pl.multiple_of(s * 32 + c * 16 + g * 8, 8)
                    e_ref[k, pl.ds(at, 8), :] = v[k][c]
        return carry

    lax.fori_loop(0, 8, first, 0)

    def second(k, carry):
        hi, lo = split(e_ref[k])
        wide = dot(ah_ref[k], jnp.concatenate([hi, lo], axis=1))
        e_ref[k] = wide[:, :128] + wide[:, 128:] + dot(al_ref[k], hi)
        return carry

    lax.fori_loop(0, 16, second, 0)


def _azimuth_rows(e_ref, g):
    at = [pl.multiple_of(c * 128 + g * 8, 8) for c in range(2)]
    v = [(e_ref[k, pl.ds(at[0], 8), :], e_ref[k, pl.ds(at[1], 8), :]) for k in range(16)]
    return dft16(v, 1)


def _slave_kernel(x_ref, ah_ref, al_ref, o_ref, left_ref, right_ref, e_ref):
    _azimuth_front(x_ref, ah_ref, al_ref, e_ref)
    low = lax.broadcasted_iota(jnp.int32, (8, 128), 1) < 64

    def third(g, carry):
        v = _azimuth_rows(e_ref, g)
        for a in range(16):
            rows = pl.ds(pl.multiple_of(a * 128 + g * 8, 8), 8)
            r, i = v[a]
            o_ref[0, rows, :] = r
            o_ref[1, rows, :] = i
            left_ref[rows, :] = jnp.where(low, r, pltpu.roll(i, 64, 1))
            right_ref[rows, :] = jnp.where(low, pltpu.roll(r, 64, 1), i)
        return carry

    lax.fori_loop(0, 16, third, 0)


def slave_azimuth(x, ah, al):
    side = jax.ShapeDtypeStruct((LINES, 128), F32)
    return pl.pallas_call(
        _slave_kernel,
        out_shape=(jax.ShapeDtypeStruct((2, LINES, 128), F32), side, side),
        scratch_shapes=[pltpu.VMEM((16, 256, 128), F32)],
        cost_estimate=pl.CostEstimate(flops=5 * 10**9, bytes_accessed=10**7, transcendentals=0),
        name="slave_azimuth",
    )(x, ah, al)


def _resample_kernel(az_ref, rg_ref, s_ref, left_ref, right_ref, o_ref, w_ref):
    lane = lax.broadcasted_iota(jnp.int32, (64, 128), 1)
    low = lane < 64
    for i in range(4):
        w_ref[i, 0:ASH, :] = jnp.zeros((ASH, 128), F32)
        w_ref[i, ASH + LINES : 2 * ASH + LINES, :] = jnp.zeros((ASH, 128), F32)

    def fill(t, carry):
        rows = pl.ds(pl.multiple_of(t * 64, 64), 64)
        at = pl.ds(pl.multiple_of(t * 64 + ASH, 32), 64)
        sr = pltpu.roll(s_ref[0, rows, :], 64, 1)
        si = pltpu.roll(s_ref[1, rows, :], 64, 1)
        left, right = left_ref[rows, :], right_ref[rows, :]
        w_ref[0, at, :] = jnp.where(low, left, sr)
        w_ref[1, at, :] = jnp.where(low, pltpu.roll(left, 64, 1), si)
        w_ref[2, at, :] = jnp.where(low, sr, pltpu.roll(right, 64, 1))
        w_ref[3, at, :] = jnp.where(low, si, right)
        return carry

    lax.fori_loop(0, LINES // 64, fill, 0)

    def move(t, carry):
        block = t // 8
        parts = []
        for r in range(2):
            start = t * 64 + ASH + az_ref[block, r]
            shift = RSH + rg_ref[block, r]
            back = lax.rem(256 - shift, 128)
            rows = pl.ds(start, 64)
            near = lane + shift < 128
            parts.append(
                [
                    jnp.where(
                        near,
                        pltpu.roll(w_ref[c, rows, :], back, 1),
                        pltpu.roll(w_ref[2 + c, rows, :], back, 1),
                    )
                    for c in range(2)
                ]
            )
        rows = pl.ds(pl.multiple_of(t * 64, 64), 64)
        for c in range(2):
            o_ref[c, rows, :] = jnp.where(low, parts[0][c], parts[1][c])
        return carry

    lax.fori_loop(0, LINES // 64, move, 0)


def resample(az_shift, rg_shift, focused, left, right):
    return pl.pallas_call(
        _resample_kernel,
        in_specs=[pl.BlockSpec(memory_space=pltpu.SMEM)] * 2
        + [pl.BlockSpec(memory_space=pltpu.VMEM)] * 3,
        out_shape=jax.ShapeDtypeStruct((2, LINES, 128), F32),
        scratch_shapes=[pltpu.VMEM((4, LINES + 2 * ASH, 128), F32)],
        cost_estimate=pl.CostEstimate(flops=2 * 10**9, bytes_accessed=10**7, transcendentals=0),
        name="resample",
    )(az_shift, rg_shift, focused, left, right)


def _master_kernel(x_ref, ah_ref, al_ref, m_ref, n_ref, band_ref, edge_ref, box_ref, left_ref, right_ref, e_ref, c_ref):
    _azimuth_front(x_ref, ah_ref, al_ref, e_ref)
    line = lax.broadcasted_iota(jnp.int32, (8, 128), 0)
    count = n_ref[...]

    def third(g, carry):
        v = _azimuth_rows(e_ref, g)
        for a in range(16):
            at = pl.multiple_of(a * 128 + g * 8, 8)
            r, i = v[a]
            sr, si = m_ref[0, pl.ds(at, 8), :], m_ref[1, pl.ds(at, 8), :]
            keep = line + at < count
            c_ref[pl.ds(at, 8), :] = jnp.where(keep, r * sr + i * si, 0.0)
            c_ref[pl.ds(at + LINES, 8), :] = jnp.where(keep, i * sr - r * si, 0.0)
        return carry

    lax.fori_loop(0, 16, third, 0)
    total = c_ref[pl.ds(0, 512, stride=LOOK), :]
    for j in range(1, LOOK):
        total = total + c_ref[pl.ds(j, 512, stride=LOOK), :]
    parts = (total[:256], total[256:])
    for c in range(2):
        box_ref[c] = jnp.dot(
            parts[c], band_ref[...], precision=lax.Precision.HIGHEST, preferred_element_type=F32
        )
    left_ref[...] = _dot_t(edge_ref[0], parts[0]) + _dot_t(edge_ref[1], parts[1])
    right_ref[...] = _dot_t(edge_ref[2], parts[0]) + _dot_t(edge_ref[3], parts[1])


def master_looks(x, ah, al, moved, counts):
    t = TABLES
    side = jax.ShapeDtypeStruct((8, 256), F32)
    return pl.pallas_call(
        _master_kernel,
        out_shape=(jax.ShapeDtypeStruct((2, 256, 128), F32), side, side),
        scratch_shapes=[pltpu.VMEM((16, 256, 128), F32), pltpu.VMEM((2 * LINES, 128), F32)],
        cost_estimate=pl.CostEstimate(flops=5 * 10**9, bytes_accessed=10**7, transcendentals=0),
        name="master_looks",
    )(x, ah, al, moved, counts, t["band"], t["edge"])


def _final_kernel(box_ref, left_ref, right_ref, scale_ref, o_ref):
    row = lax.broadcasted_iota(jnp.int32, (256, 128), 0)
    sub = lax.broadcasted_iota(jnp.int32, (8, 128), 0)
    lane = lax.broadcasted_iota(jnp.int32, (8, 128), 1)
    for c in range(2):
        put = [
            jnp.where((sub == c) & (lane == at), 1.0, 0.0).astype(F32) for at in (0, 15)
        ]
        x = box_ref[c]
        for ref, onto in ((left_ref, put[0]), (right_ref, put[1])):
            x = x + lax.dot_general(
                ref[...],
                onto,
                (((0,), (0,)), ((), ())),
                precision=lax.Precision.HIGHEST,
                preferred_element_type=F32,
            )
        up = jnp.where(row == 0, 0.0, pltpu.roll(x, 1, 0))
        down = jnp.where(row == 255, 0.0, pltpu.roll(x, 255, 0))
        o_ref[c] = (x + up + down)[:, :16] * scale_ref[...]


def final(box, left, right, scale):
    return pl.pallas_call(
        _final_kernel,
        out_shape=jax.ShapeDtypeStruct((2, 256, 16), F32),
        name="final",
    )(box, left, right, scale)


def neighbours(first, second):
    devices = lax.axis_size(ALL)
    up = [(i, i + 1) for i in range(devices - 1)]
    down = [(j, i) for i, j in up]
    return lax.ppermute(first, ALL, up), lax.ppermute(second, ALL, down)


def local(master_raw, slave_raw, range_ref, az_ref, az_shift, rg_shift, valid_lines):
    hf = range_ref.reshape(2, NS, NQ, NP).transpose(3, 2, 0, 1).reshape(NP * NQ, 2, NS)
    hf = jnp.pad(hf, ((0, 0), (0, 0), (0, 3)))
    h = az_ref.reshape(2, 128, 16).transpose(2, 0, 1) * (1.0 / LINES)

    def lines_of(raw):
        return lax.all_to_all(pre(raw), "rg", 0, 0, tiled=True)

    def columns_of(ranged):
        return lax.all_to_all(ranged, ALL, 0, 0, tiled=True)

    slave = lines_of(slave_raw)
    master = lines_of(master_raw)
    slave = columns_of(range_compress(slave, hf))
    master = columns_of(range_compress(master, hf))
    ah, al = prep(h)
    focused, to_left, to_right = slave_azimuth(slave, ah, al)
    from_left, from_right = neighbours(to_right, to_left)
    moved = resample(az_shift, rg_shift, focused, from_left, from_right)

    flat = lax.axis_index(ALL)
    counts = lax.dynamic_slice(jnp.pad(valid_lines, 1), (flat * 2,), (4,))
    col_counts = jnp.repeat(counts[1:3], BR)[None, :]
    wide = jnp.concatenate([counts[:1], jnp.repeat(counts[1:3], BR // LOOK), counts[3:]])
    rows = LINES // LOOK
    groups = lax.broadcasted_iota(jnp.int32, (rows + 2, 18), 0) - 1
    pixels = jnp.clip(wide[None, :] - LOOK * groups, 0, LOOK) * LOOK
    pixels = jnp.where((groups >= 0) & (groups < rows), pixels, 0).astype(F32)
    box_pixels = sum(pixels[i : i + rows, j : j + 16] for i in range(3) for j in range(3))
    scale = 1.0 / jnp.sqrt(jnp.maximum(box_pixels, 1.0))

    box, edge_left, edge_right = master_looks(master, ah, al, moved, col_counts)
    left, right = neighbours(edge_right, edge_left)
    return final(box, left, right, scale)


def solution(mesh):
    return jax.shard_map(
        local,
        mesh=mesh,
        in_specs=(
            P(None, "az", "rg"),
            P(None, "az", "rg"),
            P(),
            P(),
            P(None, ALL),
            P(None, ALL),
            P(),
        ),
        out_specs=P(None, None, ALL),
        check_vma=False,
    )
```

```python
import math

import jax
import jax.numpy as jnp
import numpy as np
from jax import lax
from jax.experimental import pallas as pl
from jax.experimental.pallas import tpu as pltpu
from jax.sharding import PartitionSpec as P

LINES = 2048
RANGE = 20000
RV = 16384
LOOK = 8
BA = 512
BR = 64
ASH = 32
RSH = 64
NBA = 4
ALL = ("az", "rg")
NP = 16
NQ = 10
NS = 125
RPAD = 1280
F32 = jnp.float32
BF16 = jnp.bfloat16


def _rot(v, angle):
    c, s = math.cos(angle), math.sin(angle)
    turns = angle / (math.pi / 4)
    eighth = round(turns)
    x, y = v
    if abs(turns - eighth) < 1e-9:
        e = eighth % 8
        if e == 0:
            return v
        if e == 2:
            return (-y, x)
        if e == 4:
            return (-x, -y)
        if e == 6:
            return (y, -x)
        h = math.sqrt(0.5)
        if e == 1:
            return ((x - y) * h, (x + y) * h)
        if e == 3:
            return (-(x + y) * h, (x - y) * h)
        if e == 5:
            return ((y - x) * h, -(x + y) * h)
        return ((x + y) * h, (y - x) * h)
    return (x * c - y * s, x * s + y * c)


def _add(a, b):
    return (a[0] + b[0], a[1] + b[1])


def _sub(a, b):
    return (a[0] - b[0], a[1] - b[1])


def _dft2(v, sign):
    return [_add(v[0], v[1]), _sub(v[0], v[1])]


def _dft4(v, sign):
    a, b = _add(v[0], v[2]), _sub(v[0], v[2])
    c, d = _add(v[1], v[3]), _sub(v[1], v[3])
    if sign < 0:
        return [_add(a, c), (b[0] + d[1], b[1] - d[0]), _sub(a, c), (b[0] - d[1], b[1] + d[0])]
    return [_add(a, c), (b[0] - d[1], b[1] + d[0]), _sub(a, c), (b[0] + d[1], b[1] - d[0])]


def _dft5(v, sign):
    c1, c2 = math.cos(2 * math.pi / 5), math.cos(4 * math.pi / 5)
    s1, s2 = sign * math.sin(2 * math.pi / 5), sign * math.sin(4 * math.pi / 5)
    a1, b1 = _add(v[1], v[4]), _sub(v[1], v[4])
    a2, b2 = _add(v[2], v[3]), _sub(v[2], v[3])
    x0 = v[0]
    y0 = (x0[0] + a1[0] + a2[0], x0[1] + a1[1] + a2[1])
    p1 = tuple(x0[i] + c1 * a1[i] + c2 * a2[i] for i in range(2))
    p2 = tuple(x0[i] + c2 * a1[i] + c1 * a2[i] for i in range(2))
    q1 = tuple(s1 * b1[i] + s2 * b2[i] for i in range(2))
    q2 = tuple(s2 * b1[i] - s1 * b2[i] for i in range(2))
    return [
        y0,
        (p1[0] - q1[1], p1[1] + q1[0]),
        (p2[0] - q2[1], p2[1] + q2[0]),
        (p2[0] + q2[1], p2[1] - q2[0]),
        (p1[0] + q1[1], p1[1] - q1[0]),
    ]


def _dft_two(v, n1, n2, first, second, sign):
    n = n1 * n2
    out = [None] * n
    mid = []
    for b in range(n2):
        col = first([v[n2 * a + b] for a in range(n1)], sign)
        mid.append([_rot(col[k], sign * 2 * math.pi * ((b * k) % n) / n) for k in range(n1)])
    for k1 in range(n1):
        row = second([mid[b][k1] for b in range(n2)], sign)
        for k2 in range(n2):
            out[k1 + n1 * k2] = row[k2]
    return out


def dft16(v, sign):
    return _dft_two(v, 4, 4, _dft4, _dft4, sign)


def dft10(v, sign):
    return _dft_two(v, 2, 5, _dft2, _dft5, sign)


def cmul(a, b):
    return (a[0] * b[0] - a[1] * b[1], a[0] * b[1] + a[1] * b[0])


def split(x):
    hi = x.astype(BF16)
    return hi, (x - hi.astype(F32)).astype(BF16)


def dot(a, b):
    return jnp.dot(a, b, preferred_element_type=F32)


def worker(block):
    chip, core = divmod(block, 2)
    y, rest = divmod(chip, 16)
    return (y * 2 + core) * 16 + rest


def _np_split(x):
    x = np.asarray(x, np.float32)
    hi = x.astype(BF16)
    return hi, (x - hi.astype(np.float32)).astype(BF16)


def _tables():
    t = {}
    two = 2 * np.pi
    q2 = np.arange(128)
    keep = (q2 < NS)[None, :]
    ang = -two * ((np.arange(NQ)[:, None] * q2[None, :]) % 1250) / 1250
    t["twb"] = np.stack([np.cos(ang) * keep, np.sin(ang) * keep], 1).astype(np.float32)
    n = np.arange(NQ)[None, :, None] * NS + q2[None, None, :]
    ang = two * ((np.arange(NP)[:, None, None] * n) % RANGE) / RANGE
    t["twc"] = np.stack([np.cos(ang), np.sin(ang)], 2).reshape(NP * NQ, 2, 128).astype(np.float32)
    ang = two * ((q2[:, None] * q2[None, :]) % NS) / NS
    both = keep & keep.T
    c, s = np.cos(ang) * both, np.sin(ang) * both
    t["fh"], t["fl"] = _np_split(np.block([[c, -s], [s, c]]))
    t["gh"], t["gl"] = _np_split(np.block([[c, s], [-s, c]]))
    k2 = np.arange(128)
    l2 = np.arange(128)
    ang = -two * ((l2[:, None] * k2[None, :]) % 128) / 128
    pr, pi = np.cos(ang), np.sin(ang)
    ang = np.broadcast_to(-two * l2[:, None] / LINES, (128, 128))
    wr, wi = np.cos(ang), np.sin(ang)
    t["p"] = np.stack([pr, pi]).astype(np.float32)
    t["w"] = np.stack([wr, wi]).astype(np.float32)
    kk = np.arange(256)
    part, line = (kk // 16) % 2, (kk // 32) * 16 + kk % 16
    sel = (part == 0)[:, None]
    t["q"] = np.stack(
        [np.where(sel, pr[line], -pi[line]), np.where(sel, -pi[line], -pr[line])]
    ).astype(np.float32)
    t["v"] = np.stack([wr[line], wi[line]]).astype(np.float32)
    lane = np.arange(128)
    pick = np.zeros((24, 128), np.float32)
    for o in range(16):
        pick[o] = np.abs(lane // LOOK - o) <= 1
    pick[16] = lane < LOOK
    pick[17] = lane >= 128 - LOOK
    t["pick"] = pick
    return t


TABLES = _tables()


def _pre_kernel(x_ref, o_ref):
    for q in range(2):
        for half in range(2):
            for c in range(2):
                v = x_ref[pl.ds(500 * q + 2 * half + c, NS, stride=4), :]
                v = jnp.concatenate([v, jnp.zeros((128 - NS, 128), F32)], axis=0).T
                for k in range(8):
                    o_ref[8 * half + k, q, c] = v[16 * k : 16 * k + 16]


def pre(raw):
    rows = raw.transpose(2, 0, 1).reshape(1250, 2, 2, 128).transpose(0, 2, 1, 3).reshape(5000, 128)
    return pl.pallas_call(
        _pre_kernel,
        grid=(5,),
        in_specs=[pl.BlockSpec((1000, 128), lambda i: (i, 0))],
        out_specs=pl.BlockSpec((NP, 2, 2, 16, 128), lambda i: (0, i, 0, 0, 0)),
        out_shape=jax.ShapeDtypeStruct((NP, NQ, 2, 16, 128), F32),
        cost_estimate=pl.CostEstimate(flops=10**8, bytes_accessed=5 * 10**6, transcendentals=0),
        compiler_params=pltpu.CompilerParams(vmem_limit_bytes=8 << 20),
        name="pre",
    )(rows)


def _range_kernel(x_ref, twb_ref, hf_ref, fh_ref, fl_ref, gh_ref, gl_ref, twc_ref, o_ref, d_ref):
    lane = lax.broadcasted_iota(jnp.int32, (16, 128), 1)

    def outer(q, carry):
        for g in range(2):
            rows = slice(8 * g, 8 * g + 8)
            v = [(x_ref[p, q, 0, rows, :], x_ref[p, q, 1, rows, :]) for p in range(NP)]
            v = dft16(v, -1)
            for k in range(NP):
                at = k * NQ + q
                r, i = cmul(v[k], (twc_ref[at, 0:1, :], -twc_ref[at, 1:2, :]))
                d_ref[at, 0, rows, :] = r
                d_ref[at, 1, rows, :] = i
        return carry

    lax.fori_loop(0, NQ, outer, 0)

    def middle(kp, carry):
        v = [(d_ref[kp * NQ + q, 0], d_ref[kp * NQ + q, 1]) for q in range(NQ)]
        v = dft10(v, -1)
        rows = []
        for k in range(NQ):
            r, i = cmul(v[k], (twb_ref[k, 0:1, :], twb_ref[k, 1:2, :]))
            rows.append(jnp.concatenate([r, i], axis=1))
        hi, lo = split(jnp.concatenate(rows, axis=0))
        y = dot(hi, fh_ref[...]) + dot(lo, fh_ref[...]) + dot(hi, fl_ref[...])
        rows = []
        for k in range(NQ):
            val = (y[16 * k : 16 * k + 16, :128], y[16 * k : 16 * k + 16, 128:])
            r, i = cmul(val, (hf_ref[kp * NQ + k, 0:1, :], hf_ref[kp * NQ + k, 1:2, :]))
            rows.append(jnp.concatenate([r, i], axis=1))
        hi, lo = split(jnp.concatenate(rows, axis=0))
        y = dot(hi, gh_ref[...]) + dot(lo, gh_ref[...]) + dot(hi, gl_ref[...])
        v = []
        for k in range(NQ):
            val = (y[16 * k : 16 * k + 16, :128], y[16 * k : 16 * k + 16, 128:])
            v.append(cmul(val, (twb_ref[k, 0:1, :], -twb_ref[k, 1:2, :])))
        v = dft10(v, 1)
        for q in range(NQ):
            at = kp * NQ + q
            r, i = cmul(v[q], (twc_ref[at, 0:1, :], twc_ref[at, 1:2, :]))
            d_ref[at, 0] = r
            d_ref[at, 1] = i
        return carry

    lax.fori_loop(0, NP, middle, 0, unroll=2)

    def inner(q, carry):
        for g in range(2):
            rows = slice(8 * g, 8 * g + 8)
            v = [(d_ref[k * NQ + q, 0, rows, :], d_ref[k * NQ + q, 1, rows, :]) for k in range(NP)]
            v = dft16(v, 1)
            for p in range(14):
                d_ref[p * NQ + q, 0, rows, :] = v[p][0]
                d_ref[p * NQ + q, 1, rows, :] = v[p][1]
        return carry

    lax.fori_loop(0, NQ, inner, 0)

    for d in range(128):
        n, a = divmod(128 * d, NS)
        for c in range(2):
            val = d_ref[n, c]
            if a:
                val = pltpu.roll(val, 128 - a, 1)
            start = NS - a
            while start < 128:
                n2 = (128 * d + start) // NS
                nxt = d_ref[n2, c]
                nxt = pltpu.roll(nxt, start % 128, 1)
                val = jnp.where(lane < start, val, nxt)
                start += NS
            o_ref[worker(d), c] = val


def range_compress(x, hf):
    t = TABLES
    return pl.pallas_call(
        _range_kernel,
        out_shape=jax.ShapeDtypeStruct((128, 2, 16, 128), F32),
        scratch_shapes=[pltpu.VMEM((NP * NQ, 2, 16, 128), F32)],
        cost_estimate=pl.CostEstimate(flops=10**10, bytes_accessed=6 * 10**6, transcendentals=0),
        compiler_params=pltpu.CompilerParams(vmem_limit_bytes=24 << 20),
        name="range",
    )(x, t["twb"], hf, t["fh"], t["fl"], t["gh"], t["gl"], t["twc"])


def _dot_t(a, b):
    return lax.dot_general(
        a, b, (((1,), (1,)), ((), ())), precision=lax.Precision.HIGHEST, preferred_element_type=F32
    )


def _prep_kernel(h_ref, p0_ref, w_ref, q0_ref, v_ref, ah_ref, al_ref, p_ref, q_ref):
    p_ref[...] = p0_ref[...]
    q_ref[...] = q0_ref[...]

    def body(k, carry):
        pr, pi = p_ref[0], p_ref[1]
        q1, q2 = q_ref[0], q_ref[1]
        hr, hi = h_ref[k, 0:1, :], h_ref[k, 1:2, :]
        vr, vi = cmul((pr, -pi), (hr, hi))
        top = _dot_t(vr, q1) + _dot_t(vi, q2)
        bottom = _dot_t(vi, q1) - _dot_t(vr, q2)
        high, low = split(top)
        ah_ref[k, 0:128, :] = high
        al_ref[k, 0:128, :] = low
        high, low = split(bottom)
        ah_ref[k, 128:256, :] = high
        al_ref[k, 128:256, :] = low
        pr, pi = cmul((pr, pi), (w_ref[0], w_ref[1]))
        p_ref[0] = pr
        p_ref[1] = pi
        wr, wi = v_ref[0], v_ref[1]
        q_ref[0] = q1 * wr + q2 * wi
        q_ref[1] = q2 * wr - q1 * wi
        return carry

    lax.fori_loop(0, 16, body, 0)


def prep(h):
    t = TABLES
    shape = jax.ShapeDtypeStruct((16, 256, 256), BF16)
    return pl.pallas_call(
        _prep_kernel,
        out_shape=(shape, shape),
        scratch_shapes=[pltpu.VMEM((2, 128, 128), F32), pltpu.VMEM((2, 256, 128), F32)],
        cost_estimate=pl.CostEstimate(flops=5 * 10**9, bytes_accessed=5 * 10**6, transcendentals=0),
        compiler_params=pltpu.CompilerParams(vmem_limit_bytes=16 << 20),
        name="prep",
    )(h, t["p"], t["w"], t["q"], t["v"])


def _azimuth_front(x_ref, ah_ref, al_ref, e_ref):
    def first(s, carry):
        for g in range(2):
            rows = slice(8 * g, 8 * g + 8)
            v = [(x_ref[8 * a + s, 0, rows, :], x_ref[8 * a + s, 1, rows, :]) for a in range(16)]
            v = dft16(v, -1)
            for k in range(16):
                for c in range(2):
                    at = pl.multiple_of(s * 32 + c * 16 + g * 8, 8)
                    e_ref[k, pl.ds(at, 8), :] = v[k][c]
        return carry

    lax.fori_loop(0, 8, first, 0)

    def second(k, carry):
        hi, lo = split(e_ref[k])
        wide = dot(ah_ref[k], jnp.concatenate([hi, lo], axis=1))
        e_ref[k] = wide[:, :128] + wide[:, 128:] + dot(al_ref[k], hi)
        return carry

    lax.fori_loop(0, 16, second, 0, unroll=4)


def _azimuth_rows(e_ref, g):
    at = [pl.multiple_of(c * 128 + g * 8, 8) for c in range(2)]
    v = [(e_ref[k, pl.ds(at[0], 8), :], e_ref[k, pl.ds(at[1], 8), :]) for k in range(16)]
    return dft16(v, 1)


def _slave_kernel(x_ref, ah_ref, al_ref, o_ref, left_ref, right_ref, e_ref):
    _azimuth_front(x_ref, ah_ref, al_ref, e_ref)
    low = lax.broadcasted_iota(jnp.int32, (8, 128), 1) < 64
    zero = jnp.zeros((ASH, 128), F32)
    for ref in (o_ref.at[0], o_ref.at[1], left_ref, right_ref):
        ref[0:ASH, :] = zero
        ref[ASH + LINES :, :] = zero

    def third(g, carry):
        v = _azimuth_rows(e_ref, g)
        for a in range(16):
            rows = pl.ds(pl.multiple_of(a * 128 + g * 8 + ASH, 8), 8)
            r, i = v[a]
            o_ref[0, rows, :] = r
            o_ref[1, rows, :] = i
            left_ref[rows, :] = jnp.where(low, r, pltpu.roll(i, 64, 1))
            right_ref[rows, :] = jnp.where(low, pltpu.roll(r, 64, 1), i)
        return carry

    lax.fori_loop(0, 16, third, 0)


def slave_azimuth(x, ah, al):
    side = jax.ShapeDtypeStruct((LINES + 2 * ASH, 128), F32)
    return pl.pallas_call(
        _slave_kernel,
        out_shape=(jax.ShapeDtypeStruct((2, LINES + 2 * ASH, 128), F32), side, side),
        scratch_shapes=[pltpu.VMEM((16, 256, 128), F32)],
        cost_estimate=pl.CostEstimate(flops=5 * 10**9, bytes_accessed=10**7, transcendentals=0),
        compiler_params=pltpu.CompilerParams(vmem_limit_bytes=24 << 20),
        name="slave_azimuth",
    )(x, ah, al)


def _resample_kernel(az_ref, rg_ref, s_ref, left_ref, right_ref, o_ref):
    lane = lax.broadcasted_iota(jnp.int32, (64, 128), 1)
    low = lane < 64

    def move(t, carry):
        block = t // 8
        parts = []
        for r, side_ref in ((0, left_ref), (1, right_ref)):
            shift = rg_ref[block, r]
            rows = pl.ds(t * 64 + ASH + az_ref[block, r], 64)
            whole = lax.rem(256 - shift, 128)
            half = lax.rem(192 - shift, 128)
            near = lane + shift >= 0 if r == 0 else lane + shift < 128
            side = side_ref[rows, :]
            turns = (half, whole) if r == 0 else (whole, half)
            parts.append(
                [
                    jnp.where(
                        near,
                        pltpu.roll(s_ref[c, rows, :], whole, 1),
                        pltpu.roll(side, turns[c], 1),
                    )
                    for c in range(2)
                ]
            )
        rows = pl.ds(pl.multiple_of(t * 64, 64), 64)
        for c in range(2):
            o_ref[c, rows, :] = jnp.where(low, parts[0][c], parts[1][c])
        return carry

    lax.fori_loop(0, LINES // 64, move, 0, unroll=2)


def resample(az_shift, rg_shift, focused, left, right):
    return pl.pallas_call(
        _resample_kernel,
        in_specs=[pl.BlockSpec(memory_space=pltpu.SMEM)] * 2
        + [pl.BlockSpec(memory_space=pltpu.VMEM)] * 3,
        out_shape=jax.ShapeDtypeStruct((2, LINES, 128), F32),
        cost_estimate=pl.CostEstimate(flops=2 * 10**9, bytes_accessed=10**7, transcendentals=0),
        compiler_params=pltpu.CompilerParams(vmem_limit_bytes=16 << 20),
        name="resample",
    )(az_shift, rg_shift, focused, left, right)


def _master_kernel(x_ref, ah_ref, al_ref, m_ref, n_ref, pick_ref, box_ref, side_ref, e_ref, c_ref):
    _azimuth_front(x_ref, ah_ref, al_ref, e_ref)
    line = lax.broadcasted_iota(jnp.int32, (8, 128), 0)
    count = n_ref[...]

    def third(g, carry):
        v = _azimuth_rows(e_ref, g)
        for a in range(16):
            at = pl.multiple_of(a * 128 + g * 8, 8)
            r, i = v[a]
            sr, si = m_ref[0, pl.ds(at, 8), :], m_ref[1, pl.ds(at, 8), :]
            keep = line + at < count
            c_ref[pl.ds(at, 8), :] = jnp.where(keep, r * sr + i * si, 0.0)
            c_ref[pl.ds(at + LINES, 8), :] = jnp.where(keep, i * sr - r * si, 0.0)
        return carry

    lax.fori_loop(0, 16, third, 0)
    total = c_ref[pl.ds(0, 512, stride=LOOK), :]
    for j in range(1, LOOK):
        total = total + c_ref[pl.ds(j, 512, stride=LOOK), :]
    y = _dot_t(pick_ref[...], total)
    cell = lax.broadcasted_iota(jnp.int32, (24, 512), 1) % 256
    y = (
        y
        + jnp.where(cell == 0, 0.0, pltpu.roll(y, 1, 1))
        + jnp.where(cell == 255, 0.0, pltpu.roll(y, 511, 1))
    )
    box_ref[...] = y[:16]
    side_ref[...] = y[16:]


def master_looks(x, ah, al, moved, counts):
    return pl.pallas_call(
        _master_kernel,
        out_shape=(
            jax.ShapeDtypeStruct((16, 512), F32),
            jax.ShapeDtypeStruct((8, 512), F32),
        ),
        scratch_shapes=[pltpu.VMEM((16, 256, 128), F32), pltpu.VMEM((2 * LINES, 128), F32)],
        cost_estimate=pl.CostEstimate(flops=5 * 10**9, bytes_accessed=10**7, transcendentals=0),
        compiler_params=pltpu.CompilerParams(vmem_limit_bytes=24 << 20),
        name="master_looks",
    )(x, ah, al, moved, counts, TABLES["pick"])


def _final_kernel(box_ref, left_ref, right_ref, scale_ref, o_ref):
    row = lax.broadcasted_iota(jnp.int32, (16, 256), 0)
    for c in range(2):
        at = slice(256 * c, 256 * c + 256)
        x = box_ref[:, at]
        x = x + jnp.where(row == 0, left_ref[1:2, at], 0.0)
        x = x + jnp.where(row == 15, right_ref[0:1, at], 0.0)
        o_ref[c] = x * scale_ref[...]


def final(box, left, right, scale):
    return pl.pallas_call(
        _final_kernel,
        out_shape=jax.ShapeDtypeStruct((2, 16, 256), F32),
        compiler_params=pltpu.CompilerParams(vmem_limit_bytes=4 << 20),
        name="final",
    )(box, left, right, scale)


def to_worker(x):
    return lax.ppermute(x, ALL, [(b, worker(b)) for b in range(128)])


def halo(to_right, to_left):
    up = [(worker(b), worker(b + 1)) for b in range(127)]
    down = [(j, i) for i, j in up]
    return lax.ppermute(to_right, ALL, up), lax.ppermute(to_left, ALL, down)


def local(master_raw, slave_raw, range_ref, az_ref, az_shift, rg_shift, valid_lines):
    hf = range_ref.reshape(2, NS, NQ, NP).transpose(3, 2, 0, 1).reshape(NP * NQ, 2, NS)
    hf = jnp.pad(hf * (1.0 / RANGE), ((0, 0), (0, 0), (0, 3)))
    h = az_ref.reshape(2, 128, 16).transpose(2, 0, 1) * (1.0 / LINES)

    def lines_of(raw):
        return lax.all_to_all(pre(raw), "rg", 0, 0, tiled=True)

    def columns_of(ranged):
        return lax.all_to_all(ranged, ALL, 0, 0, tiled=True)

    flat = lax.axis_index(ALL)
    counts = lax.dynamic_slice(jnp.pad(valid_lines, 1), (flat * 2,), (4,))
    wide = jnp.concatenate([counts[:1], jnp.repeat(counts[1:3], BR // LOOK), counts[3:]])
    rows = LINES // LOOK
    groups = lax.broadcasted_iota(jnp.int32, (18, rows + 2), 1) - 1
    pixels = jnp.clip(wide[:, None] - LOOK * groups, 0, LOOK) * LOOK
    pixels = jnp.where((groups >= 0) & (groups < rows), pixels, 0).astype(F32)
    box_pixels = sum(pixels[j : j + 16, i : i + rows] for i in range(3) for j in range(3))
    scale = 1.0 / jnp.sqrt(jnp.maximum(box_pixels, 1.0))
    core = lax.axis_index("az") % 2
    block = ((lax.axis_index("az") // 2) * 16 + lax.axis_index("rg")) * 2 + core
    own = lax.dynamic_slice(valid_lines, (block * 2,), (2,))
    col_counts = jnp.repeat(own, BR)[None, :]
    shifts = to_worker(jnp.stack([az_shift, rg_shift]))

    slave = lines_of(slave_raw)
    master = lines_of(master_raw)
    ah, al = prep(h)
    slave, ah, al, hf, shifts, scale, col_counts = lax.optimization_barrier(
        (slave, ah, al, hf, shifts, scale, col_counts)
    )
    slave = columns_of(range_compress(slave, hf))
    master = columns_of(range_compress(master, hf))
    focused, to_left, to_right = slave_azimuth(slave, ah, al)
    from_left, from_right = halo(to_right, to_left)
    moved = resample(shifts[0], shifts[1], focused, from_left, from_right)

    box, side = master_looks(master, ah, al, moved, col_counts)
    box = lax.ppermute(box, ALL, [(worker(b), b) for b in range(128)])
    left = lax.ppermute(side, ALL, [(worker(b), b + 1) for b in range(127)])
    right = lax.ppermute(side, ALL, [(worker(b + 1), b) for b in range(127)])
    return final(box, left, right, scale).transpose(0, 2, 1)


def solution(mesh):
    return jax.shard_map(
        local,
        mesh=mesh,
        in_specs=(
            P(None, "az", "rg"),
            P(None, "az", "rg"),
            P(),
            P(),
            P(None, ALL),
            P(None, ALL),
            P(),
        ),
        out_specs=P(None, None, ALL),
        check_vma=False,
    )
```

```python
import math
from functools import partial

import jax
import jax.numpy as jnp
import numpy as np
from jax import lax
from jax.experimental import pallas as pl
from jax.experimental.pallas import tpu as pltpu
from jax.sharding import PartitionSpec as P

LINES = 2048
RANGE = 20000
RV = 16384
LOOK = 8
BA = 512
BR = 64
ASH = 32
RSH = 64
NBA = 4
ALL = ("az", "rg")
NP = 16
NQ = 10
NS = 125
RPAD = 1280
F32 = jnp.float32
BF16 = jnp.bfloat16


def _rot(v, angle):
    c, s = math.cos(angle), math.sin(angle)
    turns = angle / (math.pi / 4)
    eighth = round(turns)
    x, y = v
    if abs(turns - eighth) < 1e-9:
        e = eighth % 8
        if e == 0:
            return v
        if e == 2:
            return (-y, x)
        if e == 4:
            return (-x, -y)
        if e == 6:
            return (y, -x)
        h = math.sqrt(0.5)
        if e == 1:
            return ((x - y) * h, (x + y) * h)
        if e == 3:
            return (-(x + y) * h, (x - y) * h)
        if e == 5:
            return ((y - x) * h, -(x + y) * h)
        return ((x + y) * h, (y - x) * h)
    return (x * c - y * s, x * s + y * c)


def _add(a, b):
    return (a[0] + b[0], a[1] + b[1])


def _sub(a, b):
    return (a[0] - b[0], a[1] - b[1])


def _dft2(v, sign):
    return [_add(v[0], v[1]), _sub(v[0], v[1])]


def _dft4(v, sign):
    a, b = _add(v[0], v[2]), _sub(v[0], v[2])
    c, d = _add(v[1], v[3]), _sub(v[1], v[3])
    if sign < 0:
        return [_add(a, c), (b[0] + d[1], b[1] - d[0]), _sub(a, c), (b[0] - d[1], b[1] + d[0])]
    return [_add(a, c), (b[0] - d[1], b[1] + d[0]), _sub(a, c), (b[0] + d[1], b[1] - d[0])]


def _dft5(v, sign):
    c1, c2 = math.cos(2 * math.pi / 5), math.cos(4 * math.pi / 5)
    s1, s2 = sign * math.sin(2 * math.pi / 5), sign * math.sin(4 * math.pi / 5)
    a1, b1 = _add(v[1], v[4]), _sub(v[1], v[4])
    a2, b2 = _add(v[2], v[3]), _sub(v[2], v[3])
    x0 = v[0]
    y0 = (x0[0] + a1[0] + a2[0], x0[1] + a1[1] + a2[1])
    p1 = tuple(x0[i] + c1 * a1[i] + c2 * a2[i] for i in range(2))
    p2 = tuple(x0[i] + c2 * a1[i] + c1 * a2[i] for i in range(2))
    q1 = tuple(s1 * b1[i] + s2 * b2[i] for i in range(2))
    q2 = tuple(s2 * b1[i] - s1 * b2[i] for i in range(2))
    return [
        y0,
        (p1[0] - q1[1], p1[1] + q1[0]),
        (p2[0] - q2[1], p2[1] + q2[0]),
        (p2[0] + q2[1], p2[1] - q2[0]),
        (p1[0] + q1[1], p1[1] - q1[0]),
    ]


def _dft_two(v, n1, n2, first, second, sign):
    n = n1 * n2
    out = [None] * n
    mid = []
    for b in range(n2):
        col = first([v[n2 * a + b] for a in range(n1)], sign)
        mid.append([_rot(col[k], sign * 2 * math.pi * ((b * k) % n) / n) for k in range(n1)])
    for k1 in range(n1):
        row = second([mid[b][k1] for b in range(n2)], sign)
        for k2 in range(n2):
            out[k1 + n1 * k2] = row[k2]
    return out


def dft16(v, sign):
    return _dft_two(v, 4, 4, _dft4, _dft4, sign)


def dft10(v, sign):
    return _dft_two(v, 2, 5, _dft2, _dft5, sign)


def cmul(a, b):
    return (a[0] * b[0] - a[1] * b[1], a[0] * b[1] + a[1] * b[0])


def split(x):
    hi = x.astype(BF16)
    return hi, (x - hi.astype(F32)).astype(BF16)


def dot(a, b):
    return jnp.dot(a, b, preferred_element_type=F32)


def worker(block):
    chip, core = divmod(block, 2)
    y, rest = divmod(chip, 16)
    return (y * 2 + core) * 16 + rest


def _np_split(x):
    x = np.asarray(x, np.float32)
    hi = x.astype(BF16)
    return hi, (x - hi.astype(np.float32)).astype(BF16)


def _tables():
    t = {}
    two = 2 * np.pi
    q2 = np.arange(128)
    keep = (q2 < NS)[None, :]
    ang = -two * ((np.arange(NQ)[:, None] * q2[None, :]) % 1250) / 1250
    t["twb"] = np.stack([np.cos(ang) * keep, np.sin(ang) * keep], 1).astype(np.float32)
    n = np.arange(NQ)[None, :, None] * NS + q2[None, None, :]
    ang = two * ((np.arange(NP)[:, None, None] * n) % RANGE) / RANGE
    t["twc"] = np.stack([np.cos(ang), np.sin(ang)], 2).reshape(NP * NQ, 2, 128).astype(np.float32)
    ang = two * ((q2[:, None] * q2[None, :]) % NS) / NS
    both = keep & keep.T
    c, s = np.cos(ang) * both, np.sin(ang) * both
    t["fh"], t["fl"] = _np_split(np.block([[c, -s], [s, c]]))
    t["gh"], t["gl"] = _np_split(np.block([[c, s], [-s, c]]))
    k2 = np.arange(128)
    l2 = np.arange(128)
    ang = -two * ((l2[:, None] * k2[None, :]) % 128) / 128
    pr, pi = np.cos(ang), np.sin(ang)
    ang = np.broadcast_to(-two * l2[:, None] / LINES, (128, 128))
    wr, wi = np.cos(ang), np.sin(ang)
    t["p"] = np.stack([pr, pi]).astype(np.float32)
    t["w"] = np.stack([wr, wi]).astype(np.float32)
    kk = np.arange(256)
    part, line = (kk // 16) % 2, (kk // 32) * 16 + kk % 16
    sel = (part == 0)[:, None]
    t["q"] = np.stack(
        [np.where(sel, pr[line], -pi[line]), np.where(sel, -pi[line], -pr[line])]
    ).astype(np.float32)
    t["v"] = np.stack([wr[line], wi[line]]).astype(np.float32)
    lane = np.arange(128)
    pick = np.zeros((24, 128), np.float32)
    for o in range(16):
        pick[o] = np.abs(lane // LOOK - o) <= 1
    pick[16] = lane < LOOK
    pick[17] = lane >= 128 - LOOK
    t["pick"] = pick
    return t


TABLES = _tables()


HBM = pl.BlockSpec(memory_space=pltpu.HBM)
VMEM = pl.BlockSpec(memory_space=pltpu.VMEM)
SMEM = pl.BlockSpec(memory_space=pltpu.SMEM)


def limit(mib):
    return pltpu.CompilerParams(vmem_limit_bytes=mib << 20)


def _pre_kernel(first_ref, second_ref, o_ref):
    for image, x_ref in enumerate((first_ref, second_ref)):
        for q in range(2):
            for half in range(2):
                for c in range(2):
                    v = x_ref[pl.ds(500 * q + 2 * half + c, NS, stride=4), :]
                    v = jnp.concatenate([v, jnp.zeros((128 - NS, 128), F32)], axis=0).T
                    for k in range(8):
                        o_ref[8 * half + k, image, q, c] = v[16 * k : 16 * k + 16]


def pre(first, second):
    def rows(raw):
        raw = raw.transpose(2, 0, 1).reshape(1250, 2, 2, 128)
        return raw.transpose(0, 2, 1, 3).reshape(5000, 128)

    return pl.pallas_call(
        _pre_kernel,
        grid=(5,),
        in_specs=[pl.BlockSpec((1000, 128), lambda i: (i, 0))] * 2,
        out_specs=pl.BlockSpec((NP, 2, 2, 2, 16, 128), lambda i: (0, 0, i, 0, 0, 0)),
        out_shape=jax.ShapeDtypeStruct((NP, 2, NQ, 2, 16, 128), F32),
        cost_estimate=pl.CostEstimate(flops=10**8, bytes_accessed=10**7, transcendentals=0),
        name="pre",
    )(rows(first), rows(second))


def _range_kernel(image, x_hbm, twb_ref, hf_ref, fh_ref, fl_ref, gh_ref, gl_ref, twc_ref, o_hbm, d_ref, x_ref, o_ref, in_sem, out_sem):
    lane = lax.broadcasted_iota(jnp.int32, (16, 128), 1)

    def load(q):
        return pltpu.make_async_copy(x_hbm.at[:, image, q], x_ref.at[:, q], in_sem.at[q])

    for q in range(NQ):
        load(q).start()

    def outer(q, carry):
        load(q).wait()
        for g in range(2):
            rows = slice(8 * g, 8 * g + 8)
            v = [(x_ref[p, q, 0, rows, :], x_ref[p, q, 1, rows, :]) for p in range(NP)]
            v = dft16(v, -1)
            for k in range(NP):
                at = k * NQ + q
                r, i = cmul(v[k], (twc_ref[at, 0:1, :], -twc_ref[at, 1:2, :]))
                d_ref[at, 0, rows, :] = r
                d_ref[at, 1, rows, :] = i
        return carry

    lax.fori_loop(0, NQ, outer, 0)

    def middle(kp, carry):
        v = [(d_ref[kp * NQ + q, 0], d_ref[kp * NQ + q, 1]) for q in range(NQ)]
        v = dft10(v, -1)
        rows = []
        for k in range(NQ):
            r, i = cmul(v[k], (twb_ref[k, 0:1, :], twb_ref[k, 1:2, :]))
            rows.append(jnp.concatenate([r, i], axis=1))
        hi, lo = split(jnp.concatenate(rows, axis=0))
        y = dot(hi, fh_ref[...]) + dot(lo, fh_ref[...]) + dot(hi, fl_ref[...])
        rows = []
        for k in range(NQ):
            val = (y[16 * k : 16 * k + 16, :128], y[16 * k : 16 * k + 16, 128:])
            r, i = cmul(val, (hf_ref[kp * NQ + k, 0:1, :], hf_ref[kp * NQ + k, 1:2, :]))
            rows.append(jnp.concatenate([r, i], axis=1))
        hi, lo = split(jnp.concatenate(rows, axis=0))
        y = dot(hi, gh_ref[...]) + dot(lo, gh_ref[...]) + dot(hi, gl_ref[...])
        v = []
        for k in range(NQ):
            val = (y[16 * k : 16 * k + 16, :128], y[16 * k : 16 * k + 16, 128:])
            v.append(cmul(val, (twb_ref[k, 0:1, :], -twb_ref[k, 1:2, :])))
        v = dft10(v, 1)
        for q in range(NQ):
            at = kp * NQ + q
            r, i = cmul(v[q], (twc_ref[at, 0:1, :], twc_ref[at, 1:2, :]))
            d_ref[at, 0] = r
            d_ref[at, 1] = i
        return carry

    lax.fori_loop(0, NP, middle, 0, unroll=2)

    def inner(q, carry):
        for g in range(2):
            rows = slice(8 * g, 8 * g + 8)
            v = [(d_ref[k * NQ + q, 0, rows, :], d_ref[k * NQ + q, 1, rows, :]) for k in range(NP)]
            v = dft16(v, 1)
            for p in range(14):
                d_ref[p * NQ + q, 0, rows, :] = v[p][0]
                d_ref[p * NQ + q, 1, rows, :] = v[p][1]
        return carry

    lax.fori_loop(0, NQ, inner, 0)

    def store(part):
        at = pl.ds(32 * part, 32)
        return pltpu.make_async_copy(o_ref.at[at], o_hbm.at[at], out_sem.at[part])

    for d in range(128):
        n, a = divmod(128 * d, NS)
        for c in range(2):
            val = d_ref[n, c]
            if a:
                val = pltpu.roll(val, 128 - a, 1)
            start = NS - a
            while start < 128:
                n2 = (128 * d + start) // NS
                nxt = d_ref[n2, c]
                nxt = pltpu.roll(nxt, start % 128, 1)
                val = jnp.where(lane < start, val, nxt)
                start += NS
            o_ref[worker(d), c] = val
        if d % 32 == 31:
            store(d // 32).start()
    for part in range(4):
        store(part).wait()


def range_compress(x, image, hf):
    t = TABLES
    return pl.pallas_call(
        partial(_range_kernel, image),
        in_specs=[HBM] + [VMEM] * 7,
        out_specs=HBM,
        out_shape=jax.ShapeDtypeStruct((128, 2, 16, 128), F32),
        scratch_shapes=[
            pltpu.VMEM((NP * NQ, 2, 16, 128), F32),
            pltpu.VMEM((NP, NQ, 2, 16, 128), F32),
            pltpu.VMEM((128, 2, 16, 128), F32),
            pltpu.SemaphoreType.DMA((NQ,)),
            pltpu.SemaphoreType.DMA((4,)),
        ],
        cost_estimate=pl.CostEstimate(flops=10**10, bytes_accessed=6 * 10**6, transcendentals=0),
        name="range",
    )(x, t["twb"], hf, t["fh"], t["fl"], t["gh"], t["gl"], t["twc"])


def _dot_t(a, b):
    return lax.dot_general(
        a, b, (((1,), (1,)), ((), ())), precision=lax.Precision.HIGHEST, preferred_element_type=F32
    )


def _prep_kernel(h_ref, p0_ref, w_ref, q0_ref, v_ref, ah_ref, al_ref, p_ref, q_ref):
    p_ref[...] = p0_ref[...]
    q_ref[...] = q0_ref[...]

    def body(k, carry):
        pr, pi = p_ref[0], p_ref[1]
        q1, q2 = q_ref[0], q_ref[1]
        hr, hi = h_ref[k, 0:1, :], h_ref[k, 1:2, :]
        vr, vi = cmul((pr, -pi), (hr, hi))
        top = _dot_t(vr, q1) + _dot_t(vi, q2)
        bottom = _dot_t(vi, q1) - _dot_t(vr, q2)
        high, low = split(top)
        ah_ref[k, 0:128, :] = high
        al_ref[k, 0:128, :] = low
        high, low = split(bottom)
        ah_ref[k, 128:256, :] = high
        al_ref[k, 128:256, :] = low
        pr, pi = cmul((pr, pi), (w_ref[0], w_ref[1]))
        p_ref[0] = pr
        p_ref[1] = pi
        wr, wi = v_ref[0], v_ref[1]
        q_ref[0] = q1 * wr + q2 * wi
        q_ref[1] = q2 * wr - q1 * wi
        return carry

    lax.fori_loop(0, 16, body, 0)


def prep(h):
    t = TABLES
    shape = jax.ShapeDtypeStruct((16, 256, 256), BF16)
    return pl.pallas_call(
        _prep_kernel,
        out_shape=(shape, shape),
        scratch_shapes=[pltpu.VMEM((2, 128, 128), F32), pltpu.VMEM((2, 256, 128), F32)],
        cost_estimate=pl.CostEstimate(flops=5 * 10**9, bytes_accessed=5 * 10**6, transcendentals=0),
        name="prep",
    )(h, t["p"], t["w"], t["q"], t["v"])


def _azimuth_front(x_ref, ah_hbm, al_hbm, e_ref, ah_ref, al_ref, sem):
    matrices = [
        pltpu.make_async_copy(ah_hbm, ah_ref, sem.at[0]),
        pltpu.make_async_copy(al_hbm, al_ref, sem.at[1]),
    ]
    for copy in matrices:
        copy.start()

    def first(s, carry):
        for g in range(2):
            rows = slice(8 * g, 8 * g + 8)
            v = [(x_ref[a, s, 0, rows, :], x_ref[a, s, 1, rows, :]) for a in range(16)]
            v = dft16(v, -1)
            for k in range(16):
                for c in range(2):
                    at = pl.multiple_of(s * 32 + c * 16 + g * 8, 8)
                    e_ref[k, pl.ds(at, 8), :] = v[k][c]
        return carry

    lax.fori_loop(0, 8, first, 0)
    for copy in matrices:
        copy.wait()

    def second(k, carry):
        hi, lo = split(e_ref[k])
        wide = dot(ah_ref[k], jnp.concatenate([hi, lo], axis=1))
        e_ref[k] = wide[:, :128] + wide[:, 128:] + dot(al_ref[k], hi)
        return carry

    lax.fori_loop(0, 16, second, 0, unroll=4)


AZIMUTH_SCRATCH = [
    pltpu.VMEM((16, 256, 128), F32),
    pltpu.VMEM((16, 256, 256), BF16),
    pltpu.VMEM((16, 256, 256), BF16),
    pltpu.SemaphoreType.DMA((4,)),
]


def _azimuth_rows(e_ref, g):
    at = [pl.multiple_of(c * 128 + g * 8, 8) for c in range(2)]
    v = [(e_ref[k, pl.ds(at[0], 8), :], e_ref[k, pl.ds(at[1], 8), :]) for k in range(16)]
    return dft16(v, 1)


def _slave_kernel(x_ref, ah_hbm, al_hbm, o_hbm, left_ref, right_ref, o_ref, e_ref, *scratch):
    _azimuth_front(x_ref, ah_hbm, al_hbm, e_ref, *scratch)
    low = lax.broadcasted_iota(jnp.int32, (8, 128), 1) < 64
    zero = jnp.zeros((ASH, 128), F32)
    for ref in (o_ref.at[0], o_ref.at[1], left_ref, right_ref):
        ref[0:ASH, :] = zero
        ref[ASH + LINES :, :] = zero

    def third(g, carry):
        v = _azimuth_rows(e_ref, g)
        for a in range(16):
            rows = pl.ds(pl.multiple_of(a * 128 + g * 8 + ASH, 8), 8)
            r, i = v[a]
            o_ref[0, rows, :] = r
            o_ref[1, rows, :] = i
            left_ref[rows, :] = jnp.where(low, r, pltpu.roll(i, 64, 1))
            right_ref[rows, :] = jnp.where(low, pltpu.roll(r, 64, 1), i)
        return carry

    lax.fori_loop(0, 16, third, 0)
    out = pltpu.make_async_copy(o_ref, o_hbm, scratch[-1].at[2])
    out.start()
    out.wait()


def slave_azimuth(x, ah, al):
    side = jax.ShapeDtypeStruct((LINES + 2 * ASH, 128), F32)
    return pl.pallas_call(
        _slave_kernel,
        out_shape=(jax.ShapeDtypeStruct((2, LINES + 2 * ASH, 128), F32), side, side),
        in_specs=[VMEM, HBM, HBM],
        out_specs=(HBM, VMEM, VMEM),
        scratch_shapes=[pltpu.VMEM((2, LINES + 2 * ASH, 128), F32)] + AZIMUTH_SCRATCH,
        compiler_params=limit(52),
        cost_estimate=pl.CostEstimate(flops=5 * 10**9, bytes_accessed=10**7, transcendentals=0),
        name="slave_azimuth",
    )(x.reshape(16, 8, 2, 16, 128), ah, al)


def _resample_kernel(az_ref, rg_ref, s_hbm, left_ref, right_ref, o_hbm, s_ref, o_ref, sem):
    lane = lax.broadcasted_iota(jnp.int32, (64, 128), 1)
    low = lane < 64

    def load(block):
        rows = pl.ds(0, BA + 2 * ASH) if block == 0 else pl.ds(block * BA + 2 * ASH, BA)
        return pltpu.make_async_copy(s_hbm.at[:, rows], s_ref.at[:, rows], sem.at[block])

    def store(block):
        rows = pl.ds(block * BA, BA)
        return pltpu.make_async_copy(o_ref.at[:, rows], o_hbm.at[:, rows], sem.at[4 + block])

    for block in range(NBA):
        load(block).start()
    for block in range(NBA):
        load(block).wait()

        def move(t, carry):
            parts = []
            for r, side_ref in ((0, left_ref), (1, right_ref)):
                shift = rg_ref[block, r]
                rows = pl.ds(block * BA + t * 64 + ASH + az_ref[block, r], 64)
                whole = lax.rem(256 - shift, 128)
                half = lax.rem(192 - shift, 128)
                near = lane + shift >= 0 if r == 0 else lane + shift < 128
                side = side_ref[rows, :]
                turns = (half, whole) if r == 0 else (whole, half)
                parts.append(
                    [
                        jnp.where(
                            near,
                            pltpu.roll(s_ref[c, rows, :], whole, 1),
                            pltpu.roll(side, turns[c], 1),
                        )
                        for c in range(2)
                    ]
                )
            rows = pl.ds(pl.multiple_of(block * BA + t * 64, 64), 64)
            for c in range(2):
                o_ref[c, rows, :] = jnp.where(low, parts[0][c], parts[1][c])
            return carry

        lax.fori_loop(0, BA // 64, move, 0, unroll=2)
        store(block).start()
    for block in range(NBA):
        store(block).wait()


def resample(az_shift, rg_shift, focused, left, right):
    return pl.pallas_call(
        _resample_kernel,
        in_specs=[SMEM, SMEM, HBM, VMEM, VMEM],
        out_specs=HBM,
        out_shape=jax.ShapeDtypeStruct((2, LINES, 128), F32),
        scratch_shapes=[
            pltpu.VMEM((2, LINES + 2 * ASH, 128), F32),
            pltpu.VMEM((2, LINES, 128), F32),
            pltpu.SemaphoreType.DMA((8,)),
        ],
        cost_estimate=pl.CostEstimate(flops=2 * 10**9, bytes_accessed=10**7, transcendentals=0),
        compiler_params=limit(61),
        name="resample",
    )(az_shift, rg_shift, focused, left, right)


def _master_kernel(x_ref, ah_hbm, al_hbm, m_hbm, n_ref, pick_ref, box_ref, side_ref, c_ref, m_ref, e_ref, *scratch):
    moved = pltpu.make_async_copy(m_hbm, m_ref, scratch[-1].at[2])
    moved.start()
    _azimuth_front(x_ref, ah_hbm, al_hbm, e_ref, *scratch)
    moved.wait()
    line = lax.broadcasted_iota(jnp.int32, (8, 128), 0)
    count = n_ref[...]

    def third(g, carry):
        v = _azimuth_rows(e_ref, g)
        for a in range(16):
            at = pl.multiple_of(a * 128 + g * 8, 8)
            r, i = v[a]
            sr, si = m_ref[0, pl.ds(at, 8), :], m_ref[1, pl.ds(at, 8), :]
            keep = line + at < count
            c_ref[pl.ds(at, 8), :] = jnp.where(keep, r * sr + i * si, 0.0)
            c_ref[pl.ds(at + LINES, 8), :] = jnp.where(keep, i * sr - r * si, 0.0)
        return carry

    lax.fori_loop(0, 16, third, 0)
    total = c_ref[pl.ds(0, 512, stride=LOOK), :]
    for j in range(1, LOOK):
        total = total + c_ref[pl.ds(j, 512, stride=LOOK), :]
    y = _dot_t(pick_ref[...], total)
    cell = lax.broadcasted_iota(jnp.int32, (24, 512), 1) % 256
    y = (
        y
        + jnp.where(cell == 0, 0.0, pltpu.roll(y, 1, 1))
        + jnp.where(cell == 255, 0.0, pltpu.roll(y, 511, 1))
    )
    box_ref[...] = y[:16]
    side_ref[...] = y[16:]


def master_looks(x, ah, al, moved, counts):
    return pl.pallas_call(
        _master_kernel,
        out_shape=(
            jax.ShapeDtypeStruct((16, 512), F32),
            jax.ShapeDtypeStruct((8, 512), F32),
        ),
        in_specs=[VMEM, HBM, HBM, HBM, VMEM, VMEM],
        compiler_params=limit(52),
        scratch_shapes=[pltpu.VMEM((2 * LINES, 128), F32), pltpu.VMEM((2, LINES, 128), F32)]
        + AZIMUTH_SCRATCH,
        cost_estimate=pl.CostEstimate(flops=5 * 10**9, bytes_accessed=10**7, transcendentals=0),
        name="master_looks",
    )(x.reshape(16, 8, 2, 16, 128), ah, al, moved, counts, TABLES["pick"])


def _final_kernel(box_ref, left_ref, right_ref, scale_ref, o_ref):
    row = lax.broadcasted_iota(jnp.int32, (16, 256), 0)
    for c in range(2):
        at = slice(256 * c, 256 * c + 256)
        x = box_ref[:, at]
        x = x + jnp.where(row == 0, left_ref[1:2, at], 0.0)
        x = x + jnp.where(row == 15, right_ref[0:1, at], 0.0)
        o_ref[c] = x * scale_ref[...]


def final(box, left, right, scale):
    return pl.pallas_call(
        _final_kernel,
        out_shape=jax.ShapeDtypeStruct((2, 16, 256), F32),
        compiler_params=limit(4),
        name="final",
    )(box, left, right, scale)


def to_worker(x):
    return lax.ppermute(x, ALL, [(b, worker(b)) for b in range(128)])


def halo(to_right, to_left):
    up = [(worker(b), worker(b + 1)) for b in range(127)]
    down = [(j, i) for i, j in up]
    return lax.ppermute(to_right, ALL, up), lax.ppermute(to_left, ALL, down)


def local(master_raw, slave_raw, range_ref, az_ref, az_shift, rg_shift, valid_lines):
    hf = range_ref.reshape(2, NS, NQ, NP).transpose(3, 2, 0, 1).reshape(NP * NQ, 2, NS)
    hf = jnp.pad(hf * (1.0 / RANGE), ((0, 0), (0, 0), (0, 3)))
    h = az_ref.reshape(2, 128, 16).transpose(2, 0, 1) * (1.0 / LINES)

    def columns_of(ranged):
        return lax.all_to_all(ranged, ALL, 0, 0, tiled=True)

    flat = lax.axis_index(ALL)
    counts = lax.dynamic_slice(jnp.pad(valid_lines, 1), (flat * 2,), (4,))
    wide = jnp.concatenate([counts[:1], jnp.repeat(counts[1:3], BR // LOOK), counts[3:]])
    rows = LINES // LOOK
    groups = lax.broadcasted_iota(jnp.int32, (18, rows + 2), 1) - 1
    pixels = jnp.clip(wide[:, None] - LOOK * groups, 0, LOOK) * LOOK
    pixels = jnp.where((groups >= 0) & (groups < rows), pixels, 0).astype(F32)
    box_pixels = sum(pixels[j : j + 16, i : i + rows] for i in range(3) for j in range(3))
    scale = 1.0 / jnp.sqrt(jnp.maximum(box_pixels, 1.0))
    core = lax.axis_index("az") % 2
    block = ((lax.axis_index("az") // 2) * 16 + lax.axis_index("rg")) * 2 + core
    own = lax.dynamic_slice(valid_lines, (block * 2,), (2,))
    col_counts = jnp.repeat(own, BR)[None, :]
    shifts = to_worker(jnp.stack([az_shift, rg_shift]))

    lines = lax.all_to_all(pre(slave_raw, master_raw), "rg", 0, 0, tiled=True)
    ah, al = prep(h)
    lines, ah, al, hf, shifts, scale, col_counts = lax.optimization_barrier(
        (lines, ah, al, hf, shifts, scale, col_counts)
    )
    slave = columns_of(range_compress(lines, 0, hf))
    master = columns_of(range_compress(lines, 1, hf))
    focused, to_left, to_right = slave_azimuth(slave, ah, al)
    from_left, from_right = halo(to_right, to_left)
    moved = resample(shifts[0], shifts[1], focused, from_left, from_right)

    box, side = master_looks(master, ah, al, moved, col_counts)
    box = lax.ppermute(box, ALL, [(worker(b), b) for b in range(128)])
    left = lax.ppermute(side, ALL, [(worker(b), b + 1) for b in range(127)])
    right = lax.ppermute(side, ALL, [(worker(b + 1), b) for b in range(127)])
    return final(box, left, right, scale).transpose(0, 2, 1)


def solution(mesh):
    return jax.shard_map(
        local,
        mesh=mesh,
        in_specs=(
            P(None, "az", "rg"),
            P(None, "az", "rg"),
            P(),
            P(),
            P(None, ALL),
            P(None, ALL),
            P(),
        ),
        out_specs=P(None, None, ALL),
        check_vma=False,
    )
```

```python
import math

import jax
import jax.numpy as jnp
import numpy as np
from jax import lax
from jax.experimental import pallas as pl
from jax.experimental.pallas import tpu as pltpu
from jax.sharding import PartitionSpec as P


LINES = 2048
RANGE = 20000
LOOK = 8
BA = 512
BR = 64
ASH = 32
NBA = 4
ALL = ("az", "rg")
NP = 16
NQ = 10
NS = 125
F32 = jnp.float32
BF16 = jnp.bfloat16


SHIFTS = sorted(
    ((dx, dz) for dx in range(4) for dz in range(4)),
    key=lambda s: -(min(s[0], 4 - s[0]) + min(s[1], 4 - s[1])),
)


def shifted(r, shift):
    return ((r // 4 + shift[1]) % 4) * 4 + (r % 4 + shift[0]) % 4


def _rot(v, angle):
    c, s = math.cos(angle), math.sin(angle)
    turns = angle / (math.pi / 4)
    eighth = round(turns)
    x, y = v
    if abs(turns - eighth) < 1e-9:
        e = eighth % 8
        if e == 0:
            return v
        if e == 2:
            return (-y, x)
        if e == 4:
            return (-x, -y)
        if e == 6:
            return (y, -x)
        h = math.sqrt(0.5)
        if e == 1:
            return ((x - y) * h, (x + y) * h)
        if e == 3:
            return (-(x + y) * h, (x - y) * h)
        if e == 5:
            return ((y - x) * h, -(x + y) * h)
        return ((x + y) * h, (y - x) * h)
    return (x * c - y * s, x * s + y * c)


def _add(a, b):
    return (a[0] + b[0], a[1] + b[1])


def _sub(a, b):
    return (a[0] - b[0], a[1] - b[1])


def _dft2(v, sign):
    return [_add(v[0], v[1]), _sub(v[0], v[1])]


def _dft4(v, sign):
    a, b = _add(v[0], v[2]), _sub(v[0], v[2])
    c, d = _add(v[1], v[3]), _sub(v[1], v[3])
    if sign < 0:
        return [_add(a, c), (b[0] + d[1], b[1] - d[0]), _sub(a, c), (b[0] - d[1], b[1] + d[0])]
    return [_add(a, c), (b[0] - d[1], b[1] + d[0]), _sub(a, c), (b[0] + d[1], b[1] - d[0])]


def _dft5(v, sign):
    c1, c2 = math.cos(2 * math.pi / 5), math.cos(4 * math.pi / 5)
    s1, s2 = sign * math.sin(2 * math.pi / 5), sign * math.sin(4 * math.pi / 5)
    a1, b1 = _add(v[1], v[4]), _sub(v[1], v[4])
    a2, b2 = _add(v[2], v[3]), _sub(v[2], v[3])
    x0 = v[0]
    y0 = (x0[0] + a1[0] + a2[0], x0[1] + a1[1] + a2[1])
    p1 = tuple(x0[i] + c1 * a1[i] + c2 * a2[i] for i in range(2))
    p2 = tuple(x0[i] + c2 * a1[i] + c1 * a2[i] for i in range(2))
    q1 = tuple(s1 * b1[i] + s2 * b2[i] for i in range(2))
    q2 = tuple(s2 * b1[i] - s1 * b2[i] for i in range(2))
    return [
        y0,
        (p1[0] - q1[1], p1[1] + q1[0]),
        (p2[0] - q2[1], p2[1] + q2[0]),
        (p2[0] + q2[1], p2[1] - q2[0]),
        (p1[0] + q1[1], p1[1] - q1[0]),
    ]


def _dft_two(v, n1, n2, first, second, sign):
    n = n1 * n2
    out = [None] * n
    mid = []
    for b in range(n2):
        col = first([v[n2 * a + b] for a in range(n1)], sign)
        mid.append([_rot(col[k], sign * 2 * math.pi * ((b * k) % n) / n) for k in range(n1)])
    for k1 in range(n1):
        row = second([mid[b][k1] for b in range(n2)], sign)
        for k2 in range(n2):
            out[k1 + n1 * k2] = row[k2]
    return out


def dft16(v, sign):
    return _dft_two(v, 4, 4, _dft4, _dft4, sign)


def dft10(v, sign):
    return _dft_two(v, 2, 5, _dft2, _dft5, sign)


def cmul(a, b):
    return (a[0] * b[0] - a[1] * b[1], a[0] * b[1] + a[1] * b[0])


def split(x):
    hi = x.astype(BF16)
    return hi, (x - hi.astype(F32)).astype(BF16)


def dot(a, b):
    return jnp.dot(a, b, preferred_element_type=F32)


def worker(block):
    chip, core = divmod(block, 2)
    y, rest = divmod(chip, 16)
    return (y * 2 + core) * 16 + rest


def _np_split(x):
    x = np.asarray(x, np.float32)
    hi = x.astype(BF16)
    return hi, (x - hi.astype(np.float32)).astype(BF16)


def _tables():
    t = {}
    two = 2 * np.pi
    q2 = np.arange(128)
    keep = (q2 < NS)[None, :]
    ang = -two * ((np.arange(NQ)[:, None] * q2[None, :]) % 1250) / 1250
    t["twb"] = np.stack([np.cos(ang) * keep, np.sin(ang) * keep], 1).astype(np.float32)
    n = np.arange(NQ)[None, :, None] * NS + q2[None, None, :]
    ang = two * ((np.arange(NP)[:, None, None] * n) % RANGE) / RANGE
    t["twc"] = np.stack([np.cos(ang), np.sin(ang)], 2).reshape(NP * NQ, 2, 128).astype(np.float32)
    ang = two * ((q2[:, None] * q2[None, :]) % NS) / NS
    both = keep & keep.T
    c, s = np.cos(ang) * both, np.sin(ang) * both
    t["fh"], t["fl"] = _np_split(np.block([[c, -s], [s, c]]))
    t["gh"], t["gl"] = _np_split(np.block([[c, s], [-s, c]]))
    k2 = np.arange(128)
    l2 = np.arange(128)
    ang = -two * ((l2[:, None] * k2[None, :]) % 128) / 128
    pr, pi = np.cos(ang), np.sin(ang)
    ang = np.broadcast_to(-two * l2[:, None] / LINES, (128, 128))
    wr, wi = np.cos(ang), np.sin(ang)
    t["p"] = np.stack([pr, pi]).astype(np.float32)
    t["w"] = np.stack([wr, wi]).astype(np.float32)
    kk = np.arange(256)
    part, line = (kk // 16) % 2, (kk // 32) * 16 + kk % 16
    sel = (part == 0)[:, None]
    t["q"] = np.stack(
        [np.where(sel, pr[line], -pi[line]), np.where(sel, -pi[line], -pr[line])]
    ).astype(np.float32)
    t["v"] = np.stack([wr[line], wi[line]]).astype(np.float32)
    lane = np.arange(128)
    pick = np.zeros((24, 128), np.float32)
    for o in range(16):
        pick[o] = np.abs(lane // LOOK - o) <= 1
    pick[16] = lane < LOOK
    pick[17] = lane >= 128 - LOOK
    t["pick"] = pick
    return t


TABLES = _tables()


HBM = pl.BlockSpec(memory_space=pltpu.HBM)
VMEM = pl.BlockSpec(memory_space=pltpu.VMEM)
SMEM = pl.BlockSpec(memory_space=pltpu.SMEM)


def limit(mib):
    return pltpu.CompilerParams(vmem_limit_bytes=mib << 20)


def _line_tile(x_ref, q, half, c):
    v = x_ref[pl.ds(500 * q + 2 * half + c, NS, stride=4), :]
    return jnp.concatenate([v, jnp.zeros((128 - NS, 128), F32)], axis=0).T


def _pre_kernel(x_ref, o_ref):
    for q in range(2):
        for half in range(2):
            for c in range(2):
                v = _line_tile(x_ref, q, half, c)
                for k in range(8):
                    o_ref[8 * half + k, q, c] = v[16 * k : 16 * k + 16]


def _pre_shift_kernel(me_ref, x_ref, *refs):
    outs, t_ref = refs[:-1], refs[-1]
    _pre_kernel(x_ref, t_ref)
    me = me_ref[0]
    for shift, o_ref in zip(SHIFTS, outs):
        o_ref[...] = t_ref[shifted(me, shift)]


def _raw_rows(raw):
    raw = raw.transpose(2, 0, 1).reshape(1250, 2, 2, 128)
    return raw.transpose(0, 2, 1, 3).reshape(5000, 128)


def pre(raw):
    return pl.pallas_call(
        _pre_kernel,
        grid=(5,),
        in_specs=[pl.BlockSpec((1000, 128), lambda i: (i, 0))],
        out_specs=pl.BlockSpec((NP, 2, 2, 16, 128), lambda i: (0, i, 0, 0, 0)),
        out_shape=jax.ShapeDtypeStruct((NP, NQ, 2, 16, 128), F32),
        cost_estimate=pl.CostEstimate(flops=10**8, bytes_accessed=10**7, transcendentals=0),
        name="pre",
    )(_raw_rows(raw))


def pre_shifts(me, raw):
    return pl.pallas_call(
        _pre_shift_kernel,
        grid=(5,),
        in_specs=[SMEM, pl.BlockSpec((1000, 128), lambda i: (i, 0))],
        out_specs=[pl.BlockSpec((2, 2, 16, 128), lambda i: (i, 0, 0, 0))] * NP,
        out_shape=[jax.ShapeDtypeStruct((NQ, 2, 16, 128), F32)] * NP,
        scratch_shapes=[pltpu.VMEM((NP, 2, 2, 16, 128), F32)],
        cost_estimate=pl.CostEstimate(flops=10**8, bytes_accessed=10**7, transcendentals=0),
        name="pre_shifts",
    )(me, _raw_rows(raw))


def _range_body(ready, twb_ref, hf_ref, fh_ref, fl_ref, gh_ref, gl_ref, twc_ref, o_hbm, d_ref, x_ref, o_ref, out_sem):
    lane = lax.broadcasted_iota(jnp.int32, (16, 128), 1)

    def outer(q, carry):
        ready(q)
        for g in range(2):
            rows = slice(8 * g, 8 * g + 8)
            v = [(x_ref[p, q, 0, rows, :], x_ref[p, q, 1, rows, :]) for p in range(NP)]
            v = dft16(v, -1)
            for k in range(NP):
                at = k * NQ + q
                r, i = cmul(v[k], (twc_ref[at, 0:1, :], -twc_ref[at, 1:2, :]))
                d_ref[at, 0, rows, :] = r
                d_ref[at, 1, rows, :] = i
        return carry

    lax.fori_loop(0, NQ, outer, 0)

    def middle(kp, carry):
        v = [(d_ref[kp * NQ + q, 0], d_ref[kp * NQ + q, 1]) for q in range(NQ)]
        v = dft10(v, -1)
        rows = []
        for k in range(NQ):
            r, i = cmul(v[k], (twb_ref[k, 0:1, :], twb_ref[k, 1:2, :]))
            rows.append(jnp.concatenate([r, i], axis=1))
        hi, lo = split(jnp.concatenate(rows, axis=0))
        y = dot(hi, fh_ref[...]) + dot(lo, fh_ref[...]) + dot(hi, fl_ref[...])
        rows = []
        for k in range(NQ):
            val = (y[16 * k : 16 * k + 16, :128], y[16 * k : 16 * k + 16, 128:])
            r, i = cmul(val, (hf_ref[kp * NQ + k, 0:1, :], hf_ref[kp * NQ + k, 1:2, :]))
            rows.append(jnp.concatenate([r, i], axis=1))
        hi, lo = split(jnp.concatenate(rows, axis=0))
        y = dot(hi, gh_ref[...]) + dot(lo, gh_ref[...]) + dot(hi, gl_ref[...])
        v = []
        for k in range(NQ):
            val = (y[16 * k : 16 * k + 16, :128], y[16 * k : 16 * k + 16, 128:])
            v.append(cmul(val, (twb_ref[k, 0:1, :], -twb_ref[k, 1:2, :])))
        v = dft10(v, 1)
        for q in range(NQ):
            at = kp * NQ + q
            r, i = cmul(v[q], (twc_ref[at, 0:1, :], twc_ref[at, 1:2, :]))
            d_ref[at, 0] = r
            d_ref[at, 1] = i
        return carry

    lax.fori_loop(0, NP, middle, 0, unroll=2)

    def inner(q, carry):
        for g in range(2):
            rows = slice(8 * g, 8 * g + 8)
            v = [(d_ref[k * NQ + q, 0, rows, :], d_ref[k * NQ + q, 1, rows, :]) for k in range(NP)]
            v = dft16(v, 1)
            for p in range(14):
                d_ref[p * NQ + q, 0, rows, :] = v[p][0]
                d_ref[p * NQ + q, 1, rows, :] = v[p][1]
        return carry

    lax.fori_loop(0, NQ, inner, 0)

    def store(part):
        at = pl.ds(32 * part, 32)
        return pltpu.make_async_copy(o_ref.at[at], o_hbm.at[at], out_sem.at[part])

    for d in range(128):
        n, a = divmod(128 * d, NS)
        for c in range(2):
            val = d_ref[n, c]
            if a:
                val = pltpu.roll(val, 128 - a, 1)
            start = NS - a
            while start < 128:
                n2 = (128 * d + start) // NS
                nxt = d_ref[n2, c]
                nxt = pltpu.roll(nxt, start % 128, 1)
                val = jnp.where(lane < start, val, nxt)
                start += NS
            o_ref[worker(d), c] = val
        if d % 32 == 31:
            store(d // 32).start()
    for part in range(4):
        store(part).wait()


def _range_kernel(x_hbm, *refs):
    in_sem, x_ref = refs[-1], refs[-4]

    def load(q):
        return pltpu.make_async_copy(x_hbm.at[:, q], x_ref.at[:, q], in_sem.at[q])

    for q in range(NQ):
        load(q).start()
    _range_body(lambda q: load(q).wait(), *refs[:-1])


def _range_shift_kernel(me_ref, *refs):
    parts, refs = refs[:NP], refs[NP:]
    in_sem, x_ref = refs[-1], refs[-4]
    me = me_ref[0]
    loads = [
        pltpu.make_async_copy(
            part, x_ref.at[shifted(me, (4 - shift[0], 4 - shift[1]))], in_sem.at[k]
        )
        for k, (shift, part) in enumerate(zip(SHIFTS, parts))
    ]
    for load in loads:
        load.start()
    for load in loads:
        load.wait()
    _range_body(lambda q: None, *refs[:-1])


def range_compress(kernel, specs, operands, hf):
    t = TABLES
    return pl.pallas_call(
        kernel,
        in_specs=specs + [VMEM] * 7,
        out_specs=HBM,
        out_shape=jax.ShapeDtypeStruct((128, 2, 16, 128), F32),
        scratch_shapes=[
            pltpu.VMEM((NP * NQ, 2, 16, 128), F32),
            pltpu.VMEM((NP, NQ, 2, 16, 128), F32),
            pltpu.VMEM((128, 2, 16, 128), F32),
            pltpu.SemaphoreType.DMA((4,)),
            pltpu.SemaphoreType.DMA((NP,)),
        ],
        cost_estimate=pl.CostEstimate(flops=10**10, bytes_accessed=6 * 10**6, transcendentals=0),
    )(*operands, t["twb"], hf, t["fh"], t["fl"], t["gh"], t["gl"], t["twc"])


def _dot_t(a, b):
    return lax.dot_general(
        a, b, (((1,), (1,)), ((), ())), precision=lax.Precision.HIGHEST, preferred_element_type=F32
    )


def _prep_kernel(h_ref, p0_ref, w_ref, q0_ref, v_ref, ah_ref, al_ref, p_ref, q_ref):
    p_ref[...] = p0_ref[...]
    q_ref[...] = q0_ref[...]

    def body(k, carry):
        pr, pi = p_ref[0], p_ref[1]
        q1, q2 = q_ref[0], q_ref[1]
        hr, hi = h_ref[k, 0:1, :], h_ref[k, 1:2, :]
        vr, vi = cmul((pr, -pi), (hr, hi))
        top = _dot_t(vr, q1) + _dot_t(vi, q2)
        bottom = _dot_t(vi, q1) - _dot_t(vr, q2)
        high, low = split(top)
        ah_ref[k, 0:128, :] = high
        al_ref[k, 0:128, :] = low
        high, low = split(bottom)
        ah_ref[k, 128:256, :] = high
        al_ref[k, 128:256, :] = low
        pr, pi = cmul((pr, pi), (w_ref[0], w_ref[1]))
        p_ref[0] = pr
        p_ref[1] = pi
        wr, wi = v_ref[0], v_ref[1]
        q_ref[0] = q1 * wr + q2 * wi
        q_ref[1] = q2 * wr - q1 * wi
        return carry

    lax.fori_loop(0, 16, body, 0)


def prep(h):
    t = TABLES
    shape = jax.ShapeDtypeStruct((16, 256, 256), BF16)
    return pl.pallas_call(
        _prep_kernel,
        out_shape=(shape, shape),
        scratch_shapes=[pltpu.VMEM((2, 128, 128), F32), pltpu.VMEM((2, 256, 128), F32)],
        cost_estimate=pl.CostEstimate(flops=5 * 10**9, bytes_accessed=5 * 10**6, transcendentals=0),
        name="prep",
    )(h, t["p"], t["w"], t["q"], t["v"])


def _azimuth_front(x_ref, ah_hbm, al_hbm, e_ref, ah_ref, al_ref, sem):
    matrices = [
        pltpu.make_async_copy(ah_hbm, ah_ref, sem.at[0]),
        pltpu.make_async_copy(al_hbm, al_ref, sem.at[1]),
    ]
    for copy in matrices:
        copy.start()

    def first(s, carry):
        for g in range(2):
            rows = slice(8 * g, 8 * g + 8)
            v = [(x_ref[a, s, 0, rows, :], x_ref[a, s, 1, rows, :]) for a in range(16)]
            v = dft16(v, -1)
            for k in range(16):
                for c in range(2):
                    at = pl.multiple_of(s * 32 + c * 16 + g * 8, 8)
                    e_ref[k, pl.ds(at, 8), :] = v[k][c]
        return carry

    lax.fori_loop(0, 8, first, 0)
    for copy in matrices:
        copy.wait()

    def second(k, carry):
        hi, lo = split(e_ref[k])
        wide = dot(ah_ref[k], jnp.concatenate([hi, lo], axis=1))
        e_ref[k] = wide[:, :128] + wide[:, 128:] + dot(al_ref[k], hi)
        return carry

    lax.fori_loop(0, 16, second, 0, unroll=4)


AZIMUTH_SCRATCH = [
    pltpu.VMEM((16, 256, 128), F32),
    pltpu.VMEM((16, 256, 256), BF16),
    pltpu.VMEM((16, 256, 256), BF16),
    pltpu.SemaphoreType.DMA((4,)),
]


def _azimuth_rows(e_ref, g):
    at = [pl.multiple_of(c * 128 + g * 8, 8) for c in range(2)]
    v = [(e_ref[k, pl.ds(at[0], 8), :], e_ref[k, pl.ds(at[1], 8), :]) for k in range(16)]
    return dft16(v, 1)


def _slave_kernel(x_ref, ah_hbm, al_hbm, o_hbm, left_ref, right_ref, o_ref, e_ref, *scratch):
    _azimuth_front(x_ref, ah_hbm, al_hbm, e_ref, *scratch)
    low = lax.broadcasted_iota(jnp.int32, (8, 128), 1) < 64
    zero = jnp.zeros((ASH, 128), F32)
    for ref in (o_ref.at[0], o_ref.at[1], left_ref, right_ref):
        ref[0:ASH, :] = zero
        ref[ASH + LINES :, :] = zero

    def third(g, carry):
        v = _azimuth_rows(e_ref, g)
        for a in range(16):
            rows = pl.ds(pl.multiple_of(a * 128 + g * 8 + ASH, 8), 8)
            r, i = v[a]
            o_ref[0, rows, :] = r
            o_ref[1, rows, :] = i
            left_ref[rows, :] = jnp.where(low, r, pltpu.roll(i, 64, 1))
            right_ref[rows, :] = jnp.where(low, pltpu.roll(r, 64, 1), i)
        return carry

    lax.fori_loop(0, 16, third, 0)
    out = pltpu.make_async_copy(o_ref, o_hbm, scratch[-1].at[2])
    out.start()
    out.wait()


def slave_azimuth(x, ah, al):
    side = jax.ShapeDtypeStruct((LINES + 2 * ASH, 128), F32)
    return pl.pallas_call(
        _slave_kernel,
        out_shape=(jax.ShapeDtypeStruct((2, LINES + 2 * ASH, 128), F32), side, side),
        in_specs=[VMEM, HBM, HBM],
        out_specs=(HBM, VMEM, VMEM),
        scratch_shapes=[pltpu.VMEM((2, LINES + 2 * ASH, 128), F32)] + AZIMUTH_SCRATCH,
        compiler_params=limit(52),
        cost_estimate=pl.CostEstimate(flops=5 * 10**9, bytes_accessed=10**7, transcendentals=0),
        name="slave_azimuth",
    )(x.reshape(16, 8, 2, 16, 128), ah, al)


def _resample_kernel(az_ref, rg_ref, s_hbm, left_ref, right_ref, o_hbm, s_ref, o_ref, sem):
    lane = lax.broadcasted_iota(jnp.int32, (64, 128), 1)
    low = lane < 64

    def load(block):
        rows = pl.ds(0, BA + 2 * ASH) if block == 0 else pl.ds(block * BA + 2 * ASH, BA)
        return pltpu.make_async_copy(s_hbm.at[:, rows], s_ref.at[:, rows], sem.at[block])

    def store(block):
        rows = pl.ds(block * BA, BA)
        return pltpu.make_async_copy(o_ref.at[:, rows], o_hbm.at[:, rows], sem.at[4 + block])

    for block in range(NBA):
        load(block).start()
    for block in range(NBA):
        load(block).wait()

        def move(t, carry):
            parts = []
            for r, side_ref in ((0, left_ref), (1, right_ref)):
                shift = rg_ref[block, r]
                rows = pl.ds(block * BA + t * 64 + ASH + az_ref[block, r], 64)
                whole = lax.rem(256 - shift, 128)
                half = lax.rem(192 - shift, 128)
                near = lane + shift >= 0 if r == 0 else lane + shift < 128
                side = side_ref[rows, :]
                turns = (half, whole) if r == 0 else (whole, half)
                parts.append(
                    [
                        jnp.where(
                            near,
                            pltpu.roll(s_ref[c, rows, :], whole, 1),
                            pltpu.roll(side, turns[c], 1),
                        )
                        for c in range(2)
                    ]
                )
            rows = pl.ds(pl.multiple_of(block * BA + t * 64, 64), 64)
            for c in range(2):
                o_ref[c, rows, :] = jnp.where(low, parts[0][c], parts[1][c])
            return carry

        lax.fori_loop(0, BA // 64, move, 0, unroll=2)
        store(block).start()
    for block in range(NBA):
        store(block).wait()


def resample(az_shift, rg_shift, focused, left, right):
    return pl.pallas_call(
        _resample_kernel,
        in_specs=[SMEM, SMEM, HBM, VMEM, VMEM],
        out_specs=HBM,
        out_shape=jax.ShapeDtypeStruct((2, LINES, 128), F32),
        scratch_shapes=[
            pltpu.VMEM((2, LINES + 2 * ASH, 128), F32),
            pltpu.VMEM((2, LINES, 128), F32),
            pltpu.SemaphoreType.DMA((8,)),
        ],
        cost_estimate=pl.CostEstimate(flops=2 * 10**9, bytes_accessed=10**7, transcendentals=0),
        compiler_params=limit(61),
        name="resample",
    )(az_shift, rg_shift, focused, left, right)


def _master_kernel(x_ref, ah_hbm, al_hbm, m_hbm, n_ref, pick_ref, box_ref, side_ref, c_ref, m_ref, e_ref, *scratch):
    moved = pltpu.make_async_copy(m_hbm, m_ref, scratch[-1].at[2])
    moved.start()
    _azimuth_front(x_ref, ah_hbm, al_hbm, e_ref, *scratch)
    moved.wait()
    line = lax.broadcasted_iota(jnp.int32, (8, 128), 0)
    count = n_ref[...]

    def third(g, carry):
        v = _azimuth_rows(e_ref, g)
        for a in range(16):
            at = pl.multiple_of(a * 128 + g * 8, 8)
            r, i = v[a]
            sr, si = m_ref[0, pl.ds(at, 8), :], m_ref[1, pl.ds(at, 8), :]
            keep = line + at < count
            c_ref[pl.ds(at, 8), :] = jnp.where(keep, r * sr + i * si, 0.0)
            c_ref[pl.ds(at + LINES, 8), :] = jnp.where(keep, i * sr - r * si, 0.0)
        return carry

    lax.fori_loop(0, 16, third, 0)
    total = c_ref[pl.ds(0, 512, stride=LOOK), :]
    for j in range(1, LOOK):
        total = total + c_ref[pl.ds(j, 512, stride=LOOK), :]
    y = _dot_t(pick_ref[...], total)
    cell = lax.broadcasted_iota(jnp.int32, (24, 512), 1) % 256
    y = (
        y
        + jnp.where(cell == 0, 0.0, pltpu.roll(y, 1, 1))
        + jnp.where(cell == 255, 0.0, pltpu.roll(y, 511, 1))
    )
    box_ref[...] = y[:16]
    side_ref[...] = y[16:]


def master_looks(x, ah, al, moved, counts):
    return pl.pallas_call(
        _master_kernel,
        out_shape=(
            jax.ShapeDtypeStruct((16, 512), F32),
            jax.ShapeDtypeStruct((8, 512), F32),
        ),
        in_specs=[VMEM, HBM, HBM, HBM, VMEM, VMEM],
        compiler_params=limit(52),
        scratch_shapes=[pltpu.VMEM((2 * LINES, 128), F32), pltpu.VMEM((2, LINES, 128), F32)]
        + AZIMUTH_SCRATCH,
        cost_estimate=pl.CostEstimate(flops=5 * 10**9, bytes_accessed=10**7, transcendentals=0),
        name="master_looks",
    )(x.reshape(16, 8, 2, 16, 128), ah, al, moved, counts, TABLES["pick"])


def _final_kernel(box_ref, left_ref, right_ref, scale_ref, o_ref):
    row = lax.broadcasted_iota(jnp.int32, (16, 256), 0)
    for c in range(2):
        at = slice(256 * c, 256 * c + 256)
        x = box_ref[:, at]
        x = x + jnp.where(row == 0, left_ref[1:2, at], 0.0)
        x = x + jnp.where(row == 15, right_ref[0:1, at], 0.0)
        o_ref[c] = x * scale_ref[...]


def final(box, left, right, scale):
    return pl.pallas_call(
        _final_kernel,
        out_shape=jax.ShapeDtypeStruct((2, 16, 256), F32),
        compiler_params=limit(4),
        name="final",
    )(box, left, right, scale)


def to_worker(x):
    return lax.ppermute(x, ALL, [(b, worker(b)) for b in range(128)])


def halo(to_right, to_left):
    up = [(worker(b), worker(b + 1)) for b in range(127)]
    down = [(j, i) for i, j in up]
    return lax.ppermute(to_right, ALL, up), lax.ppermute(to_left, ALL, down)


def local(master_raw, slave_raw, range_ref, az_ref, az_shift, rg_shift, valid_lines):
    hf = range_ref.reshape(2, NS, NQ, NP).transpose(3, 2, 0, 1).reshape(NP * NQ, 2, NS)
    hf = jnp.pad(hf * (1.0 / RANGE), ((0, 0), (0, 0), (0, 3)))
    h = az_ref.reshape(2, 128, 16).transpose(2, 0, 1) * (1.0 / LINES)

    def columns_of(ranged):
        return lax.all_to_all(ranged, ALL, 0, 0, tiled=True)

    flat = lax.axis_index(ALL)
    counts = lax.dynamic_slice(jnp.pad(valid_lines, 1), (flat * 2,), (4,))
    wide = jnp.concatenate([counts[:1], jnp.repeat(counts[1:3], BR // LOOK), counts[3:]])
    rows = LINES // LOOK
    groups = lax.broadcasted_iota(jnp.int32, (18, rows + 2), 1) - 1
    pixels = jnp.clip(wide[:, None] - LOOK * groups, 0, LOOK) * LOOK
    pixels = jnp.where((groups >= 0) & (groups < rows), pixels, 0).astype(F32)
    box_pixels = sum(pixels[j : j + 16, i : i + rows] for i in range(3) for j in range(3))
    scale = 1.0 / jnp.sqrt(jnp.maximum(box_pixels, 1.0))
    core = lax.axis_index("az") % 2
    block = ((lax.axis_index("az") // 2) * 16 + lax.axis_index("rg")) * 2 + core
    own = lax.dynamic_slice(valid_lines, (block * 2,), (2,))
    col_counts = jnp.repeat(own, BR)[None, :]
    shifts = to_worker(jnp.stack([az_shift, rg_shift]))

    slave = pre(slave_raw)
    slave = lax.all_to_all(slave, "rg", 0, 0, tiled=True)
    me = lax.axis_index("rg").astype(jnp.int32)[None]
    pieces = pre_shifts(me, master_raw)
    master = [
        lax.ppermute(piece, "rg", [(r, shifted(r, shift)) for r in range(NP)])
        if any(shift)
        else piece
        for shift, piece in zip(SHIFTS, pieces)
    ]
    slave, hf, scale, col_counts = lax.optimization_barrier((slave, hf, scale, col_counts))
    slave = range_compress(_range_kernel, [HBM], [slave], hf)
    slave = columns_of(slave)
    ah, al = prep(h)
    master = range_compress(_range_shift_kernel, [SMEM] + [HBM] * NP, [me, *master], hf)
    master = columns_of(master)
    focused, to_left, to_right = slave_azimuth(slave, ah, al)
    from_left, from_right = halo(to_right, to_left)
    moved = resample(shifts[0], shifts[1], focused, from_left, from_right)

    box, side = master_looks(master, ah, al, moved, col_counts)
    box = lax.ppermute(box, ALL, [(worker(b), b) for b in range(128)])
    left = lax.ppermute(side, ALL, [(worker(b), b + 1) for b in range(127)])
    right = lax.ppermute(side, ALL, [(worker(b + 1), b) for b in range(127)])
    return final(box, left, right, scale).transpose(0, 2, 1)


def solution(mesh):
    return jax.shard_map(
        local,
        mesh=mesh,
        in_specs=(
            P(None, "az", "rg"),
            P(None, "az", "rg"),
            P(),
            P(),
            P(None, ALL),
            P(None, ALL),
            P(),
        ),
        out_specs=P(None, None, ALL),
        check_vma=False,
    )
```

```python
import math

import jax
import jax.numpy as jnp
import numpy as np
from jax import lax
from jax.experimental import pallas as pl
from jax.experimental.pallas import tpu as pltpu
from jax.sharding import PartitionSpec as P


LINES = 2048
RANGE = 20000
LOOK = 8
BA = 512
BR = 64
ASH = 32
NBA = 4
ALL = ("az", "rg")
NP = 16
NQ = 10
NS = 125
F32 = jnp.float32
BF16 = jnp.bfloat16


SHIFTS = sorted(
    ((dx, dz) for dx in range(4) for dz in range(4)),
    key=lambda s: -(min(s[0], 4 - s[0]) + min(s[1], 4 - s[1])),
)


def shifted(r, shift):
    return ((r // 4 + shift[1]) % 4) * 4 + (r % 4 + shift[0]) % 4


def _rot(v, angle):
    c, s = math.cos(angle), math.sin(angle)
    turns = angle / (math.pi / 4)
    eighth = round(turns)
    x, y = v
    if abs(turns - eighth) < 1e-9:
        e = eighth % 8
        if e == 0:
            return v
        if e == 2:
            return (-y, x)
        if e == 4:
            return (-x, -y)
        if e == 6:
            return (y, -x)
        h = math.sqrt(0.5)
        if e == 1:
            return ((x - y) * h, (x + y) * h)
        if e == 3:
            return (-(x + y) * h, (x - y) * h)
        if e == 5:
            return ((y - x) * h, -(x + y) * h)
        return ((x + y) * h, (y - x) * h)
    return (x * c - y * s, x * s + y * c)


def _add(a, b):
    return (a[0] + b[0], a[1] + b[1])


def _sub(a, b):
    return (a[0] - b[0], a[1] - b[1])


def _dft2(v, sign):
    return [_add(v[0], v[1]), _sub(v[0], v[1])]


def _dft4(v, sign):
    a, b = _add(v[0], v[2]), _sub(v[0], v[2])
    c, d = _add(v[1], v[3]), _sub(v[1], v[3])
    if sign < 0:
        return [_add(a, c), (b[0] + d[1], b[1] - d[0]), _sub(a, c), (b[0] - d[1], b[1] + d[0])]
    return [_add(a, c), (b[0] - d[1], b[1] + d[0]), _sub(a, c), (b[0] + d[1], b[1] - d[0])]


def _dft5(v, sign):
    c1, c2 = math.cos(2 * math.pi / 5), math.cos(4 * math.pi / 5)
    s1, s2 = sign * math.sin(2 * math.pi / 5), sign * math.sin(4 * math.pi / 5)
    a1, b1 = _add(v[1], v[4]), _sub(v[1], v[4])
    a2, b2 = _add(v[2], v[3]), _sub(v[2], v[3])
    x0 = v[0]
    y0 = (x0[0] + a1[0] + a2[0], x0[1] + a1[1] + a2[1])
    p1 = tuple(x0[i] + c1 * a1[i] + c2 * a2[i] for i in range(2))
    p2 = tuple(x0[i] + c2 * a1[i] + c1 * a2[i] for i in range(2))
    q1 = tuple(s1 * b1[i] + s2 * b2[i] for i in range(2))
    q2 = tuple(s2 * b1[i] - s1 * b2[i] for i in range(2))
    return [
        y0,
        (p1[0] - q1[1], p1[1] + q1[0]),
        (p2[0] - q2[1], p2[1] + q2[0]),
        (p2[0] + q2[1], p2[1] - q2[0]),
        (p1[0] + q1[1], p1[1] - q1[0]),
    ]


def _dft_two(v, n1, n2, first, second, sign):
    n = n1 * n2
    out = [None] * n
    mid = []
    for b in range(n2):
        col = first([v[n2 * a + b] for a in range(n1)], sign)
        mid.append([_rot(col[k], sign * 2 * math.pi * ((b * k) % n) / n) for k in range(n1)])
    for k1 in range(n1):
        row = second([mid[b][k1] for b in range(n2)], sign)
        for k2 in range(n2):
            out[k1 + n1 * k2] = row[k2]
    return out


def dft16(v, sign):
    return _dft_two(v, 4, 4, _dft4, _dft4, sign)


def dft10(v, sign):
    return _dft_two(v, 2, 5, _dft2, _dft5, sign)


def cmul(a, b):
    return (a[0] * b[0] - a[1] * b[1], a[0] * b[1] + a[1] * b[0])


def split(x):
    hi = x.astype(BF16)
    return hi, (x - hi.astype(F32)).astype(BF16)


def dot(a, b):
    return jnp.dot(a, b, preferred_element_type=F32)


def worker(block):
    chip, core = divmod(block, 2)
    y, rest = divmod(chip, 16)
    return (y * 2 + core) * 16 + rest


def _np_split(x):
    x = np.asarray(x, np.float32)
    hi = x.astype(BF16)
    return hi, (x - hi.astype(np.float32)).astype(BF16)


def _tables():
    t = {}
    two = 2 * np.pi
    q2 = np.arange(128)
    keep = (q2 < NS)[None, :]
    ang = -two * ((np.arange(NQ)[:, None] * q2[None, :]) % 1250) / 1250
    t["twb"] = np.stack([np.cos(ang) * keep, np.sin(ang) * keep], 1).astype(np.float32)
    n = np.arange(NQ)[None, :, None] * NS + q2[None, None, :]
    ang = two * ((np.arange(NP)[:, None, None] * n) % RANGE) / RANGE
    t["twc"] = np.stack([np.cos(ang), np.sin(ang)], 2).reshape(NP * NQ, 2, 128).astype(np.float32)
    ang = two * ((q2[:, None] * q2[None, :]) % NS) / NS
    both = keep & keep.T
    c, s = np.cos(ang) * both, np.sin(ang) * both
    t["fh"], t["fl"] = _np_split(np.block([[c, -s], [s, c]]))
    t["gh"], t["gl"] = _np_split(np.block([[c, s], [-s, c]]))
    k2 = np.arange(128)
    back = (-np.arange(128)) % 128
    ang = two * ((k2[:, None] * back[None, :]) % 128) / 128
    t["dft"] = np.stack([np.cos(ang), np.sin(ang)]).astype(np.float32)
    ang = two * (np.arange(16)[:, None] * back[None, :]) / LINES
    t["turn"] = np.stack([np.cos(ang), np.sin(ang)]).astype(np.float32)
    ang = np.broadcast_to(-two * np.arange(16)[:, None] / 16, (16, 128))
    t["wrap"] = np.stack([np.cos(ang), np.sin(ang)], 1).astype(np.float32)
    lane = np.arange(128)
    pick = np.zeros((24, 128), np.float32)
    for o in range(16):
        pick[o] = np.abs(lane // LOOK - o) <= 1
    pick[16] = lane < LOOK
    pick[17] = lane >= 128 - LOOK
    t["pick"] = pick
    return t


TABLES = _tables()


HBM = pl.BlockSpec(memory_space=pltpu.HBM)
VMEM = pl.BlockSpec(memory_space=pltpu.VMEM)
SMEM = pl.BlockSpec(memory_space=pltpu.SMEM)


def limit(mib):
    return pltpu.CompilerParams(vmem_limit_bytes=mib << 20)


def _raw_rows(raw):
    raw = raw.transpose(2, 0, 1).reshape(1250, 2, 2, 128)
    return raw.transpose(0, 2, 1, 3).reshape(5000, 128)


def _read_lines(x_hbm, x_ref, t_ref, sem, done):
    def load(q):
        rows = pl.ds(1000 * q, 1000)
        return pltpu.make_async_copy(x_hbm.at[rows], x_ref.at[rows], sem.at[q])

    for q in range(5):
        load(q).start()
    for q in range(NQ):
        if q % 2 == 0:
            load(q // 2).wait()
        for half in range(2):
            for c in range(2):
                v = x_ref[pl.ds(500 * q + 2 * half + c, NS, stride=4), :]
                v = jnp.concatenate([v, jnp.zeros((128 - NS, 128), F32)], axis=0).T
                for k in range(8):
                    t_ref[8 * half + k, q, c] = v[16 * k : 16 * k + 16]
        done(q)


def _pre_kernel(x_hbm, o_hbm, x_ref, t_ref, sem):
    def store(q):
        at = pl.ds(2 * (q // 2), 2)
        return pltpu.make_async_copy(t_ref.at[:, at], o_hbm.at[:, at], sem.at[5 + q // 2])

    _read_lines(x_hbm, x_ref, t_ref, sem, lambda q: store(q).start() if q % 2 else None)
    for q in range(0, NQ, 2):
        store(q).wait()


def _pre_shift_kernel(me_ref, x_hbm, *refs):
    outs, (x_ref, t_ref, sem) = refs[:NP], refs[NP:]
    _read_lines(x_hbm, x_ref, t_ref, sem, lambda q: None)
    me = me_ref[0]
    stores = [
        pltpu.make_async_copy(t_ref.at[shifted(me, shift)], o_hbm, sem.at[5 + k])
        for k, (shift, o_hbm) in enumerate(zip(SHIFTS, outs))
    ]
    for store in stores:
        store.start()
    for store in stores:
        store.wait()


PRE_SCRATCH = [
    pltpu.VMEM((5000, 128), F32),
    pltpu.VMEM((NP, NQ, 2, 16, 128), F32),
    pltpu.SemaphoreType.DMA((5 + NP,)),
]


def pre(raw):
    return pl.pallas_call(
        _pre_kernel,
        in_specs=[HBM],
        out_specs=HBM,
        out_shape=jax.ShapeDtypeStruct((NP, NQ, 2, 16, 128), F32),
        scratch_shapes=PRE_SCRATCH,
        cost_estimate=pl.CostEstimate(flops=10**8, bytes_accessed=10**7, transcendentals=0),
        name="pre",
    )(_raw_rows(raw))


def pre_shifts(me, raw):
    return pl.pallas_call(
        _pre_shift_kernel,
        in_specs=[SMEM, HBM],
        out_specs=[HBM] * NP,
        out_shape=[jax.ShapeDtypeStruct((NQ, 2, 16, 128), F32)] * NP,
        scratch_shapes=PRE_SCRATCH,
        cost_estimate=pl.CostEstimate(flops=10**8, bytes_accessed=10**7, transcendentals=0),
        name="pre_shifts",
    )(me, _raw_rows(raw))


def _range_body(ready, tables, o_hbm, d_ref, x_ref, o_ref, out_sem):
    twb_ref, hf_ref, fh_ref, fl_ref, gh_ref, gl_ref, twc_ref = tables
    lane = lax.broadcasted_iota(jnp.int32, (16, 128), 1)

    def outer(q, carry):
        ready(q)
        for g in range(2):
            rows = slice(8 * g, 8 * g + 8)
            v = [(x_ref[p, q, 0, rows, :], x_ref[p, q, 1, rows, :]) for p in range(NP)]
            v = dft16(v, -1)
            for k in range(NP):
                at = k * NQ + q
                r, i = cmul(v[k], (twc_ref[at, 0:1, :], -twc_ref[at, 1:2, :]))
                d_ref[at, 0, rows, :] = r
                d_ref[at, 1, rows, :] = i
        return carry

    lax.fori_loop(0, NQ, outer, 0)
    ready(None)

    def middle(kp, carry):
        v = [(d_ref[kp * NQ + q, 0], d_ref[kp * NQ + q, 1]) for q in range(NQ)]
        v = dft10(v, -1)
        rows = []
        for k in range(NQ):
            r, i = cmul(v[k], (twb_ref[k, 0:1, :], twb_ref[k, 1:2, :]))
            rows.append(jnp.concatenate([r, i], axis=1))
        hi, lo = split(jnp.concatenate(rows, axis=0))
        y = dot(hi, fh_ref[...]) + dot(lo, fh_ref[...]) + dot(hi, fl_ref[...])
        rows = []
        for k in range(NQ):
            val = (y[16 * k : 16 * k + 16, :128], y[16 * k : 16 * k + 16, 128:])
            r, i = cmul(val, (hf_ref[kp * NQ + k, 0:1, :], hf_ref[kp * NQ + k, 1:2, :]))
            rows.append(jnp.concatenate([r, i], axis=1))
        hi, lo = split(jnp.concatenate(rows, axis=0))
        y = dot(hi, gh_ref[...]) + dot(lo, gh_ref[...]) + dot(hi, gl_ref[...])
        v = []
        for k in range(NQ):
            val = (y[16 * k : 16 * k + 16, :128], y[16 * k : 16 * k + 16, 128:])
            v.append(cmul(val, (twb_ref[k, 0:1, :], -twb_ref[k, 1:2, :])))
        v = dft10(v, 1)
        for q in range(NQ):
            at = kp * NQ + q
            r, i = cmul(v[q], (twc_ref[at, 0:1, :], twc_ref[at, 1:2, :]))
            d_ref[at, 0] = r
            d_ref[at, 1] = i
        return carry

    lax.fori_loop(0, NP, middle, 0, unroll=2)

    def inner(q, carry):
        for g in range(2):
            rows = slice(8 * g, 8 * g + 8)
            v = [(d_ref[k * NQ + q, 0, rows, :], d_ref[k * NQ + q, 1, rows, :]) for k in range(NP)]
            v = dft16(v, 1)
            for p in range(14):
                d_ref[p * NQ + q, 0, rows, :] = v[p][0]
                d_ref[p * NQ + q, 1, rows, :] = v[p][1]
        return carry

    lax.fori_loop(0, NQ, inner, 0)

    def store(part):
        at = pl.ds(32 * part, 32)
        return pltpu.make_async_copy(o_ref.at[at], o_hbm.at[at], out_sem.at[part])

    for d in range(128):
        n, a = divmod(128 * d, NS)
        for c in range(2):
            val = d_ref[n, c]
            if a:
                val = pltpu.roll(val, 128 - a, 1)
            start = NS - a
            while start < 128:
                n2 = (128 * d + start) // NS
                nxt = d_ref[n2, c]
                nxt = pltpu.roll(nxt, start % 128, 1)
                val = jnp.where(lane < start, val, nxt)
                start += NS
            o_ref[worker(d), c] = val
        if d % 32 == 31:
            store(d // 32).start()
    for part in range(4):
        store(part).wait()


def _tables_in(table_hbm, tables, sem):
    copies = [
        pltpu.make_async_copy(src, dst, sem.at[k]) for k, (src, dst) in enumerate(zip(table_hbm, tables))
    ]
    for copy in copies[::-1]:
        copy.start()
    return copies


def _range_kernel(x_hbm, *refs):
    table_hbm, o_hbm, tables, (d_ref, x_ref, o_ref, out_sem, in_sem, sem) = refs[:7], refs[7], refs[8:15], refs[15:]

    def load(q):
        return pltpu.make_async_copy(x_hbm.at[:, q], x_ref.at[:, q], in_sem.at[q])

    def ready(q):
        if q is None:
            for copy in copies[:6]:
                copy.wait()
        else:
            load(q).wait()

    copies = _tables_in(table_hbm, tables, sem)
    for q in range(NQ):
        load(q).start()
    copies[6].wait()
    _range_body(ready, tables, o_hbm, d_ref, x_ref, o_ref, out_sem)


def _range_shift_kernel(me_ref, *refs):
    parts, refs = refs[:NP], refs[NP:]
    table_hbm, o_hbm, tables, (d_ref, x_ref, o_ref, out_sem, in_sem, sem) = refs[:7], refs[7], refs[8:15], refs[15:]
    me = me_ref[0]
    loads = [
        pltpu.make_async_copy(
            part, x_ref.at[shifted(me, (4 - shift[0], 4 - shift[1]))], in_sem.at[k]
        )
        for k, (shift, part) in enumerate(zip(SHIFTS, parts))
    ]

    def ready(q):
        if q is None:
            for copy in copies[:6]:
                copy.wait()

    copies = _tables_in(table_hbm, tables, sem)
    for load in loads:
        load.start()
    for load in loads:
        load.wait()
    copies[6].wait()
    _range_body(ready, tables, o_hbm, d_ref, x_ref, o_ref, out_sem)


def range_compress(kernel, specs, operands, hf):
    t = TABLES
    tables = (t["twb"], hf, t["fh"], t["fl"], t["gh"], t["gl"], t["twc"])
    return pl.pallas_call(
        kernel,
        in_specs=specs + [HBM] * 7,
        out_specs=HBM,
        out_shape=jax.ShapeDtypeStruct((128, 2, 16, 128), F32),
        scratch_shapes=[pltpu.VMEM(x.shape, x.dtype) for x in tables]
        + [
            pltpu.VMEM((NP * NQ, 2, 16, 128), F32),
            pltpu.VMEM((NP, NQ, 2, 16, 128), F32),
            pltpu.VMEM((128, 2, 16, 128), F32),
            pltpu.SemaphoreType.DMA((4,)),
            pltpu.SemaphoreType.DMA((NP,)),
            pltpu.SemaphoreType.DMA((7,)),
        ],
        cost_estimate=pl.CostEstimate(flops=10**10, bytes_accessed=6 * 10**6, transcendentals=0),
    )(*operands, *tables)


def _dot_t(a, b):
    return lax.dot_general(
        a, b, (((1,), (1,)), ((), ())), precision=lax.Precision.HIGHEST, preferred_element_type=F32
    )


def _prep_kernel(h_ref, dft_ref, turn_ref, wrap_ref, ah_ref, al_ref, g_ref):
    def mul(a, b):
        return jnp.dot(a, b, precision=lax.Precision.HIGHEST, preferred_element_type=F32)

    hr, hi = h_ref[0], h_ref[1]
    dr, di = dft_ref[0], dft_ref[1]
    g = (mul(hr, dr) - mul(hi, di), mul(hr, di) + mul(hi, dr))
    r, i = cmul(g, (turn_ref[0], turn_ref[1]))
    g_ref[:, 0, :] = r
    g_ref[:, 1, :] = i
    row = lax.broadcasted_iota(jnp.int32, (128, 128), 0)
    lane = lax.broadcasted_iota(jnp.int32, (128, 128), 1)
    over = lane > row

    def body(k, carry):
        m = []
        for c in range(2):
            line = jnp.broadcast_to(g_ref[k, c : c + 1, :], (128, 128))
            m.append(pltpu.roll(line, 0, 1, stride=1, stride_axis=0))
        turned = cmul(m, (wrap_ref[k, 0:1, :], wrap_ref[k, 1:2, :]))
        re = jnp.where(over, turned[0], m[0])
        im = jnp.where(over, turned[1], m[1])
        for rows, cols, block in ((0, 0, re), (0, 1, -im), (1, 0, im), (1, 1, re)):
            high, low = split(block)
            at = (k, slice(128 * rows, 128 * rows + 128), slice(128 * cols, 128 * cols + 128))
            ah_ref[at] = high
            al_ref[at] = low
        return carry

    lax.fori_loop(0, 16, body, 0, unroll=2)


def prep(h):
    t = TABLES
    shape = jax.ShapeDtypeStruct((16, 256, 256), BF16)
    return pl.pallas_call(
        _prep_kernel,
        out_shape=(shape, shape),
        scratch_shapes=[pltpu.VMEM((16, 2, 128), F32)],
        cost_estimate=pl.CostEstimate(flops=2 * 10**9, bytes_accessed=5 * 10**6, transcendentals=0),
        name="prep",
    )(h, t["dft"], t["turn"], t["wrap"])


def _azimuth_front(x_ref, ah_hbm, al_hbm, e_ref, ah_ref, al_ref, sem):
    matrices = [
        pltpu.make_async_copy(ah_hbm, ah_ref, sem.at[0]),
        pltpu.make_async_copy(al_hbm, al_ref, sem.at[1]),
    ]
    for copy in matrices:
        copy.start()

    def first(s, carry):
        for g in range(2):
            rows = slice(8 * g, 8 * g + 8)
            v = [(x_ref[a, s, 0, rows, :], x_ref[a, s, 1, rows, :]) for a in range(16)]
            v = dft16(v, -1)
            for k in range(16):
                for c in range(2):
                    at = pl.multiple_of(c * 128 + s * 16 + g * 8, 8)
                    e_ref[k, pl.ds(at, 8), :] = v[k][c]
        return carry

    lax.fori_loop(0, 8, first, 0)
    for copy in matrices:
        copy.wait()

    def second(k, carry):
        hi, lo = split(e_ref[k])
        wide = dot(ah_ref[k], jnp.concatenate([hi, lo], axis=1))
        e_ref[k] = wide[:, :128] + wide[:, 128:] + dot(al_ref[k], hi)
        return carry

    lax.fori_loop(0, 16, second, 0, unroll=4)


AZIMUTH_SCRATCH = [
    pltpu.VMEM((16, 256, 128), F32),
    pltpu.VMEM((16, 256, 256), BF16),
    pltpu.VMEM((16, 256, 256), BF16),
    pltpu.SemaphoreType.DMA((4,)),
]


def _azimuth_rows(e_ref, g):
    at = [pl.multiple_of(c * 128 + g * 8, 8) for c in range(2)]
    v = [(e_ref[k, pl.ds(at[0], 8), :], e_ref[k, pl.ds(at[1], 8), :]) for k in range(16)]
    return dft16(v, 1)


def _slave_kernel(x_ref, ah_hbm, al_hbm, o_hbm, left_ref, right_ref, o_ref, e_ref, *scratch):
    _azimuth_front(x_ref, ah_hbm, al_hbm, e_ref, *scratch)
    low = lax.broadcasted_iota(jnp.int32, (8, 128), 1) < 64
    zero = jnp.zeros((ASH, 128), F32)
    for ref in (o_ref.at[0], o_ref.at[1], left_ref, right_ref):
        ref[0:ASH, :] = zero
        ref[ASH + LINES :, :] = zero

    def third(g, carry):
        v = _azimuth_rows(e_ref, g)
        for a in range(16):
            rows = pl.ds(pl.multiple_of(a * 128 + g * 8 + ASH, 8), 8)
            r, i = v[a]
            o_ref[0, rows, :] = r
            o_ref[1, rows, :] = i
            left_ref[rows, :] = jnp.where(low, r, pltpu.roll(i, 64, 1))
            right_ref[rows, :] = jnp.where(low, pltpu.roll(r, 64, 1), i)
        return carry

    lax.fori_loop(0, 16, third, 0)
    out = pltpu.make_async_copy(o_ref, o_hbm, scratch[-1].at[2])
    out.start()
    out.wait()


def slave_azimuth(x, ah, al):
    side = jax.ShapeDtypeStruct((LINES + 2 * ASH, 128), F32)
    return pl.pallas_call(
        _slave_kernel,
        out_shape=(jax.ShapeDtypeStruct((2, LINES + 2 * ASH, 128), F32), side, side),
        in_specs=[VMEM, HBM, HBM],
        out_specs=(HBM, VMEM, VMEM),
        scratch_shapes=[pltpu.VMEM((2, LINES + 2 * ASH, 128), F32)] + AZIMUTH_SCRATCH,
        compiler_params=limit(52),
        cost_estimate=pl.CostEstimate(flops=5 * 10**9, bytes_accessed=10**7, transcendentals=0),
        name="slave_azimuth",
    )(x.reshape(16, 8, 2, 16, 128), ah, al)


def _resample_kernel(az_ref, rg_ref, s_hbm, left_ref, right_ref, o_hbm, s_ref, o_ref, sem):
    lane = lax.broadcasted_iota(jnp.int32, (64, 128), 1)
    low = lane < 64

    def load(block):
        rows = pl.ds(0, BA + 2 * ASH) if block == 0 else pl.ds(block * BA + 2 * ASH, BA)
        return pltpu.make_async_copy(s_hbm.at[:, rows], s_ref.at[:, rows], sem.at[block])

    def store(block):
        rows = pl.ds(block * BA, BA)
        return pltpu.make_async_copy(o_ref.at[:, rows], o_hbm.at[:, rows], sem.at[4 + block])

    for block in range(NBA):
        load(block).start()
    for block in range(NBA):
        load(block).wait()

        def move(t, carry):
            parts = []
            for r, side_ref in ((0, left_ref), (1, right_ref)):
                shift = rg_ref[block, r]
                rows = pl.ds(block * BA + t * 64 + ASH + az_ref[block, r], 64)
                whole = lax.rem(256 - shift, 128)
                half = lax.rem(192 - shift, 128)
                near = lane + shift >= 0 if r == 0 else lane + shift < 128
                side = side_ref[rows, :]
                turns = (half, whole) if r == 0 else (whole, half)
                parts.append(
                    [
                        jnp.where(
                            near,
                            pltpu.roll(s_ref[c, rows, :], whole, 1),
                            pltpu.roll(side, turns[c], 1),
                        )
                        for c in range(2)
                    ]
                )
            rows = pl.ds(pl.multiple_of(block * BA + t * 64, 64), 64)
            for c in range(2):
                o_ref[c, rows, :] = jnp.where(low, parts[0][c], parts[1][c])
            return carry

        lax.fori_loop(0, BA // 64, move, 0, unroll=2)
        store(block).start()
    for block in range(NBA):
        store(block).wait()


def resample(az_shift, rg_shift, focused, left, right):
    return pl.pallas_call(
        _resample_kernel,
        in_specs=[SMEM, SMEM, HBM, VMEM, VMEM],
        out_specs=HBM,
        out_shape=jax.ShapeDtypeStruct((2, LINES, 128), F32),
        scratch_shapes=[
            pltpu.VMEM((2, LINES + 2 * ASH, 128), F32),
            pltpu.VMEM((2, LINES, 128), F32),
            pltpu.SemaphoreType.DMA((8,)),
        ],
        cost_estimate=pl.CostEstimate(flops=2 * 10**9, bytes_accessed=10**7, transcendentals=0),
        compiler_params=limit(61),
        name="resample",
    )(az_shift, rg_shift, focused, left, right)


def _master_kernel(x_ref, ah_hbm, al_hbm, m_hbm, n_ref, pick_ref, box_ref, side_ref, c_ref, m_ref, e_ref, *scratch):
    moved = pltpu.make_async_copy(m_hbm, m_ref, scratch[-1].at[2])
    moved.start()
    _azimuth_front(x_ref, ah_hbm, al_hbm, e_ref, *scratch)
    moved.wait()
    line = lax.broadcasted_iota(jnp.int32, (8, 128), 0)
    count = n_ref[...]

    def third(g, carry):
        v = _azimuth_rows(e_ref, g)
        for a in range(16):
            at = pl.multiple_of(a * 128 + g * 8, 8)
            r, i = v[a]
            sr, si = m_ref[0, pl.ds(at, 8), :], m_ref[1, pl.ds(at, 8), :]
            keep = line + at < count
            c_ref[pl.ds(at, 8), :] = jnp.where(keep, r * sr + i * si, 0.0)
            c_ref[pl.ds(at + LINES, 8), :] = jnp.where(keep, i * sr - r * si, 0.0)
        return carry

    lax.fori_loop(0, 16, third, 0)
    total = c_ref[pl.ds(0, 512, stride=LOOK), :]
    for j in range(1, LOOK):
        total = total + c_ref[pl.ds(j, 512, stride=LOOK), :]
    y = _dot_t(pick_ref[...], total)
    cell = lax.broadcasted_iota(jnp.int32, (24, 512), 1) % 256
    y = (
        y
        + jnp.where(cell == 0, 0.0, pltpu.roll(y, 1, 1))
        + jnp.where(cell == 255, 0.0, pltpu.roll(y, 511, 1))
    )
    box_ref[...] = y[:16]
    side_ref[...] = y[16:]


def master_looks(x, ah, al, moved, counts):
    return pl.pallas_call(
        _master_kernel,
        out_shape=(
            jax.ShapeDtypeStruct((16, 512), F32),
            jax.ShapeDtypeStruct((8, 512), F32),
        ),
        in_specs=[VMEM, HBM, HBM, HBM, VMEM, VMEM],
        compiler_params=limit(52),
        scratch_shapes=[pltpu.VMEM((2 * LINES, 128), F32), pltpu.VMEM((2, LINES, 128), F32)]
        + AZIMUTH_SCRATCH,
        cost_estimate=pl.CostEstimate(flops=5 * 10**9, bytes_accessed=10**7, transcendentals=0),
        name="master_looks",
    )(x.reshape(16, 8, 2, 16, 128), ah, al, moved, counts, TABLES["pick"])


def _final_kernel(box_ref, left_ref, right_ref, scale_ref, o_ref):
    row = lax.broadcasted_iota(jnp.int32, (16, 256), 0)
    for c in range(2):
        at = slice(256 * c, 256 * c + 256)
        x = box_ref[:, at]
        x = x + jnp.where(row == 0, left_ref[1:2, at], 0.0)
        x = x + jnp.where(row == 15, right_ref[0:1, at], 0.0)
        o_ref[c] = x * scale_ref[...]


def final(box, left, right, scale):
    return pl.pallas_call(
        _final_kernel,
        out_shape=jax.ShapeDtypeStruct((2, 16, 256), F32),
        compiler_params=limit(4),
        name="final",
    )(box, left, right, scale)


def to_worker(x):
    return lax.ppermute(x, ALL, [(b, worker(b)) for b in range(128)])


def halo(to_right, to_left):
    up = [(worker(b), worker(b + 1)) for b in range(127)]
    down = [(j, i) for i, j in up]
    return lax.ppermute(to_right, ALL, up), lax.ppermute(to_left, ALL, down)


def local(master_raw, slave_raw, range_ref, az_ref, az_shift, rg_shift, valid_lines):
    hf = range_ref.reshape(2, NS, NQ, NP).transpose(3, 2, 0, 1).reshape(NP * NQ, 2, NS)
    hf = jnp.pad(hf * (1.0 / RANGE), ((0, 0), (0, 0), (0, 3)))
    h = az_ref.reshape(2, 128, 16).transpose(0, 2, 1) * (1.0 / LINES)

    def columns_of(ranged):
        return lax.all_to_all(ranged, ALL, 0, 0, tiled=True)

    flat = lax.axis_index(ALL)
    counts = lax.dynamic_slice(jnp.pad(valid_lines, 1), (flat * 2,), (4,))
    wide = jnp.concatenate([counts[:1], jnp.repeat(counts[1:3], BR // LOOK), counts[3:]])
    rows = LINES // LOOK
    groups = lax.broadcasted_iota(jnp.int32, (18, rows + 2), 1) - 1
    pixels = jnp.clip(wide[:, None] - LOOK * groups, 0, LOOK) * LOOK
    pixels = jnp.where((groups >= 0) & (groups < rows), pixels, 0).astype(F32)
    box_pixels = sum(pixels[j : j + 16, i : i + rows] for i in range(3) for j in range(3))
    scale = 1.0 / jnp.sqrt(jnp.maximum(box_pixels, 1.0))
    core = lax.axis_index("az") % 2
    block = ((lax.axis_index("az") // 2) * 16 + lax.axis_index("rg")) * 2 + core
    own = lax.dynamic_slice(valid_lines, (block * 2,), (2,))
    col_counts = jnp.repeat(own, BR)[None, :]
    shifts = to_worker(jnp.stack([az_shift, rg_shift]))

    slave = pre(slave_raw)
    slave = lax.all_to_all(slave, "rg", 0, 0, tiled=True)
    me = lax.axis_index("rg").astype(jnp.int32)[None]
    pieces = pre_shifts(me, master_raw)
    master = [
        lax.ppermute(piece, "rg", [(r, shifted(r, shift)) for r in range(NP)])
        if any(shift)
        else piece
        for shift, piece in zip(SHIFTS, pieces)
    ]
    slave = range_compress(_range_kernel, [HBM], [slave], hf)
    slave = columns_of(slave)
    ah, al = prep(h)
    master = range_compress(_range_shift_kernel, [SMEM] + [HBM] * NP, [me, *master], hf)
    master = columns_of(master)
    focused, to_left, to_right = slave_azimuth(slave, ah, al)
    from_left, from_right = halo(to_right, to_left)
    moved = resample(shifts[0], shifts[1], focused, from_left, from_right)

    box, side = master_looks(master, ah, al, moved, col_counts)
    box = lax.ppermute(box, ALL, [(worker(b), b) for b in range(128)])
    left = lax.ppermute(side, ALL, [(worker(b), b + 1) for b in range(127)])
    right = lax.ppermute(side, ALL, [(worker(b + 1), b) for b in range(127)])
    return final(box, left, right, scale).transpose(0, 2, 1)


def solution(mesh):
    return jax.shard_map(
        local,
        mesh=mesh,
        in_specs=(
            P(None, "az", "rg"),
            P(None, "az", "rg"),
            P(),
            P(),
            P(None, ALL),
            P(None, ALL),
            P(),
        ),
        out_specs=P(None, None, ALL),
        check_vma=False,
    )
```

```python
import math

import jax
import jax.numpy as jnp
import numpy as np
from jax import lax
from jax.experimental import pallas as pl
from jax.experimental.pallas import tpu as pltpu
from jax.sharding import PartitionSpec as P


LINES = 2048
RANGE = 20000
LOOK = 8
BA = 512
BR = 64
ASH = 32
RSH = 64
NBA = 4
ALL = ("az", "rg")
NP = 16
NQ = 10
NS = 125
F32 = jnp.float32
BF16 = jnp.bfloat16


SHIFTS = sorted(
    ((dx, dz) for dx in range(4) for dz in range(4)),
    key=lambda s: -(min(s[0], 4 - s[0]) + min(s[1], 4 - s[1])),
)


def shifted(r, shift):
    return ((r // 4 + shift[1]) % 4) * 4 + (r % 4 + shift[0]) % 4


def _rot(v, angle):
    c, s = math.cos(angle), math.sin(angle)
    turns = angle / (math.pi / 4)
    eighth = round(turns)
    x, y = v
    if abs(turns - eighth) < 1e-9:
        e = eighth % 8
        if e == 0:
            return v
        if e == 2:
            return (-y, x)
        if e == 4:
            return (-x, -y)
        if e == 6:
            return (y, -x)
        h = math.sqrt(0.5)
        if e == 1:
            return ((x - y) * h, (x + y) * h)
        if e == 3:
            return (-(x + y) * h, (x - y) * h)
        if e == 5:
            return ((y - x) * h, -(x + y) * h)
        return ((x + y) * h, (y - x) * h)
    return (x * c - y * s, x * s + y * c)


def _add(a, b):
    return (a[0] + b[0], a[1] + b[1])


def _sub(a, b):
    return (a[0] - b[0], a[1] - b[1])


def _dft2(v, sign):
    return [_add(v[0], v[1]), _sub(v[0], v[1])]


def _dft4(v, sign):
    a, b = _add(v[0], v[2]), _sub(v[0], v[2])
    c, d = _add(v[1], v[3]), _sub(v[1], v[3])
    if sign < 0:
        return [_add(a, c), (b[0] + d[1], b[1] - d[0]), _sub(a, c), (b[0] - d[1], b[1] + d[0])]
    return [_add(a, c), (b[0] - d[1], b[1] + d[0]), _sub(a, c), (b[0] + d[1], b[1] - d[0])]


def _dft5(v, sign):
    c1, c2 = math.cos(2 * math.pi / 5), math.cos(4 * math.pi / 5)
    s1, s2 = sign * math.sin(2 * math.pi / 5), sign * math.sin(4 * math.pi / 5)
    a1, b1 = _add(v[1], v[4]), _sub(v[1], v[4])
    a2, b2 = _add(v[2], v[3]), _sub(v[2], v[3])
    x0 = v[0]
    y0 = (x0[0] + a1[0] + a2[0], x0[1] + a1[1] + a2[1])
    p1 = tuple(x0[i] + c1 * a1[i] + c2 * a2[i] for i in range(2))
    p2 = tuple(x0[i] + c2 * a1[i] + c1 * a2[i] for i in range(2))
    q1 = tuple(s1 * b1[i] + s2 * b2[i] for i in range(2))
    q2 = tuple(s2 * b1[i] - s1 * b2[i] for i in range(2))
    return [
        y0,
        (p1[0] - q1[1], p1[1] + q1[0]),
        (p2[0] - q2[1], p2[1] + q2[0]),
        (p2[0] + q2[1], p2[1] - q2[0]),
        (p1[0] + q1[1], p1[1] - q1[0]),
    ]


def _dft_two(v, n1, n2, first, second, sign):
    n = n1 * n2
    out = [None] * n
    mid = []
    for b in range(n2):
        col = first([v[n2 * a + b] for a in range(n1)], sign)
        mid.append([_rot(col[k], sign * 2 * math.pi * ((b * k) % n) / n) for k in range(n1)])
    for k1 in range(n1):
        row = second([mid[b][k1] for b in range(n2)], sign)
        for k2 in range(n2):
            out[k1 + n1 * k2] = row[k2]
    return out


def dft16(v, sign):
    return _dft_two(v, 4, 4, _dft4, _dft4, sign)


def dft10(v, sign):
    return _dft_two(v, 2, 5, _dft2, _dft5, sign)


def cmul(a, b):
    return (a[0] * b[0] - a[1] * b[1], a[0] * b[1] + a[1] * b[0])


def split(x):
    hi = x.astype(BF16)
    return hi, (x - hi.astype(F32)).astype(BF16)


def dot(a, b):
    return jnp.dot(a, b, preferred_element_type=F32)


def worker(block):
    chip, core = divmod(block, 2)
    y, rest = divmod(chip, 16)
    return (y * 2 + core) * 16 + rest


def _np_split(x):
    x = np.asarray(x, np.float32)
    hi = x.astype(BF16)
    return hi, (x - hi.astype(np.float32)).astype(BF16)


def _tables():
    t = {}
    two = 2 * np.pi
    q2 = np.arange(128)
    keep = (q2 < NS)[None, :]
    ang = -two * ((np.arange(NQ)[:, None] * q2[None, :]) % 1250) / 1250
    t["twb"] = np.stack([np.cos(ang) * keep, np.sin(ang) * keep], 1).astype(np.float32)
    n = np.arange(NQ)[None, :, None] * NS + q2[None, None, :]
    ang = two * ((np.arange(NP)[:, None, None] * n) % RANGE) / RANGE
    t["twc"] = np.stack([np.cos(ang), np.sin(ang)], 2).reshape(NP * NQ, 2, 128).astype(np.float32)
    ang = two * ((q2[:, None] * q2[None, :]) % NS) / NS
    both = keep & keep.T
    c, s = np.cos(ang) * both, np.sin(ang) * both
    t["fh"], t["fl"] = _np_split(np.block([[c, -s], [s, c]]))
    t["gh"], t["gl"] = _np_split(np.block([[c, s], [-s, c]]))
    k2 = np.arange(128)
    back = (-np.arange(128)) % 128
    ang = two * ((k2[:, None] * back[None, :]) % 128) / 128
    t["dft"] = np.stack([np.cos(ang), np.sin(ang)]).astype(np.float32)
    ang = two * (np.arange(16)[:, None] * back[None, :]) / LINES
    t["turn"] = np.stack([np.cos(ang), np.sin(ang)]).astype(np.float32)
    ang = np.broadcast_to(-two * np.arange(16)[:, None] / 16, (16, 128))
    t["wrap"] = np.stack([np.cos(ang), np.sin(ang)], 1).astype(np.float32)
    lane = np.arange(128)
    pick = np.zeros((24, 128), np.float32)
    for o in range(16):
        pick[o] = np.abs(lane // LOOK - o) <= 1
    pick[16] = lane < LOOK
    pick[17] = lane >= 128 - LOOK
    t["pick"] = pick
    return t


TABLES = _tables()


HBM = pl.BlockSpec(memory_space=pltpu.HBM)
VMEM = pl.BlockSpec(memory_space=pltpu.VMEM)
SMEM = pl.BlockSpec(memory_space=pltpu.SMEM)


AZIMUTH_MIB = 61


def limit(mib):
    return pltpu.CompilerParams(vmem_limit_bytes=mib << 20)


def _raw_rows(raw):
    raw = raw.transpose(2, 0, 1).reshape(1250, 2, 2, 128)
    return raw.transpose(0, 2, 1, 3).reshape(5000, 128)


def _read_lines(x_hbm, x_ref, t_ref, sem, done):
    def load(q):
        rows = pl.ds(1000 * q, 1000)
        return pltpu.make_async_copy(x_hbm.at[rows], x_ref.at[rows], sem.at[q])

    for q in range(5):
        load(q).start()
    for q in range(NQ):
        if q % 2 == 0:
            load(q // 2).wait()
        for half in range(2):
            for c in range(2):
                v = x_ref[pl.ds(500 * q + 2 * half + c, NS, stride=4), :]
                v = jnp.concatenate([v, jnp.zeros((128 - NS, 128), F32)], axis=0).T
                for k in range(8):
                    t_ref[8 * half + k, q, c] = v[16 * k : 16 * k + 16]
        done(q)


def _pre_kernel(x_hbm, o_hbm, x_ref, t_ref, sem):
    def store(q):
        at = pl.ds(2 * (q // 2), 2)
        return pltpu.make_async_copy(t_ref.at[:, at], o_hbm.at[:, at], sem.at[5 + q // 2])

    _read_lines(x_hbm, x_ref, t_ref, sem, lambda q: store(q).start() if q % 2 else None)
    for q in range(0, NQ, 2):
        store(q).wait()


def _pre_shift_kernel(me_ref, x_hbm, *refs):
    outs, (x_ref, t_ref, sem) = refs[:NP], refs[NP:]
    _read_lines(x_hbm, x_ref, t_ref, sem, lambda q: None)
    me = me_ref[0]
    stores = [
        pltpu.make_async_copy(t_ref.at[shifted(me, shift)], o_hbm, sem.at[5 + k])
        for k, (shift, o_hbm) in enumerate(zip(SHIFTS, outs))
    ]
    for store in stores:
        store.start()
    for store in stores:
        store.wait()


PRE_SCRATCH = [
    pltpu.VMEM((5000, 128), F32),
    pltpu.VMEM((NP, NQ, 2, 16, 128), F32),
    pltpu.SemaphoreType.DMA((5 + NP,)),
]


def pre(raw):
    return pl.pallas_call(
        _pre_kernel,
        in_specs=[HBM],
        out_specs=HBM,
        out_shape=jax.ShapeDtypeStruct((NP, NQ, 2, 16, 128), F32),
        scratch_shapes=PRE_SCRATCH,
        cost_estimate=pl.CostEstimate(flops=10**8, bytes_accessed=10**7, transcendentals=0),
        name="pre",
    )(_raw_rows(raw))


def pre_shifts(me, raw):
    return pl.pallas_call(
        _pre_shift_kernel,
        in_specs=[SMEM, HBM],
        out_specs=[HBM] * NP,
        out_shape=[jax.ShapeDtypeStruct((NQ, 2, 16, 128), F32)] * NP,
        scratch_shapes=PRE_SCRATCH,
        cost_estimate=pl.CostEstimate(flops=10**8, bytes_accessed=10**7, transcendentals=0),
        name="pre_shifts",
    )(me, _raw_rows(raw))


def _range_body(ready, tables, o_hbm, d_ref, x_ref, o_ref, out_sem):
    twb_ref, hf_ref, fh_ref, fl_ref, gh_ref, gl_ref, twc_ref = tables
    lane = lax.broadcasted_iota(jnp.int32, (16, 128), 1)

    def outer(q, carry):
        ready(q)
        for g in range(2):
            rows = slice(8 * g, 8 * g + 8)
            v = [(x_ref[p, q, 0, rows, :], x_ref[p, q, 1, rows, :]) for p in range(NP)]
            v = dft16(v, -1)
            for k in range(NP):
                at = k * NQ + q
                r, i = cmul(v[k], (twc_ref[at, 0:1, :], -twc_ref[at, 1:2, :]))
                d_ref[at, 0, rows, :] = r
                d_ref[at, 1, rows, :] = i
        return carry

    lax.fori_loop(0, NQ, outer, 0, unroll=2)
    ready(None)

    def middle(kp, carry):
        v = [(d_ref[kp * NQ + q, 0], d_ref[kp * NQ + q, 1]) for q in range(NQ)]
        v = dft10(v, -1)
        rows = []
        for k in range(NQ):
            r, i = cmul(v[k], (twb_ref[k, 0:1, :], twb_ref[k, 1:2, :]))
            rows.append(jnp.concatenate([r, i], axis=1))
        hi, lo = split(jnp.concatenate(rows, axis=0))
        y = dot(hi, fh_ref[...]) + dot(lo, fh_ref[...]) + dot(hi, fl_ref[...])
        rows = []
        for k in range(NQ):
            val = (y[16 * k : 16 * k + 16, :128], y[16 * k : 16 * k + 16, 128:])
            r, i = cmul(val, (hf_ref[kp * NQ + k, 0:1, :], hf_ref[kp * NQ + k, 1:2, :]))
            rows.append(jnp.concatenate([r, i], axis=1))
        hi, lo = split(jnp.concatenate(rows, axis=0))
        y = dot(hi, gh_ref[...]) + dot(lo, gh_ref[...]) + dot(hi, gl_ref[...])
        v = []
        for k in range(NQ):
            val = (y[16 * k : 16 * k + 16, :128], y[16 * k : 16 * k + 16, 128:])
            v.append(cmul(val, (twb_ref[k, 0:1, :], -twb_ref[k, 1:2, :])))
        v = dft10(v, 1)
        for q in range(NQ):
            at = kp * NQ + q
            r, i = cmul(v[q], (twc_ref[at, 0:1, :], twc_ref[at, 1:2, :]))
            d_ref[at, 0] = r
            d_ref[at, 1] = i
        return carry

    lax.fori_loop(0, NP, middle, 0, unroll=4)

    def inner(q, carry):
        for g in range(2):
            rows = slice(8 * g, 8 * g + 8)
            v = [(d_ref[k * NQ + q, 0, rows, :], d_ref[k * NQ + q, 1, rows, :]) for k in range(NP)]
            v = dft16(v, 1)
            for p in range(14):
                d_ref[p * NQ + q, 0, rows, :] = v[p][0]
                d_ref[p * NQ + q, 1, rows, :] = v[p][1]
        return carry

    lax.fori_loop(0, NQ, inner, 0, unroll=2)

    def store(part):
        at = pl.ds(32 * part, 32)
        return pltpu.make_async_copy(o_ref.at[at], o_hbm.at[at], out_sem.at[part])

    for d in range(128):
        n, a = divmod(128 * d, NS)
        for c in range(2):
            val = d_ref[n, c]
            if a:
                val = pltpu.roll(val, 128 - a, 1)
            start = NS - a
            while start < 128:
                n2 = (128 * d + start) // NS
                nxt = d_ref[n2, c]
                nxt = pltpu.roll(nxt, start % 128, 1)
                val = jnp.where(lane < start, val, nxt)
                start += NS
            o_ref[worker(d), c] = val
        if d % 32 == 31:
            store(d // 32).start()
    for part in range(4):
        store(part).wait()


def _tables_in(table_hbm, tables, sem):
    copies = [
        pltpu.make_async_copy(src, dst, sem.at[k]) for k, (src, dst) in enumerate(zip(table_hbm, tables))
    ]
    for copy in copies[::-1]:
        copy.start()
    return copies


def _range_kernel(x_hbm, *refs):
    table_hbm, o_hbm, tables, (d_ref, x_ref, o_ref, out_sem, in_sem, sem) = refs[:7], refs[7], refs[8:15], refs[15:]

    def load(q):
        return pltpu.make_async_copy(x_hbm.at[:, q], x_ref.at[:, q], in_sem.at[q])

    def ready(q):
        if q is None:
            for copy in copies[:6]:
                copy.wait()
        else:
            load(q).wait()

    copies = _tables_in(table_hbm, tables, sem)
    for q in range(NQ):
        load(q).start()
    copies[6].wait()
    _range_body(ready, tables, o_hbm, d_ref, x_ref, o_ref, out_sem)


def _range_shift_kernel(me_ref, *refs):
    parts, refs = refs[:NP], refs[NP:]
    table_hbm, o_hbm, tables, (d_ref, x_ref, o_ref, out_sem, in_sem, sem) = refs[:7], refs[7], refs[8:15], refs[15:]
    me = me_ref[0]
    loads = [
        pltpu.make_async_copy(
            part, x_ref.at[shifted(me, (4 - shift[0], 4 - shift[1]))], in_sem.at[k]
        )
        for k, (shift, part) in enumerate(zip(SHIFTS, parts))
    ]

    def ready(q):
        if q is None:
            for copy in copies[:6]:
                copy.wait()

    copies = _tables_in(table_hbm, tables, sem)
    for load in loads:
        load.start()
    for load in loads:
        load.wait()
    copies[6].wait()
    _range_body(ready, tables, o_hbm, d_ref, x_ref, o_ref, out_sem)


def range_compress(kernel, specs, operands, hf):
    t = TABLES
    tables = (t["twb"], hf, t["fh"], t["fl"], t["gh"], t["gl"], t["twc"])
    return pl.pallas_call(
        kernel,
        in_specs=specs + [HBM] * 7,
        out_specs=HBM,
        out_shape=jax.ShapeDtypeStruct((128, 2, 16, 128), F32),
        scratch_shapes=[pltpu.VMEM(x.shape, x.dtype) for x in tables]
        + [
            pltpu.VMEM((NP * NQ, 2, 16, 128), F32),
            pltpu.VMEM((NP, NQ, 2, 16, 128), F32),
            pltpu.VMEM((128, 2, 16, 128), F32),
            pltpu.SemaphoreType.DMA((4,)),
            pltpu.SemaphoreType.DMA((NP,)),
            pltpu.SemaphoreType.DMA((7,)),
        ],
        cost_estimate=pl.CostEstimate(flops=10**10, bytes_accessed=6 * 10**6, transcendentals=0),
    )(*operands, *tables)


def _dot_t(a, b):
    return lax.dot_general(
        a, b, (((1,), (1,)), ((), ())), precision=lax.Precision.HIGHEST, preferred_element_type=F32
    )


def _prep_kernel(h_ref, dft_ref, turn_ref, wrap_ref, a_ref, g_ref):
    def mul(a, b):
        return jnp.dot(a, b, precision=lax.Precision.HIGHEST, preferred_element_type=F32)

    hr, hi = h_ref[0], h_ref[1]
    dr, di = dft_ref[0], dft_ref[1]
    g = (mul(hr, dr) - mul(hi, di), mul(hr, di) + mul(hi, dr))
    r, i = cmul(g, (turn_ref[0], turn_ref[1]))
    g_ref[:, 0, :] = r
    g_ref[:, 1, :] = i
    row = lax.broadcasted_iota(jnp.int32, (128, 128), 0)
    lane = lax.broadcasted_iota(jnp.int32, (128, 128), 1)
    over = lane > row

    def body(k, carry):
        m = []
        for c in range(2):
            line = jnp.broadcast_to(g_ref[k, c : c + 1, :], (128, 128))
            m.append(pltpu.roll(line, 0, 1, stride=1, stride_axis=0))
        turned = cmul(m, (wrap_ref[k, 0:1, :], wrap_ref[k, 1:2, :]))
        re = jnp.where(over, turned[0], m[0])
        im = jnp.where(over, turned[1], m[1])
        for part, block in enumerate((re, -im)):
            cols = slice(128 * part, 128 * part + 128)
            high, low = split(block)
            a_ref[k, 0:128, cols] = high
            a_ref[k, 128:256, cols] = low
        return carry

    lax.fori_loop(0, 16, body, 0, unroll=2)


def prep(h):
    t = TABLES
    return pl.pallas_call(
        _prep_kernel,
        out_shape=jax.ShapeDtypeStruct((16, 256, 256), BF16),
        scratch_shapes=[pltpu.VMEM((16, 2, 128), F32)],
        cost_estimate=pl.CostEstimate(flops=2 * 10**9, bytes_accessed=5 * 10**6, transcendentals=0),
        name="prep",
    )(h, t["dft"], t["turn"], t["wrap"])


def _azimuth_front(x_hbm, a_hbm, e_ref, x_ref, a_ref, sem):
    def load(s):
        return pltpu.make_async_copy(x_hbm.at[:, s], x_ref.at[:, s], sem.at[s])

    matrices = pltpu.make_async_copy(a_hbm, a_ref, sem.at[8])
    for s in range(8):
        load(s).start()
    matrices.start()

    def first(s, carry):
        load(s).wait()
        for g in range(2):
            rows = slice(8 * g, 8 * g + 8)
            v = [(x_ref[a, s, 0, rows, :], x_ref[a, s, 1, rows, :]) for a in range(16)]
            v = dft16(v, -1)
            for k in range(16):
                for c in range(2):
                    at = pl.multiple_of(c * 128 + s * 16 + g * 8, 8)
                    e_ref[k, pl.ds(at, 8), :] = v[k][c]
        return carry

    lax.fori_loop(0, 8, first, 0, unroll=2)
    matrices.wait()

    def second(k, carry):
        re_hi, re_lo = split(e_ref[k, 0:128, :])
        im_hi, im_lo = split(e_ref[k, 128:256, :])

        def turned(re, im):
            straight = jnp.concatenate([re, im], axis=0)
            return jnp.concatenate([straight, jnp.concatenate([im, -re], axis=0)], axis=1)

        y = dot(a_ref[k], turned(re_hi, im_hi))
        y = y[:128] + y[128:] + dot(a_ref[k, 0:128, :], turned(re_lo, im_lo))
        e_ref[k, 0:128, :] = y[:, :128]
        e_ref[k, 128:256, :] = y[:, 128:]
        return carry

    lax.fori_loop(0, 16, second, 0, unroll=4)


AZIMUTH_SCRATCH = [
    pltpu.VMEM((16, 256, 128), F32),
    pltpu.VMEM((16, 8, 2, 16, 128), F32),
    pltpu.VMEM((16, 256, 256), BF16),
    pltpu.SemaphoreType.DMA((13,)),
]


def _azimuth_rows(e_ref, g):
    at = [pl.multiple_of(c * 128 + g * 8, 8) for c in range(2)]
    v = [(e_ref[k, pl.ds(at[0], 8), :], e_ref[k, pl.ds(at[1], 8), :]) for k in range(16)]
    return dft16(v, 1)


def _slave_kernel(x_hbm, a_hbm, left_hbm, right_hbm, left_ref, right_ref, *scratch):
    _azimuth_front(x_hbm, a_hbm, *scratch)
    e_ref, sem = scratch[0], scratch[-1]
    low = lax.broadcasted_iota(jnp.int32, (8, 128), 1) < 64
    zero = jnp.zeros((ASH, 128), F32)
    for ref in (left_ref, right_ref):
        ref[0:ASH, :] = zero
        ref[ASH + LINES :, :] = zero

    def third(g, carry):
        v = _azimuth_rows(e_ref, g)
        for a in range(16):
            rows = pl.ds(pl.multiple_of(a * 128 + g * 8 + ASH, 8), 8)
            r, i = v[a]
            left_ref[rows, :] = jnp.where(low, r, pltpu.roll(i, 64, 1))
            right_ref[rows, :] = jnp.where(low, pltpu.roll(r, 64, 1), i)
        return carry

    lax.fori_loop(0, 16, third, 0, unroll=2)
    copies = [
        pltpu.make_async_copy(right_ref, right_hbm, sem.at[10]),
        pltpu.make_async_copy(left_ref, left_hbm, sem.at[9]),
    ]
    for copy in copies:
        copy.start()
    for copy in copies:
        copy.wait()


def slave_azimuth(x, a):
    side = jax.ShapeDtypeStruct((LINES + 2 * ASH, 128), F32)
    return pl.pallas_call(
        _slave_kernel,
        in_specs=[HBM, HBM],
        out_specs=(HBM, HBM),
        out_shape=(side, side),
        scratch_shapes=[pltpu.VMEM(side.shape, F32)] * 2 + AZIMUTH_SCRATCH,
        cost_estimate=pl.CostEstimate(flops=5 * 10**9, bytes_accessed=10**7, transcendentals=0),
        compiler_params=limit(AZIMUTH_MIB),
        name="slave_azimuth",
    )(x.reshape(16, 8, 2, 16, 128), a)


def _resample_kernel(az_ref, rg_ref, *refs):
    packs, o_hbm, w_ref, o_ref, sem = refs[:4], refs[4], refs[5], refs[6], refs[7]
    lane = lax.broadcasted_iota(jnp.int32, (64, 128), 1)
    low = lane < 64

    def load(block):
        rows = pl.ds(0, BA + 2 * ASH) if block == 0 else pl.ds(block * BA + 2 * ASH, BA)
        return [
            pltpu.make_async_copy(pack.at[rows], w_ref.at[k, rows], sem.at[4 * block + k])
            for k, pack in enumerate(packs)
        ]

    def store(block):
        rows = pl.ds(block * BA, BA)
        return pltpu.make_async_copy(o_ref.at[:, rows], o_hbm.at[:, rows], sem.at[16 + block])

    for block in range(NBA):
        for copy in load(block):
            copy.start()
    for block in range(NBA):
        for copy in load(block):
            copy.wait()

        def move(t, carry):
            parts = []
            for r in range(2):
                shift = rg_ref[block, r] + RSH
                first = shift // 64 + r
                second = jnp.minimum(first + 1, 3)
                s = lax.rem(shift, 64)
                rows = pl.ds(block * BA + t * 64 + ASH + az_ref[block, r], 64)
                parts.append(
                    jnp.where(
                        (lane & 63) + s < 64,
                        pltpu.roll(w_ref[first, rows, :], lax.rem(128 - s, 128), 1),
                        pltpu.roll(w_ref[second, rows, :], 64 - s, 1),
                    )
                )
            rows = pl.ds(pl.multiple_of(block * BA + t * 64, 64), 64)
            o_ref[0, rows, :] = jnp.where(low, parts[0], pltpu.roll(parts[1], 64, 1))
            o_ref[1, rows, :] = jnp.where(low, pltpu.roll(parts[0], 64, 1), parts[1])
            return carry

        lax.fori_loop(0, BA // 64, move, 0, unroll=4)
        store(block).start()
    for block in range(NBA):
        store(block).wait()


def resample(az_shift, rg_shift, packs):
    return pl.pallas_call(
        _resample_kernel,
        in_specs=[SMEM, SMEM] + [HBM] * 4,
        out_specs=HBM,
        out_shape=jax.ShapeDtypeStruct((2, LINES, 128), F32),
        scratch_shapes=[
            pltpu.VMEM((4, LINES + 2 * ASH, 128), F32),
            pltpu.VMEM((2, LINES, 128), F32),
            pltpu.SemaphoreType.DMA((20,)),
        ],
        cost_estimate=pl.CostEstimate(flops=2 * 10**9, bytes_accessed=10**7, transcendentals=0),
        compiler_params=limit(61),
        name="resample",
    )(az_shift, rg_shift, *packs)


def _master_kernel(x_hbm, a_hbm, m_hbm, n_ref, pick_ref, box_ref, side_ref, c_ref, m_ref, *scratch):
    e_ref = scratch[0]
    moved = pltpu.make_async_copy(m_hbm, m_ref, scratch[-1].at[9])
    moved.start()
    _azimuth_front(x_hbm, a_hbm, *scratch)
    moved.wait()
    line = lax.broadcasted_iota(jnp.int32, (8, 128), 0)
    count = n_ref[...]

    def third(g, carry):
        v = _azimuth_rows(e_ref, g)
        for a in range(16):
            at = pl.multiple_of(a * 128 + g * 8, 8)
            r, i = v[a]
            sr, si = m_ref[0, pl.ds(at, 8), :], m_ref[1, pl.ds(at, 8), :]
            keep = line + at < count
            c_ref[pl.ds(at, 8), :] = jnp.where(keep, r * sr + i * si, 0.0)
            c_ref[pl.ds(at + LINES, 8), :] = jnp.where(keep, i * sr - r * si, 0.0)
        return carry

    lax.fori_loop(0, 16, third, 0, unroll=2)
    total = c_ref[pl.ds(0, 512, stride=LOOK), :]
    for j in range(1, LOOK):
        total = total + c_ref[pl.ds(j, 512, stride=LOOK), :]
    y = _dot_t(pick_ref[...], total)
    cell = lax.broadcasted_iota(jnp.int32, (24, 512), 1) % 256
    y = (
        y
        + jnp.where(cell == 0, 0.0, pltpu.roll(y, 1, 1))
        + jnp.where(cell == 255, 0.0, pltpu.roll(y, 511, 1))
    )
    box_ref[...] = y[:16]
    side_ref[...] = y[16:]


def master_looks(x, a, moved, counts):
    return pl.pallas_call(
        _master_kernel,
        out_shape=(
            jax.ShapeDtypeStruct((16, 512), F32),
            jax.ShapeDtypeStruct((8, 512), F32),
        ),
        in_specs=[HBM, HBM, HBM, VMEM, VMEM],
        compiler_params=limit(AZIMUTH_MIB),
        scratch_shapes=[pltpu.VMEM((2 * LINES, 128), F32), pltpu.VMEM((2, LINES, 128), F32)]
        + AZIMUTH_SCRATCH,
        cost_estimate=pl.CostEstimate(flops=5 * 10**9, bytes_accessed=10**7, transcendentals=0),
        name="master_looks",
    )(x.reshape(16, 8, 2, 16, 128), a, moved, counts, TABLES["pick"])


def _final_kernel(box_ref, left_ref, right_ref, scale_ref, o_ref):
    row = lax.broadcasted_iota(jnp.int32, (16, 256), 0)
    for c in range(2):
        at = slice(256 * c, 256 * c + 256)
        x = box_ref[:, at]
        x = x + jnp.where(row == 0, left_ref[1:2, at], 0.0)
        x = x + jnp.where(row == 15, right_ref[0:1, at], 0.0)
        o_ref[c] = x * scale_ref[...]


def final(box, left, right, scale):
    return pl.pallas_call(
        _final_kernel,
        out_shape=jax.ShapeDtypeStruct((2, 16, 256), F32),
        compiler_params=limit(4),
        name="final",
    )(box, left, right, scale)


def to_worker(x):
    return lax.ppermute(x, ALL, [(b, worker(b)) for b in range(128)])


def halo(to_right, to_left):
    up = [(worker(b), worker(b + 1)) for b in range(127)]
    down = [(j, i) for i, j in up]
    return lax.ppermute(to_right, ALL, up), lax.ppermute(to_left, ALL, down)


def local(master_raw, slave_raw, range_ref, az_ref, az_shift, rg_shift, valid_lines):
    hf = range_ref.reshape(2, NS, NQ, NP).transpose(3, 2, 0, 1).reshape(NP * NQ, 2, NS)
    hf = jnp.pad(hf * (1.0 / RANGE), ((0, 0), (0, 0), (0, 3)))
    h = az_ref.reshape(2, 128, 16).transpose(0, 2, 1) * (1.0 / LINES)

    def columns_of(ranged):
        return lax.all_to_all(ranged, ALL, 0, 0, tiled=True)

    flat = lax.axis_index(ALL)
    counts = lax.dynamic_slice(jnp.pad(valid_lines, 1), (flat * 2,), (4,))
    wide = jnp.concatenate([counts[:1], jnp.repeat(counts[1:3], BR // LOOK), counts[3:]])
    rows = LINES // LOOK
    groups = lax.broadcasted_iota(jnp.int32, (18, rows + 2), 1) - 1
    pixels = jnp.clip(wide[:, None] - LOOK * groups, 0, LOOK) * LOOK
    pixels = jnp.where((groups >= 0) & (groups < rows), pixels, 0).astype(F32)
    box_pixels = sum(pixels[j : j + 16, i : i + rows] for i in range(3) for j in range(3))
    scale = 1.0 / jnp.sqrt(jnp.maximum(box_pixels, 1.0))
    core = lax.axis_index("az") % 2
    block = ((lax.axis_index("az") // 2) * 16 + lax.axis_index("rg")) * 2 + core
    own = lax.dynamic_slice(valid_lines, (block * 2,), (2,))
    col_counts = jnp.repeat(own, BR)[None, :]
    shifts = to_worker(jnp.stack([az_shift, rg_shift]))

    slave = pre(slave_raw)
    slave = lax.all_to_all(slave, "rg", 0, 0, tiled=True)
    me = lax.axis_index("rg").astype(jnp.int32)[None]
    pieces = pre_shifts(me, master_raw)
    master = [
        lax.ppermute(piece, "rg", [(r, shifted(r, shift)) for r in range(NP)])
        if any(shift)
        else piece
        for shift, piece in zip(SHIFTS, pieces)
    ]
    slave = range_compress(_range_kernel, [HBM], [slave], hf)
    slave = columns_of(slave)
    matrices = prep(h)
    master = range_compress(_range_shift_kernel, [SMEM] + [HBM] * NP, [me, *master], hf)
    master = columns_of(master)
    low, high = slave_azimuth(slave, matrices)
    from_left, from_right = halo(high, low)
    moved = resample(shifts[0], shifts[1], (from_left, low, high, from_right))

    box, side = master_looks(master, matrices, moved, col_counts)
    box = lax.ppermute(box, ALL, [(worker(b), b) for b in range(128)])
    left = lax.ppermute(side, ALL, [(worker(b), b + 1) for b in range(127)])
    right = lax.ppermute(side, ALL, [(worker(b + 1), b) for b in range(127)])
    return final(box, left, right, scale).transpose(0, 2, 1)


def solution(mesh):
    return jax.shard_map(
        local,
        mesh=mesh,
        in_specs=(
            P(None, "az", "rg"),
            P(None, "az", "rg"),
            P(),
            P(),
            P(None, ALL),
            P(None, ALL),
            P(),
        ),
        out_specs=P(None, None, ALL),
        check_vma=False,
    )
```

```python
import math

import jax
import jax.numpy as jnp
import numpy as np
from jax import lax
from jax.experimental import pallas as pl
from jax.experimental.pallas import tpu as pltpu
from jax.sharding import PartitionSpec as P


LINES = 2048
RANGE = 20000
LOOK = 8
BA = 512
BR = 64
ASH = 32
RSH = 64
NBA = 4
ALL = ("az", "rg")
NP = 16
NQ = 10
NS = 125
F32 = jnp.float32
BF16 = jnp.bfloat16


SHIFTS = sorted(
    ((dx, dz) for dx in range(4) for dz in range(4)),
    key=lambda s: -(min(s[0], 4 - s[0]) + min(s[1], 4 - s[1])),
)


def shifted(r, shift):
    return ((r // 4 + shift[1]) % 4) * 4 + (r % 4 + shift[0]) % 4


def _rot(v, angle):
    c, s = math.cos(angle), math.sin(angle)
    turns = angle / (math.pi / 4)
    eighth = round(turns)
    x, y = v
    if abs(turns - eighth) < 1e-9:
        e = eighth % 8
        if e == 0:
            return v
        if e == 2:
            return (-y, x)
        if e == 4:
            return (-x, -y)
        if e == 6:
            return (y, -x)
        h = math.sqrt(0.5)
        if e == 1:
            return ((x - y) * h, (x + y) * h)
        if e == 3:
            return (-(x + y) * h, (x - y) * h)
        if e == 5:
            return ((y - x) * h, -(x + y) * h)
        return ((x + y) * h, (y - x) * h)
    return (x * c - y * s, x * s + y * c)


def _add(a, b):
    return (a[0] + b[0], a[1] + b[1])


def _sub(a, b):
    return (a[0] - b[0], a[1] - b[1])


def _dft2(v, sign):
    return [_add(v[0], v[1]), _sub(v[0], v[1])]


def _dft4(v, sign):
    a, b = _add(v[0], v[2]), _sub(v[0], v[2])
    c, d = _add(v[1], v[3]), _sub(v[1], v[3])
    if sign < 0:
        return [_add(a, c), (b[0] + d[1], b[1] - d[0]), _sub(a, c), (b[0] - d[1], b[1] + d[0])]
    return [_add(a, c), (b[0] - d[1], b[1] + d[0]), _sub(a, c), (b[0] + d[1], b[1] - d[0])]


def _dft5(v, sign):
    c1, c2 = math.cos(2 * math.pi / 5), math.cos(4 * math.pi / 5)
    s1, s2 = sign * math.sin(2 * math.pi / 5), sign * math.sin(4 * math.pi / 5)
    a1, b1 = _add(v[1], v[4]), _sub(v[1], v[4])
    a2, b2 = _add(v[2], v[3]), _sub(v[2], v[3])
    x0 = v[0]
    y0 = (x0[0] + a1[0] + a2[0], x0[1] + a1[1] + a2[1])
    p1 = tuple(x0[i] + c1 * a1[i] + c2 * a2[i] for i in range(2))
    p2 = tuple(x0[i] + c2 * a1[i] + c1 * a2[i] for i in range(2))
    q1 = tuple(s1 * b1[i] + s2 * b2[i] for i in range(2))
    q2 = tuple(s2 * b1[i] - s1 * b2[i] for i in range(2))
    return [
        y0,
        (p1[0] - q1[1], p1[1] + q1[0]),
        (p2[0] - q2[1], p2[1] + q2[0]),
        (p2[0] + q2[1], p2[1] - q2[0]),
        (p1[0] + q1[1], p1[1] - q1[0]),
    ]


def _dft_two(v, n1, n2, first, second, sign):
    n = n1 * n2
    out = [None] * n
    mid = []
    for b in range(n2):
        col = first([v[n2 * a + b] for a in range(n1)], sign)
        mid.append([_rot(col[k], sign * 2 * math.pi * ((b * k) % n) / n) for k in range(n1)])
    for k1 in range(n1):
        row = second([mid[b][k1] for b in range(n2)], sign)
        for k2 in range(n2):
            out[k1 + n1 * k2] = row[k2]
    return out


def dft16(v, sign):
    return _dft_two(v, 4, 4, _dft4, _dft4, sign)


def dft10(v, sign):
    return _dft_two(v, 2, 5, _dft2, _dft5, sign)


def cmul(a, b):
    return (a[0] * b[0] - a[1] * b[1], a[0] * b[1] + a[1] * b[0])


def split(x):
    hi = x.astype(BF16)
    return hi, (x - hi.astype(F32)).astype(BF16)


def dot(a, b):
    return jnp.dot(a, b, preferred_element_type=F32)


def worker(block):
    y, rest = divmod(block, 32)
    c, rest = divmod(rest, 16)
    z, x = divmod(rest, 4)
    pair, core = divmod(x, 2)
    return (y * 2 + core) * 16 + z * 4 + 2 * c + (pair + z) % 2


def block_of(az, rg):
    y, core = az // 2, az % 2
    z, x = rg // 4, rg % 4
    return y * 32 + (x // 2) * 16 + z * 4 + 2 * ((x + z) % 2) + core


def _np_split(x):
    x = np.asarray(x, np.float32)
    hi = x.astype(BF16)
    return hi, (x - hi.astype(np.float32)).astype(BF16)


def _tables():
    t = {}
    two = 2 * np.pi
    q2 = np.arange(128)
    keep = (q2 < NS)[None, :]
    ang = -two * ((np.arange(NQ)[:, None] * q2[None, :]) % 1250) / 1250
    t["twb"] = np.stack([np.cos(ang) * keep, np.sin(ang) * keep], 1).astype(np.float32)
    n = np.arange(NQ)[None, :, None] * NS + q2[None, None, :]
    ang = two * ((np.arange(NP)[:, None, None] * n) % RANGE) / RANGE
    t["twc"] = np.stack([np.cos(ang), np.sin(ang)], 2).reshape(NP * NQ, 2, 128).astype(np.float32)
    ang = two * ((q2[:, None] * q2[None, :]) % NS) / NS
    both = keep & keep.T
    c, s = np.cos(ang) * both, np.sin(ang) * both
    t["fh"], t["fl"] = _np_split(np.block([[c, -s], [s, c]]))
    t["gh"], t["gl"] = _np_split(np.block([[c, s], [-s, c]]))
    k2 = np.arange(128)
    back = (-np.arange(128)) % 128
    ang = two * ((k2[:, None] * back[None, :]) % 128) / 128
    t["dft"] = np.stack([np.cos(ang), np.sin(ang)]).astype(np.float32)
    ang = two * (np.arange(16)[:, None] * back[None, :]) / LINES
    t["turn"] = np.stack([np.cos(ang), np.sin(ang)]).astype(np.float32)
    ang = np.broadcast_to(-two * np.arange(16)[:, None] / 16, (16, 128))
    t["wrap"] = np.stack([np.cos(ang), np.sin(ang)], 1).astype(np.float32)
    lane = np.arange(128)
    pick = np.zeros((24, 128), np.float32)
    for o in range(16):
        pick[o] = np.abs(lane // LOOK - o) <= 1
    pick[16] = lane < LOOK
    pick[17] = lane >= 128 - LOOK
    t["pick"] = pick
    return t


TABLES = _tables()


HBM = pl.BlockSpec(memory_space=pltpu.HBM)
VMEM = pl.BlockSpec(memory_space=pltpu.VMEM)
SMEM = pl.BlockSpec(memory_space=pltpu.SMEM)


AZIMUTH_MIB = 61
MASTER_MIB = 61


def limit(mib):
    return pltpu.CompilerParams(vmem_limit_bytes=mib << 20)


def _raw_rows(raw):
    raw = raw.transpose(2, 0, 1).reshape(1250, 2, 2, 128)
    return raw.transpose(0, 2, 1, 3).reshape(5000, 128)


def _read_lines(x_hbm, x_ref, t_ref, sem, done):
    def load(q):
        rows = pl.ds(1000 * q, 1000)
        return pltpu.make_async_copy(x_hbm.at[rows], x_ref.at[rows], sem.at[q])

    for q in range(5):
        load(q).start()
    for q in range(NQ):
        if q % 2 == 0:
            load(q // 2).wait()
        for half in range(2):
            for c in range(2):
                v = x_ref[pl.ds(500 * q + 2 * half + c, NS, stride=4), :]
                v = jnp.concatenate([v, jnp.zeros((128 - NS, 128), F32)], axis=0).T
                for k in range(8):
                    t_ref[8 * half + k, q, c] = v[16 * k : 16 * k + 16]
        done(q)


def _pre_kernel(x_hbm, o_hbm, x_ref, t_ref, sem):
    def store(q):
        at = pl.ds(2 * (q // 2), 2)
        return pltpu.make_async_copy(t_ref.at[:, at], o_hbm.at[:, at], sem.at[5 + q // 2])

    _read_lines(x_hbm, x_ref, t_ref, sem, lambda q: store(q).start() if q % 2 else None)
    for q in range(0, NQ, 2):
        store(q).wait()


def _pre_shift_kernel(me_ref, x_hbm, *refs):
    outs, (x_ref, t_ref, sem) = refs[:NP], refs[NP:]
    _read_lines(x_hbm, x_ref, t_ref, sem, lambda q: None)
    me = me_ref[0]
    stores = [
        pltpu.make_async_copy(t_ref.at[shifted(me, shift)], o_hbm, sem.at[5 + k])
        for k, (shift, o_hbm) in enumerate(zip(SHIFTS, outs))
    ]
    for store in stores:
        store.start()
    for store in stores:
        store.wait()


PRE_SCRATCH = [
    pltpu.VMEM((5000, 128), F32),
    pltpu.VMEM((NP, NQ, 2, 16, 128), F32),
    pltpu.SemaphoreType.DMA((5 + NP,)),
]


def pre(raw):
    return pl.pallas_call(
        _pre_kernel,
        in_specs=[HBM],
        out_specs=HBM,
        out_shape=jax.ShapeDtypeStruct((NP, NQ, 2, 16, 128), F32),
        scratch_shapes=PRE_SCRATCH,
        cost_estimate=pl.CostEstimate(flops=10**8, bytes_accessed=10**7, transcendentals=0),
        name="pre",
    )(_raw_rows(raw))


def pre_shifts(me, raw):
    return pl.pallas_call(
        _pre_shift_kernel,
        in_specs=[SMEM, HBM],
        out_specs=[HBM] * NP,
        out_shape=[jax.ShapeDtypeStruct((NQ, 2, 16, 128), F32)] * NP,
        scratch_shapes=PRE_SCRATCH,
        cost_estimate=pl.CostEstimate(flops=10**8, bytes_accessed=10**7, transcendentals=0),
        name="pre_shifts",
    )(me, _raw_rows(raw))


def _range_body(ready, tables, o_hbm, d_ref, x_ref, o_ref, out_sem):
    twb_ref, hf_ref, fh_ref, fl_ref, gh_ref, gl_ref, twc_ref = tables
    lane = lax.broadcasted_iota(jnp.int32, (16, 128), 1)

    def outer(q, carry):
        ready(q)
        for g in range(2):
            rows = slice(8 * g, 8 * g + 8)
            v = [(x_ref[p, q, 0, rows, :], x_ref[p, q, 1, rows, :]) for p in range(NP)]
            v = dft16(v, -1)
            for k in range(NP):
                at = k * NQ + q
                r, i = cmul(v[k], (twc_ref[at, 0:1, :], -twc_ref[at, 1:2, :]))
                d_ref[at, 0, rows, :] = r
                d_ref[at, 1, rows, :] = i
        return carry

    lax.fori_loop(0, NQ, outer, 0, unroll=2)
    ready(None)

    def middle(kp, carry):
        v = [(d_ref[kp * NQ + q, 0], d_ref[kp * NQ + q, 1]) for q in range(NQ)]
        v = dft10(v, -1)
        rows = []
        for k in range(NQ):
            r, i = cmul(v[k], (twb_ref[k, 0:1, :], twb_ref[k, 1:2, :]))
            rows.append(jnp.concatenate([r, i], axis=1))
        hi, lo = split(jnp.concatenate(rows, axis=0))
        y = dot(hi, fh_ref[...]) + dot(lo, fh_ref[...]) + dot(hi, fl_ref[...])
        rows = []
        for k in range(NQ):
            val = (y[16 * k : 16 * k + 16, :128], y[16 * k : 16 * k + 16, 128:])
            r, i = cmul(val, (hf_ref[kp * NQ + k, 0:1, :], hf_ref[kp * NQ + k, 1:2, :]))
            rows.append(jnp.concatenate([r, i], axis=1))
        hi, lo = split(jnp.concatenate(rows, axis=0))
        y = dot(hi, gh_ref[...]) + dot(lo, gh_ref[...]) + dot(hi, gl_ref[...])
        v = []
        for k in range(NQ):
            val = (y[16 * k : 16 * k + 16, :128], y[16 * k : 16 * k + 16, 128:])
            v.append(cmul(val, (twb_ref[k, 0:1, :], -twb_ref[k, 1:2, :])))
        v = dft10(v, 1)
        for q in range(NQ):
            at = kp * NQ + q
            r, i = cmul(v[q], (twc_ref[at, 0:1, :], twc_ref[at, 1:2, :]))
            d_ref[at, 0] = r
            d_ref[at, 1] = i
        return carry

    lax.fori_loop(0, NP, middle, 0, unroll=4)

    def inner(q, carry):
        for g in range(2):
            rows = slice(8 * g, 8 * g + 8)
            v = [(d_ref[k * NQ + q, 0, rows, :], d_ref[k * NQ + q, 1, rows, :]) for k in range(NP)]
            v = dft16(v, 1)
            for p in range(14):
                d_ref[p * NQ + q, 0, rows, :] = v[p][0]
                d_ref[p * NQ + q, 1, rows, :] = v[p][1]
        return carry

    lax.fori_loop(0, NQ, inner, 0, unroll=2)

    def store(part):
        at = pl.ds(32 * part, 32)
        return pltpu.make_async_copy(o_ref.at[at], o_hbm.at[at], out_sem.at[part])

    for d in range(128):
        n, a = divmod(128 * d, NS)
        for c in range(2):
            val = d_ref[n, c]
            if a:
                val = pltpu.roll(val, 128 - a, 1)
            start = NS - a
            while start < 128:
                n2 = (128 * d + start) // NS
                nxt = d_ref[n2, c]
                nxt = pltpu.roll(nxt, start % 128, 1)
                val = jnp.where(lane < start, val, nxt)
                start += NS
            o_ref[worker(d), c] = val
        if d % 32 == 31:
            store(d // 32).start()
    for part in range(4):
        store(part).wait()


def _tables_in(table_hbm, tables, sem):
    copies = [
        pltpu.make_async_copy(src, dst, sem.at[k]) for k, (src, dst) in enumerate(zip(table_hbm, tables))
    ]
    for copy in copies[::-1]:
        copy.start()
    return copies


def _range_kernel(x_hbm, *refs):
    table_hbm, o_hbm, tables, (d_ref, x_ref, o_ref, out_sem, in_sem, sem) = refs[:7], refs[7], refs[8:15], refs[15:]

    def load(q):
        return pltpu.make_async_copy(x_hbm.at[:, q], x_ref.at[:, q], in_sem.at[q])

    def ready(q):
        if q is None:
            for copy in copies[:6]:
                copy.wait()
        else:
            load(q).wait()

    copies = _tables_in(table_hbm, tables, sem)
    for q in range(NQ):
        load(q).start()
    copies[6].wait()
    _range_body(ready, tables, o_hbm, d_ref, x_ref, o_ref, out_sem)


def _range_shift_kernel(me_ref, *refs):
    parts, refs = refs[:NP], refs[NP:]
    table_hbm, o_hbm, tables, (d_ref, x_ref, o_ref, out_sem, in_sem, sem) = refs[:7], refs[7], refs[8:15], refs[15:]
    me = me_ref[0]
    loads = [
        pltpu.make_async_copy(
            part, x_ref.at[shifted(me, (4 - shift[0], 4 - shift[1]))], in_sem.at[k]
        )
        for k, (shift, part) in enumerate(zip(SHIFTS, parts))
    ]

    def ready(q):
        if q is None:
            for copy in copies[:6]:
                copy.wait()

    copies = _tables_in(table_hbm, tables, sem)
    for load in loads:
        load.start()
    for load in loads:
        load.wait()
    copies[6].wait()
    _range_body(ready, tables, o_hbm, d_ref, x_ref, o_ref, out_sem)


def range_compress(kernel, specs, operands, hf):
    t = TABLES
    tables = (t["twb"], hf, t["fh"], t["fl"], t["gh"], t["gl"], t["twc"])
    return pl.pallas_call(
        kernel,
        in_specs=specs + [HBM] * 7,
        out_specs=HBM,
        out_shape=jax.ShapeDtypeStruct((128, 2, 16, 128), F32),
        scratch_shapes=[pltpu.VMEM(x.shape, x.dtype) for x in tables]
        + [
            pltpu.VMEM((NP * NQ, 2, 16, 128), F32),
            pltpu.VMEM((NP, NQ, 2, 16, 128), F32),
            pltpu.VMEM((128, 2, 16, 128), F32),
            pltpu.SemaphoreType.DMA((4,)),
            pltpu.SemaphoreType.DMA((NP,)),
            pltpu.SemaphoreType.DMA((7,)),
        ],
        cost_estimate=pl.CostEstimate(flops=10**10, bytes_accessed=6 * 10**6, transcendentals=0),
    )(*operands, *tables)


def _dot_t(a, b):
    return lax.dot_general(
        a, b, (((1,), (1,)), ((), ())), precision=lax.Precision.HIGHEST, preferred_element_type=F32
    )


def _prep_kernel(h_ref, dft_ref, turn_ref, wrap_ref, a_ref, g_ref):
    def mul(a, b):
        return jnp.dot(a, b, precision=lax.Precision.HIGHEST, preferred_element_type=F32)

    hr, hi = h_ref[0], h_ref[1]
    dr, di = dft_ref[0], dft_ref[1]
    g = (mul(hr, dr) - mul(hi, di), mul(hr, di) + mul(hi, dr))
    r, i = cmul(g, (turn_ref[0], turn_ref[1]))
    g_ref[:, 0, :] = r
    g_ref[:, 1, :] = i
    row = lax.broadcasted_iota(jnp.int32, (128, 128), 0)
    lane = lax.broadcasted_iota(jnp.int32, (128, 128), 1)
    over = lane > row

    def body(k, carry):
        m = []
        for c in range(2):
            line = jnp.broadcast_to(g_ref[k, c : c + 1, :], (128, 128))
            m.append(pltpu.roll(line, 0, 1, stride=1, stride_axis=0))
        turned = cmul(m, (wrap_ref[k, 0:1, :], wrap_ref[k, 1:2, :]))
        re = jnp.where(over, turned[0], m[0])
        im = jnp.where(over, turned[1], m[1])
        for part, block in enumerate((re, -im)):
            cols = slice(128 * part, 128 * part + 128)
            high, low = split(block)
            a_ref[k, 0:128, cols] = high
            a_ref[k, 128:256, cols] = low
        return carry

    lax.fori_loop(0, 16, body, 0, unroll=2)


def prep(h):
    t = TABLES
    return pl.pallas_call(
        _prep_kernel,
        out_shape=jax.ShapeDtypeStruct((16, 256, 256), BF16),
        scratch_shapes=[pltpu.VMEM((16, 2, 128), F32)],
        cost_estimate=pl.CostEstimate(flops=2 * 10**9, bytes_accessed=5 * 10**6, transcendentals=0),
        name="prep",
    )(h, t["dft"], t["turn"], t["wrap"])


def _azimuth_front(x_hbm, a_hbm, e_ref, x_ref, a_ref, sem):
    def load(s):
        return pltpu.make_async_copy(x_hbm.at[:, s], x_ref.at[:, s], sem.at[s])

    matrices = pltpu.make_async_copy(a_hbm, a_ref, sem.at[8])
    for s in range(8):
        load(s).start()
    matrices.start()

    def first(s, carry):
        load(s).wait()
        for g in range(2):
            rows = slice(8 * g, 8 * g + 8)
            v = [(x_ref[a, s, 0, rows, :], x_ref[a, s, 1, rows, :]) for a in range(16)]
            v = dft16(v, -1)
            for k in range(16):
                for c in range(2):
                    at = pl.multiple_of(c * 128 + s * 16 + g * 8, 8)
                    e_ref[k, pl.ds(at, 8), :] = v[k][c]
        return carry

    lax.fori_loop(0, 8, first, 0, unroll=2)
    matrices.wait()

    def second(k, carry):
        re_hi, re_lo = split(e_ref[k, 0:128, :])
        im_hi, im_lo = split(e_ref[k, 128:256, :])

        def turned(re, im):
            straight = jnp.concatenate([re, im], axis=0)
            return jnp.concatenate([straight, jnp.concatenate([im, -re], axis=0)], axis=1)

        y = dot(a_ref[k], turned(re_hi, im_hi))
        y = y[:128] + y[128:] + dot(a_ref[k, 0:128, :], turned(re_lo, im_lo))
        e_ref[k, 0:128, :] = y[:, :128]
        e_ref[k, 128:256, :] = y[:, 128:]
        return carry

    lax.fori_loop(0, 16, second, 0, unroll=4)


AZIMUTH_SCRATCH = [
    pltpu.VMEM((16, 256, 128), F32),
    pltpu.VMEM((16, 8, 2, 16, 128), F32),
    pltpu.VMEM((16, 256, 256), BF16),
    pltpu.SemaphoreType.DMA((13,)),
]


def _azimuth_rows(e_ref, g):
    at = [pl.multiple_of(c * 128 + g * 8, 8) for c in range(2)]
    v = [(e_ref[k, pl.ds(at[0], 8), :], e_ref[k, pl.ds(at[1], 8), :]) for k in range(16)]
    return dft16(v, 1)


def _slave_kernel(x_hbm, a_hbm, left_hbm, right_hbm, left_ref, right_ref, *scratch):
    _azimuth_front(x_hbm, a_hbm, *scratch)
    e_ref, sem = scratch[0], scratch[-1]
    low = lax.broadcasted_iota(jnp.int32, (8, 128), 1) < 64
    zero = jnp.zeros((ASH, 128), F32)
    for ref in (left_ref, right_ref):
        ref[0:ASH, :] = zero
        ref[ASH + LINES :, :] = zero

    def third(g, carry):
        v = _azimuth_rows(e_ref, g)
        for a in range(16):
            rows = pl.ds(pl.multiple_of(a * 128 + g * 8 + ASH, 8), 8)
            r, i = v[a]
            left_ref[rows, :] = jnp.where(low, r, pltpu.roll(i, 64, 1))
            right_ref[rows, :] = jnp.where(low, pltpu.roll(r, 64, 1), i)
        return carry

    lax.fori_loop(0, 16, third, 0, unroll=2)
    copies = [
        pltpu.make_async_copy(right_ref, right_hbm, sem.at[10]),
        pltpu.make_async_copy(left_ref, left_hbm, sem.at[9]),
    ]
    for copy in copies:
        copy.start()
    for copy in copies:
        copy.wait()


def slave_azimuth(x, a):
    side = jax.ShapeDtypeStruct((LINES + 2 * ASH, 128), F32)
    return pl.pallas_call(
        _slave_kernel,
        in_specs=[HBM, HBM],
        out_specs=(HBM, HBM),
        out_shape=(side, side),
        scratch_shapes=[pltpu.VMEM(side.shape, F32)] * 2 + AZIMUTH_SCRATCH,
        cost_estimate=pl.CostEstimate(flops=5 * 10**9, bytes_accessed=10**7, transcendentals=0),
        compiler_params=limit(AZIMUTH_MIB),
        name="slave_azimuth",
    )(x.reshape(16, 8, 2, 16, 128), a)


def _master_kernel(x_hbm, a_hbm, o_hbm, o_ref, *scratch):
    _azimuth_front(x_hbm, a_hbm, *scratch)
    e_ref, sem = scratch[0], scratch[-1]

    def third(g, carry):
        v = _azimuth_rows(e_ref, g)
        for a in range(16):
            rows = pl.ds(pl.multiple_of(a * 128 + g * 8, 8), 8)
            o_ref[0, rows, :] = v[a][0]
            o_ref[1, rows, :] = v[a][1]
        return carry

    lax.fori_loop(0, 16, third, 0, unroll=2)
    copy = pltpu.make_async_copy(o_ref, o_hbm, sem.at[9])
    copy.start()
    copy.wait()


def master_azimuth(x, a):
    return pl.pallas_call(
        _master_kernel,
        in_specs=[HBM, HBM],
        out_specs=HBM,
        out_shape=jax.ShapeDtypeStruct((2, LINES, 128), F32),
        scratch_shapes=[pltpu.VMEM((2, LINES, 128), F32)] + AZIMUTH_SCRATCH,
        cost_estimate=pl.CostEstimate(flops=5 * 10**9, bytes_accessed=10**7, transcendentals=0),
        compiler_params=limit(MASTER_MIB),
        name="master_azimuth",
    )(x.reshape(16, 8, 2, 16, 128), a)


def _looks_kernel(shift_ref, *refs):
    packs, (m_hbm, n_ref, pick_ref, box_ref, side_ref) = refs[:4], refs[4:9]
    w_ref, m_ref, total_ref, sem = refs[9:]
    lane = lax.broadcasted_iota(jnp.int32, (64, 128), 1)
    line = lax.broadcasted_iota(jnp.int32, (64, 128), 0)
    low = lane < 64
    count = n_ref[...]

    def load(block):
        rows = pl.ds(0, BA + 2 * ASH) if block == 0 else pl.ds(block * BA + 2 * ASH, BA)
        mine = pl.ds(block * BA, BA)
        return [
            pltpu.make_async_copy(pack.at[rows], w_ref.at[k, rows], sem.at[5 * block + k])
            for k, pack in enumerate(packs)
        ] + [pltpu.make_async_copy(m_hbm.at[:, mine], m_ref.at[:, mine], sem.at[5 * block + 4])]

    for block in range(NBA):
        for copy in load(block):
            copy.start()
    for block in range(NBA):
        for copy in load(block):
            copy.wait()

        def move(t, carry):
            parts = []
            for r in range(2):
                shift = shift_ref[8 + 2 * block + r] + RSH
                first = shift // 64 + r
                second = jnp.minimum(first + 1, 3)
                s = lax.rem(shift, 64)
                rows = pl.ds(block * BA + t * 64 + ASH + shift_ref[2 * block + r], 64)
                parts.append(
                    jnp.where(
                        (lane & 63) + s < 64,
                        pltpu.roll(w_ref[first, rows, :], lax.rem(128 - s, 128), 1),
                        pltpu.roll(w_ref[second, rows, :], 64 - s, 1),
                    )
                )
            sr = jnp.where(low, parts[0], pltpu.roll(parts[1], 64, 1))
            si = jnp.where(low, pltpu.roll(parts[0], 64, 1), parts[1])
            at = pl.multiple_of(block * BA + t * 64, 64)
            r, i = m_ref[0, pl.ds(at, 64), :], m_ref[1, pl.ds(at, 64), :]
            keep = line + at < count
            cross = (r * sr + i * si, i * sr - r * si)
            for c in range(2):
                cells = jnp.where(keep, cross[c], 0.0).reshape(8, LOOK, 128).sum(axis=1)
                total_ref[pl.ds(pl.multiple_of(c * 256 + (block * 8 + t) * 8, 8), 8), :] = cells
            return carry

        lax.fori_loop(0, BA // 64, move, 0, unroll=4)
    y = _dot_t(pick_ref[...], total_ref[...])
    cell = lax.broadcasted_iota(jnp.int32, (24, 512), 1) % 256
    y = (
        y
        + jnp.where(cell == 0, 0.0, pltpu.roll(y, 1, 1))
        + jnp.where(cell == 255, 0.0, pltpu.roll(y, 511, 1))
    )
    box_ref[...] = y[:16]
    side_ref[...] = y[16:]


def looks(shifts, packs, master, counts):
    return pl.pallas_call(
        _looks_kernel,
        in_specs=[SMEM] + [HBM] * 5 + [VMEM] * 2,
        out_shape=(
            jax.ShapeDtypeStruct((16, 512), F32),
            jax.ShapeDtypeStruct((8, 512), F32),
        ),
        scratch_shapes=[
            pltpu.VMEM((4, LINES + 2 * ASH, 128), F32),
            pltpu.VMEM((2, LINES, 128), F32),
            pltpu.VMEM((512, 128), F32),
            pltpu.SemaphoreType.DMA((20,)),
        ],
        cost_estimate=pl.CostEstimate(flops=5 * 10**9, bytes_accessed=10**7, transcendentals=0),
        compiler_params=limit(61),
        name="looks",
    )(shifts, *packs, master, counts, TABLES["pick"])


def _final_kernel(box_ref, left_ref, right_ref, scale_ref, o_ref):
    row = lax.broadcasted_iota(jnp.int32, (16, 256), 0)
    for c in range(2):
        at = slice(256 * c, 256 * c + 256)
        x = box_ref[:, at]
        x = x + jnp.where(row == 0, left_ref[1:2, at], 0.0)
        x = x + jnp.where(row == 15, right_ref[0:1, at], 0.0)
        o_ref[c] = x * scale_ref[...]


def final(box, left, right, scale):
    return pl.pallas_call(
        _final_kernel,
        out_shape=jax.ShapeDtypeStruct((2, 16, 256), F32),
        compiler_params=limit(4),
        name="final",
    )(box, left, right, scale)


def to_worker(x):
    return lax.ppermute(x, ALL, [(b, worker(b)) for b in range(128)])


def halo(to_right, to_left):
    up = [(worker(b), worker(b + 1)) for b in range(127)]
    down = [(j, i) for i, j in up]
    return lax.ppermute(to_right, ALL, up), lax.ppermute(to_left, ALL, down)


def local(master_raw, slave_raw, range_ref, az_ref, az_shift, rg_shift, valid_lines):
    hf = range_ref.reshape(2, NS, NQ, NP).transpose(3, 2, 0, 1).reshape(NP * NQ, 2, NS)
    hf = jnp.pad(hf * (1.0 / RANGE), ((0, 0), (0, 0), (0, 3)))
    h = az_ref.reshape(2, 128, 16).transpose(0, 2, 1) * (1.0 / LINES)

    def columns_of(ranged):
        return lax.all_to_all(ranged, ALL, 0, 0, tiled=True)

    flat = lax.axis_index(ALL)
    counts = lax.dynamic_slice(jnp.pad(valid_lines, 1), (flat * 2,), (4,))
    wide = jnp.concatenate([counts[:1], jnp.repeat(counts[1:3], BR // LOOK), counts[3:]])
    rows = LINES // LOOK
    groups = lax.broadcasted_iota(jnp.int32, (18, rows + 2), 1) - 1
    pixels = jnp.clip(wide[:, None] - LOOK * groups, 0, LOOK) * LOOK
    pixels = jnp.where((groups >= 0) & (groups < rows), pixels, 0).astype(F32)
    box_pixels = sum(pixels[j : j + 16, i : i + rows] for i in range(3) for j in range(3))
    scale = 1.0 / jnp.sqrt(jnp.maximum(box_pixels, 1.0))
    block = block_of(lax.axis_index("az"), lax.axis_index("rg"))
    own = lax.dynamic_slice(valid_lines, (block * 2,), (2,))
    col_counts = jnp.repeat(own, BR)[None, :]
    shifts = to_worker(jnp.concatenate([az_shift.reshape(8), rg_shift.reshape(8)]))

    slave = pre(slave_raw)
    slave = lax.all_to_all(slave, "rg", 0, 0, tiled=True)
    me = lax.axis_index("rg").astype(jnp.int32)[None]
    pieces = pre_shifts(me, master_raw)
    master = [
        lax.ppermute(piece, "rg", [(r, shifted(r, shift)) for r in range(NP)])
        if any(shift)
        else piece
        for shift, piece in zip(SHIFTS, pieces)
    ]
    slave = range_compress(_range_kernel, [HBM], [slave], hf)
    slave = columns_of(slave)
    matrices = prep(h)
    master = range_compress(_range_shift_kernel, [SMEM] + [HBM] * NP, [me, *master], hf)
    master = columns_of(master)
    low, high = slave_azimuth(slave, matrices)
    from_left, from_right = halo(high, low)
    master = master_azimuth(master, matrices)
    box, side = looks(shifts, (from_left, low, high, from_right), master, col_counts)

    box = lax.ppermute(box, ALL, [(worker(b), b) for b in range(128)])
    left = lax.ppermute(side, ALL, [(worker(b), b + 1) for b in range(127)])
    right = lax.ppermute(side, ALL, [(worker(b + 1), b) for b in range(127)])
    return final(box, left, right, scale).transpose(0, 2, 1)


def solution(mesh):
    return jax.shard_map(
        local,
        mesh=mesh,
        in_specs=(
            P(None, "az", "rg"),
            P(None, "az", "rg"),
            P(),
            P(),
            P(None, ALL),
            P(None, ALL),
            P(),
        ),
        out_specs=P(None, None, ALL),
        check_vma=False,
    )
```

```python
import math

import jax
import jax.numpy as jnp
import numpy as np
from jax import lax
from jax.experimental import pallas as pl
from jax.experimental.pallas import tpu as pltpu
from jax.sharding import PartitionSpec as P


LINES = 2048
RANGE = 20000
LOOK = 8
BA = 512
BR = 64
ASH = 32
RSH = 64
NBA = 4
ALL = ("az", "rg")
NP = 16
NQ = 10
NS = 125
F32 = jnp.float32
BF16 = jnp.bfloat16


SHIFTS = sorted(
    ((dx, dz) for dx in range(4) for dz in range(4)),
    key=lambda s: -(min(s[0], 4 - s[0]) + min(s[1], 4 - s[1])),
)


def shifted(r, shift):
    return ((r // 4 + shift[1]) % 4) * 4 + (r % 4 + shift[0]) % 4


def _rot(v, angle):
    c, s = math.cos(angle), math.sin(angle)
    turns = angle / (math.pi / 4)
    eighth = round(turns)
    x, y = v
    if abs(turns - eighth) < 1e-9:
        e = eighth % 8
        if e == 0:
            return v
        if e == 2:
            return (-y, x)
        if e == 4:
            return (-x, -y)
        if e == 6:
            return (y, -x)
        h = math.sqrt(0.5)
        if e == 1:
            return ((x - y) * h, (x + y) * h)
        if e == 3:
            return (-(x + y) * h, (x - y) * h)
        if e == 5:
            return ((y - x) * h, -(x + y) * h)
        return ((x + y) * h, (y - x) * h)
    return (x * c - y * s, x * s + y * c)


def _add(a, b):
    return (a[0] + b[0], a[1] + b[1])


def _sub(a, b):
    return (a[0] - b[0], a[1] - b[1])


def _dft2(v, sign):
    return [_add(v[0], v[1]), _sub(v[0], v[1])]


def _dft4(v, sign):
    a, b = _add(v[0], v[2]), _sub(v[0], v[2])
    c, d = _add(v[1], v[3]), _sub(v[1], v[3])
    if sign < 0:
        return [_add(a, c), (b[0] + d[1], b[1] - d[0]), _sub(a, c), (b[0] - d[1], b[1] + d[0])]
    return [_add(a, c), (b[0] - d[1], b[1] + d[0]), _sub(a, c), (b[0] + d[1], b[1] - d[0])]


def _dft5(v, sign):
    c1, c2 = math.cos(2 * math.pi / 5), math.cos(4 * math.pi / 5)
    s1, s2 = sign * math.sin(2 * math.pi / 5), sign * math.sin(4 * math.pi / 5)
    a1, b1 = _add(v[1], v[4]), _sub(v[1], v[4])
    a2, b2 = _add(v[2], v[3]), _sub(v[2], v[3])
    x0 = v[0]
    y0 = (x0[0] + a1[0] + a2[0], x0[1] + a1[1] + a2[1])
    p1 = tuple(x0[i] + c1 * a1[i] + c2 * a2[i] for i in range(2))
    p2 = tuple(x0[i] + c2 * a1[i] + c1 * a2[i] for i in range(2))
    q1 = tuple(s1 * b1[i] + s2 * b2[i] for i in range(2))
    q2 = tuple(s2 * b1[i] - s1 * b2[i] for i in range(2))
    return [
        y0,
        (p1[0] - q1[1], p1[1] + q1[0]),
        (p2[0] - q2[1], p2[1] + q2[0]),
        (p2[0] + q2[1], p2[1] - q2[0]),
        (p1[0] + q1[1], p1[1] - q1[0]),
    ]


def _dft_two(v, n1, n2, first, second, sign):
    n = n1 * n2
    out = [None] * n
    mid = []
    for b in range(n2):
        col = first([v[n2 * a + b] for a in range(n1)], sign)
        mid.append([_rot(col[k], sign * 2 * math.pi * ((b * k) % n) / n) for k in range(n1)])
    for k1 in range(n1):
        row = second([mid[b][k1] for b in range(n2)], sign)
        for k2 in range(n2):
            out[k1 + n1 * k2] = row[k2]
    return out


def dft16(v, sign):
    return _dft_two(v, 4, 4, _dft4, _dft4, sign)


def dft10(v, sign):
    return _dft_two(v, 2, 5, _dft2, _dft5, sign)


def cmul(a, b):
    return (a[0] * b[0] - a[1] * b[1], a[0] * b[1] + a[1] * b[0])


def split(x):
    hi = x.astype(BF16)
    return hi, (x - hi.astype(F32)).astype(BF16)


def dot(a, b):
    return jnp.dot(a, b, preferred_element_type=F32)


def worker(block):
    y, rest = divmod(block, 32)
    c, rest = divmod(rest, 16)
    z, x = divmod(rest, 4)
    pair, core = divmod(x, 2)
    turn = (pair + z) % 2
    return (y * 2 + core) * 16 + (3 - z if c else z) * 4 + (3 - turn if c else turn)


def block_of(az, rg):
    y, core = az // 2, az % 2
    z, x = rg // 4, rg % 4
    c = x // 2
    z = z + c * (3 - 2 * z)
    turn = x + c * (3 - 2 * x)
    return y * 32 + c * 16 + z * 4 + 2 * ((turn + z) % 2) + core


def _np_split(x):
    x = np.asarray(x, np.float32)
    hi = x.astype(BF16)
    return hi, (x - hi.astype(np.float32)).astype(BF16)


def _tables():
    t = {}
    two = 2 * np.pi
    q2 = np.arange(128)
    keep = (q2 < NS)[None, :]
    ang = -two * ((np.arange(NQ)[:, None] * q2[None, :]) % 1250) / 1250
    t["twb"] = np.stack([np.cos(ang) * keep, np.sin(ang) * keep], 1).astype(np.float32)
    n = np.arange(NQ)[None, :, None] * NS + q2[None, None, :]
    ang = two * ((np.arange(NP)[:, None, None] * n) % RANGE) / RANGE
    t["twc"] = np.stack([np.cos(ang), np.sin(ang)], 2).reshape(NP * NQ, 2, 128).astype(np.float32)
    ang = two * ((q2[:, None] * q2[None, :]) % NS) / NS
    both = keep & keep.T
    c, s = np.cos(ang) * both, np.sin(ang) * both
    t["fh"], t["fl"] = _np_split(np.block([[c, -s], [s, c]]))
    t["gh"], t["gl"] = _np_split(np.block([[c, s], [-s, c]]))
    k2 = np.arange(128)
    back = (-np.arange(128)) % 128
    ang = two * ((k2[:, None] * back[None, :]) % 128) / 128
    t["dft"] = np.stack([np.cos(ang), np.sin(ang)]).astype(np.float32)
    ang = two * (np.arange(16)[:, None] * back[None, :]) / LINES
    t["turn"] = np.stack([np.cos(ang), np.sin(ang)]).astype(np.float32)
    ang = np.broadcast_to(-two * np.arange(16)[:, None] / 16, (16, 128))
    t["wrap"] = np.stack([np.cos(ang), np.sin(ang)], 1).astype(np.float32)
    lane = np.arange(128)
    pick = np.zeros((24, 128), np.float32)
    for o in range(16):
        pick[o] = np.abs(lane // LOOK - o) <= 1
    pick[16] = lane < LOOK
    pick[17] = lane >= 128 - LOOK
    t["pick"] = pick
    return t


TABLES = _tables()


HBM = pl.BlockSpec(memory_space=pltpu.HBM)
VMEM = pl.BlockSpec(memory_space=pltpu.VMEM)
SMEM = pl.BlockSpec(memory_space=pltpu.SMEM)


AZIMUTH_MIB = 48
MASTER_MIB = 52


def limit(mib):
    return pltpu.CompilerParams(vmem_limit_bytes=mib << 20)


def _raw_rows(raw):
    raw = raw.transpose(2, 0, 1).reshape(1250, 2, 2, 128)
    return raw.transpose(0, 2, 1, 3).reshape(5000, 128)


def _read_lines(x_hbm, x_ref, t_ref, sem, done):
    def load(q):
        rows = pl.ds(1000 * q, 1000)
        return pltpu.make_async_copy(x_hbm.at[rows], x_ref.at[rows], sem.at[q])

    for q in range(5):
        load(q).start()
    for q in range(NQ):
        if q % 2 == 0:
            load(q // 2).wait()
        for half in range(2):
            for c in range(2):
                v = x_ref[pl.ds(500 * q + 2 * half + c, NS, stride=4), :]
                v = jnp.concatenate([v, jnp.zeros((128 - NS, 128), F32)], axis=0).T
                for k in range(8):
                    t_ref[8 * half + k, q, c] = v[16 * k : 16 * k + 16]
        done(q)


def _pre_kernel(x_hbm, o_hbm, x_ref, t_ref, sem):
    def store(q):
        at = pl.ds(2 * (q // 2), 2)
        return pltpu.make_async_copy(t_ref.at[:, at], o_hbm.at[:, at], sem.at[5 + q // 2])

    _read_lines(x_hbm, x_ref, t_ref, sem, lambda q: store(q).start() if q % 2 else None)
    for q in range(0, NQ, 2):
        store(q).wait()


def _pre_shift_kernel(me_ref, x_hbm, *refs):
    outs, (x_ref, t_ref, sem) = refs[:NP], refs[NP:]
    _read_lines(x_hbm, x_ref, t_ref, sem, lambda q: None)
    me = me_ref[0]
    stores = [
        pltpu.make_async_copy(t_ref.at[shifted(me, shift)], o_hbm, sem.at[5 + k])
        for k, (shift, o_hbm) in enumerate(zip(SHIFTS, outs))
    ]
    for store in stores:
        store.start()
    for store in stores:
        store.wait()


PRE_SCRATCH = [
    pltpu.VMEM((5000, 128), F32),
    pltpu.VMEM((NP, NQ, 2, 16, 128), F32),
    pltpu.SemaphoreType.DMA((5 + NP,)),
]


def pre(raw):
    return pl.pallas_call(
        _pre_kernel,
        in_specs=[HBM],
        out_specs=HBM,
        out_shape=jax.ShapeDtypeStruct((NP, NQ, 2, 16, 128), F32),
        scratch_shapes=PRE_SCRATCH,
        cost_estimate=pl.CostEstimate(flops=10**8, bytes_accessed=10**7, transcendentals=0),
        name="pre",
    )(_raw_rows(raw))


def pre_shifts(me, raw):
    return pl.pallas_call(
        _pre_shift_kernel,
        in_specs=[SMEM, HBM],
        out_specs=[HBM] * NP,
        out_shape=[jax.ShapeDtypeStruct((NQ, 2, 16, 128), F32)] * NP,
        scratch_shapes=PRE_SCRATCH,
        cost_estimate=pl.CostEstimate(flops=10**8, bytes_accessed=10**7, transcendentals=0),
        name="pre_shifts",
    )(me, _raw_rows(raw))


def _range_body(ready, tables, o_hbm, d_ref, x_ref, o_ref, out_sem):
    twb_ref, hf_ref, fh_ref, fl_ref, gh_ref, gl_ref, twc_ref = tables
    lane = lax.broadcasted_iota(jnp.int32, (16, 128), 1)

    def outer(q, carry):
        ready(q)
        for g in range(2):
            rows = slice(8 * g, 8 * g + 8)
            v = [(x_ref[p, q, 0, rows, :], x_ref[p, q, 1, rows, :]) for p in range(NP)]
            v = dft16(v, -1)
            for k in range(NP):
                at = k * NQ + q
                r, i = cmul(v[k], (twc_ref[at, 0:1, :], -twc_ref[at, 1:2, :]))
                d_ref[at, 0, rows, :] = r
                d_ref[at, 1, rows, :] = i
        return carry

    lax.fori_loop(0, NQ, outer, 0, unroll=2)
    ready(None)

    def middle(kp, carry):
        v = [(d_ref[kp * NQ + q, 0], d_ref[kp * NQ + q, 1]) for q in range(NQ)]
        v = dft10(v, -1)
        rows = []
        for k in range(NQ):
            r, i = cmul(v[k], (twb_ref[k, 0:1, :], twb_ref[k, 1:2, :]))
            rows.append(jnp.concatenate([r, i], axis=1))
        hi, lo = split(jnp.concatenate(rows, axis=0))
        y = dot(hi, fh_ref[...]) + dot(lo, fh_ref[...]) + dot(hi, fl_ref[...])
        rows = []
        for k in range(NQ):
            val = (y[16 * k : 16 * k + 16, :128], y[16 * k : 16 * k + 16, 128:])
            r, i = cmul(val, (hf_ref[kp * NQ + k, 0:1, :], hf_ref[kp * NQ + k, 1:2, :]))
            rows.append(jnp.concatenate([r, i], axis=1))
        hi, lo = split(jnp.concatenate(rows, axis=0))
        y = dot(hi, gh_ref[...]) + dot(lo, gh_ref[...]) + dot(hi, gl_ref[...])
        v = []
        for k in range(NQ):
            val = (y[16 * k : 16 * k + 16, :128], y[16 * k : 16 * k + 16, 128:])
            v.append(cmul(val, (twb_ref[k, 0:1, :], -twb_ref[k, 1:2, :])))
        v = dft10(v, 1)
        for q in range(NQ):
            at = kp * NQ + q
            r, i = cmul(v[q], (twc_ref[at, 0:1, :], twc_ref[at, 1:2, :]))
            d_ref[at, 0] = r
            d_ref[at, 1] = i
        return carry

    lax.fori_loop(0, NP, middle, 0, unroll=8)

    def inner(q, carry):
        for g in range(2):
            rows = slice(8 * g, 8 * g + 8)
            v = [(d_ref[k * NQ + q, 0, rows, :], d_ref[k * NQ + q, 1, rows, :]) for k in range(NP)]
            v = dft16(v, 1)
            for p in range(14):
                d_ref[p * NQ + q, 0, rows, :] = v[p][0]
                d_ref[p * NQ + q, 1, rows, :] = v[p][1]
        return carry

    lax.fori_loop(0, NQ, inner, 0, unroll=2)

    def store(part):
        at = pl.ds(32 * part, 32)
        return pltpu.make_async_copy(o_ref.at[at], o_hbm.at[at], out_sem.at[part])

    for d in range(128):
        n, a = divmod(128 * d, NS)
        for c in range(2):
            val = d_ref[n, c]
            if a:
                val = pltpu.roll(val, 128 - a, 1)
            start = NS - a
            while start < 128:
                n2 = (128 * d + start) // NS
                nxt = d_ref[n2, c]
                nxt = pltpu.roll(nxt, start % 128, 1)
                val = jnp.where(lane < start, val, nxt)
                start += NS
            o_ref[worker(d), c] = val
        if d % 32 == 31:
            store(d // 32).start()
    for part in range(4):
        store(part).wait()


def _tables_in(table_hbm, tables, sem):
    copies = [
        pltpu.make_async_copy(src, dst, sem.at[k]) for k, (src, dst) in enumerate(zip(table_hbm, tables))
    ]
    for copy in copies[::-1]:
        copy.start()
    return copies


def _range_kernel(x_hbm, *refs):
    table_hbm, o_hbm, tables, (d_ref, x_ref, o_ref, out_sem, in_sem, sem) = refs[:7], refs[7], refs[8:15], refs[15:]

    def load(q):
        return pltpu.make_async_copy(x_hbm.at[:, q], x_ref.at[:, q], in_sem.at[q])

    def ready(q):
        if q is None:
            for copy in copies[:6]:
                copy.wait()
        else:
            load(q).wait()

    copies = _tables_in(table_hbm, tables, sem)
    for q in range(NQ):
        load(q).start()
    copies[6].wait()
    _range_body(ready, tables, o_hbm, d_ref, x_ref, o_ref, out_sem)


def _range_shift_kernel(me_ref, *refs):
    parts, refs = refs[:NP], refs[NP:]
    table_hbm, o_hbm, tables, (d_ref, x_ref, o_ref, out_sem, in_sem, sem) = refs[:7], refs[7], refs[8:15], refs[15:]
    me = me_ref[0]
    loads = [
        pltpu.make_async_copy(
            part, x_ref.at[shifted(me, (4 - shift[0], 4 - shift[1]))], in_sem.at[k]
        )
        for k, (shift, part) in enumerate(zip(SHIFTS, parts))
    ]

    def ready(q):
        if q is None:
            for copy in copies[:6]:
                copy.wait()

    copies = _tables_in(table_hbm, tables, sem)
    for load in loads:
        load.start()
    for load in loads:
        load.wait()
    copies[6].wait()
    _range_body(ready, tables, o_hbm, d_ref, x_ref, o_ref, out_sem)


def range_compress(kernel, specs, operands, hf):
    t = TABLES
    tables = (t["twb"], hf, t["fh"], t["fl"], t["gh"], t["gl"], t["twc"])
    return pl.pallas_call(
        kernel,
        in_specs=specs + [HBM] * 7,
        out_specs=HBM,
        out_shape=jax.ShapeDtypeStruct((128, 2, 16, 128), F32),
        scratch_shapes=[pltpu.VMEM(x.shape, x.dtype) for x in tables]
        + [
            pltpu.VMEM((NP * NQ, 2, 16, 128), F32),
            pltpu.VMEM((NP, NQ, 2, 16, 128), F32),
            pltpu.VMEM((128, 2, 16, 128), F32),
            pltpu.SemaphoreType.DMA((4,)),
            pltpu.SemaphoreType.DMA((NP,)),
            pltpu.SemaphoreType.DMA((7,)),
        ],
        cost_estimate=pl.CostEstimate(flops=10**10, bytes_accessed=6 * 10**6, transcendentals=0),
    )(*operands, *tables)


def _dot_t(a, b):
    return lax.dot_general(
        a, b, (((1,), (1,)), ((), ())), precision=lax.Precision.HIGHEST, preferred_element_type=F32
    )


def _prep_kernel(h_ref, dft_ref, turn_ref, wrap_ref, a_ref, g_ref):
    def mul(a, b):
        return jnp.dot(a, b, precision=lax.Precision.HIGHEST, preferred_element_type=F32)

    hr, hi = h_ref[0], h_ref[1]
    dr, di = dft_ref[0], dft_ref[1]
    g = (mul(hr, dr) - mul(hi, di), mul(hr, di) + mul(hi, dr))
    r, i = cmul(g, (turn_ref[0], turn_ref[1]))
    g_ref[:, 0, :] = r
    g_ref[:, 1, :] = i
    row = lax.broadcasted_iota(jnp.int32, (128, 128), 0)
    lane = lax.broadcasted_iota(jnp.int32, (128, 128), 1)
    over = lane > row

    def body(k, carry):
        m = []
        for c in range(2):
            line = jnp.broadcast_to(g_ref[k, c : c + 1, :], (128, 128))
            m.append(pltpu.roll(line, 0, 1, stride=1, stride_axis=0))
        turned = cmul(m, (wrap_ref[k, 0:1, :], wrap_ref[k, 1:2, :]))
        re = jnp.where(over, turned[0], m[0])
        im = jnp.where(over, turned[1], m[1])
        for part, block in enumerate((re, -im)):
            cols = slice(128 * part, 128 * part + 128)
            high, low = split(block)
            a_ref[k, 0:128, cols] = high
            a_ref[k, 128:256, cols] = low
        return carry

    lax.fori_loop(0, 16, body, 0, unroll=2)


def prep(h):
    t = TABLES
    return pl.pallas_call(
        _prep_kernel,
        out_shape=jax.ShapeDtypeStruct((16, 256, 256), BF16),
        scratch_shapes=[pltpu.VMEM((16, 2, 128), F32)],
        cost_estimate=pl.CostEstimate(flops=2 * 10**9, bytes_accessed=5 * 10**6, transcendentals=0),
        name="prep",
    )(h, t["dft"], t["turn"], t["wrap"])


def _azimuth_front(x_hbm, a_hbm, e_ref, a_ref, sem, x_ref=None):
    def load(s):
        return pltpu.make_async_copy(x_hbm.at[:, s], x_ref.at[:, s], sem.at[s])

    matrices = pltpu.make_async_copy(a_hbm, a_ref, sem.at[8])
    staged = x_ref is not None
    if staged:
        for s in range(8):
            load(s).start()
    else:
        x_ref = x_hbm
    matrices.start()

    def first(s, carry):
        if staged:
            load(s).wait()
        for g in range(2):
            rows = slice(8 * g, 8 * g + 8)
            v = [(x_ref[a, s, 0, rows, :], x_ref[a, s, 1, rows, :]) for a in range(16)]
            v = dft16(v, -1)
            for k in range(16):
                for c in range(2):
                    at = pl.multiple_of(c * 128 + s * 16 + g * 8, 8)
                    e_ref[k, pl.ds(at, 8), :] = v[k][c]
        return carry

    lax.fori_loop(0, 8, first, 0, unroll=2)
    matrices.wait()

    def second(k, carry):
        re_hi, re_lo = split(e_ref[k, 0:128, :])
        im_hi, im_lo = split(e_ref[k, 128:256, :])

        def turned(re, im):
            straight = jnp.concatenate([re, im], axis=0)
            return jnp.concatenate([straight, jnp.concatenate([im, -re], axis=0)], axis=1)

        y = dot(a_ref[k], turned(re_hi, im_hi))
        y = y[:128] + y[128:] + dot(a_ref[k, 0:128, :], turned(re_lo, im_lo))
        e_ref[k, 0:128, :] = y[:, :128]
        e_ref[k, 128:256, :] = y[:, 128:]
        return carry

    lax.fori_loop(0, 16, second, 0, unroll=4)


AZIMUTH_SCRATCH = [
    pltpu.VMEM((16, 256, 128), F32),
    pltpu.VMEM((16, 256, 256), BF16),
    pltpu.SemaphoreType.DMA((13,)),
]
STAGED_SCRATCH = AZIMUTH_SCRATCH + [pltpu.VMEM((16, 8, 2, 16, 128), F32)]


def _azimuth_rows(e_ref, g):
    at = [pl.multiple_of(c * 128 + g * 8, 8) for c in range(2)]
    v = [(e_ref[k, pl.ds(at[0], 8), :], e_ref[k, pl.ds(at[1], 8), :]) for k in range(16)]
    return dft16(v, 1)


def _slave_kernel(x_ref, a_hbm, left_hbm, right_hbm, left_ref, right_ref, *scratch):
    _azimuth_front(x_ref, a_hbm, *scratch)
    e_ref, sem = scratch[0], scratch[2]
    low = lax.broadcasted_iota(jnp.int32, (8, 128), 1) < 64
    zero = jnp.zeros((ASH, 128), F32)
    for ref in (left_ref, right_ref):
        ref[0:ASH, :] = zero
        ref[ASH + LINES :, :] = zero

    def third(g, carry):
        v = _azimuth_rows(e_ref, g)
        for a in range(16):
            rows = pl.ds(pl.multiple_of(a * 128 + g * 8 + ASH, 8), 8)
            r, i = v[a]
            left_ref[rows, :] = jnp.where(low, r, pltpu.roll(i, 64, 1))
            right_ref[rows, :] = jnp.where(low, pltpu.roll(r, 64, 1), i)
        return carry

    lax.fori_loop(0, 16, third, 0, unroll=2)
    copies = [
        pltpu.make_async_copy(right_ref, right_hbm, sem.at[10]),
        pltpu.make_async_copy(left_ref, left_hbm, sem.at[9]),
    ]
    for copy in copies:
        copy.start()
    for copy in copies:
        copy.wait()


def slave_azimuth(x, a):
    side = jax.ShapeDtypeStruct((LINES + 2 * ASH, 128), F32)
    return pl.pallas_call(
        _slave_kernel,
        in_specs=[VMEM, HBM],
        out_specs=(HBM, HBM),
        out_shape=(side, side),
        scratch_shapes=[pltpu.VMEM(side.shape, F32)] * 2 + AZIMUTH_SCRATCH,
        cost_estimate=pl.CostEstimate(flops=5 * 10**9, bytes_accessed=10**7, transcendentals=0),
        compiler_params=limit(AZIMUTH_MIB),
        name="slave_azimuth",
    )(x.reshape(16, 8, 2, 16, 128), a)


def _master_kernel(x_hbm, a_hbm, o_hbm, o_ref, *scratch):
    _azimuth_front(x_hbm, a_hbm, *scratch)
    e_ref, sem = scratch[0], scratch[2]

    def third(g, carry):
        v = _azimuth_rows(e_ref, g)
        for a in range(16):
            rows = pl.ds(pl.multiple_of(a * 128 + g * 8, 8), 8)
            o_ref[0, rows, :] = v[a][0]
            o_ref[1, rows, :] = v[a][1]
        return carry

    lax.fori_loop(0, 16, third, 0, unroll=2)
    copy = pltpu.make_async_copy(o_ref, o_hbm, sem.at[9])
    copy.start()
    copy.wait()


def master_azimuth(x, a):
    return pl.pallas_call(
        _master_kernel,
        in_specs=[HBM, HBM],
        out_specs=HBM,
        out_shape=jax.ShapeDtypeStruct((2, LINES, 128), F32),
        scratch_shapes=[pltpu.VMEM((2, LINES, 128), F32)] + STAGED_SCRATCH,
        cost_estimate=pl.CostEstimate(flops=5 * 10**9, bytes_accessed=10**7, transcendentals=0),
        compiler_params=limit(MASTER_MIB),
        name="master_azimuth",
    )(x.reshape(16, 8, 2, 16, 128), a)


def _looks_kernel(shift_ref, *refs):
    packs, (m_hbm, n_ref, pick_ref, box_ref, side_ref) = refs[:4], refs[4:9]
    w_ref, m_ref, total_ref, sem = refs[9:]
    lane = lax.broadcasted_iota(jnp.int32, (64, 128), 1)
    line = lax.broadcasted_iota(jnp.int32, (64, 128), 0)
    low = lane < 64
    count = n_ref[...]

    def load(block):
        rows = pl.ds(0, BA + 2 * ASH) if block == 0 else pl.ds(block * BA + 2 * ASH, BA)
        mine = pl.ds(block * BA, BA)
        return [
            pltpu.make_async_copy(pack.at[rows], w_ref.at[k, rows], sem.at[5 * block + k])
            for k, pack in enumerate(packs)
        ] + [pltpu.make_async_copy(m_hbm.at[:, mine], m_ref.at[:, mine], sem.at[5 * block + 4])]

    for block in range(NBA):
        for copy in load(block):
            copy.start()
    for block in range(NBA):
        for copy in load(block):
            copy.wait()

        def move(t, carry):
            parts = []
            for r in range(2):
                shift = shift_ref[8 + 2 * block + r] + RSH
                first = shift // 64 + r
                second = jnp.minimum(first + 1, 3)
                s = lax.rem(shift, 64)
                rows = pl.ds(block * BA + t * 64 + ASH + shift_ref[2 * block + r], 64)
                parts.append(
                    jnp.where(
                        (lane & 63) + s < 64,
                        pltpu.roll(w_ref[first, rows, :], lax.rem(128 - s, 128), 1),
                        pltpu.roll(w_ref[second, rows, :], 64 - s, 1),
                    )
                )
            sr = jnp.where(low, parts[0], pltpu.roll(parts[1], 64, 1))
            si = jnp.where(low, pltpu.roll(parts[0], 64, 1), parts[1])
            at = pl.multiple_of(block * BA + t * 64, 64)
            r, i = m_ref[0, pl.ds(at, 64), :], m_ref[1, pl.ds(at, 64), :]
            keep = line + at < count
            cross = (r * sr + i * si, i * sr - r * si)
            for c in range(2):
                cells = jnp.where(keep, cross[c], 0.0).reshape(8, LOOK, 128).sum(axis=1)
                total_ref[pl.ds(pl.multiple_of(c * 256 + (block * 8 + t) * 8, 8), 8), :] = cells
            return carry

        lax.fori_loop(0, BA // 64, move, 0, unroll=4)
    y = _dot_t(pick_ref[...], total_ref[...])
    cell = lax.broadcasted_iota(jnp.int32, (24, 512), 1) % 256
    y = (
        y
        + jnp.where(cell == 0, 0.0, pltpu.roll(y, 1, 1))
        + jnp.where(cell == 255, 0.0, pltpu.roll(y, 511, 1))
    )
    box_ref[...] = y[:16]
    side_ref[...] = y[16:]


def looks(shifts, packs, master, counts):
    return pl.pallas_call(
        _looks_kernel,
        in_specs=[SMEM] + [HBM] * 5 + [VMEM] * 2,
        out_shape=(
            jax.ShapeDtypeStruct((16, 512), F32),
            jax.ShapeDtypeStruct((8, 512), F32),
        ),
        scratch_shapes=[
            pltpu.VMEM((4, LINES + 2 * ASH, 128), F32),
            pltpu.VMEM((2, LINES, 128), F32),
            pltpu.VMEM((512, 128), F32),
            pltpu.SemaphoreType.DMA((20,)),
        ],
        cost_estimate=pl.CostEstimate(flops=5 * 10**9, bytes_accessed=10**7, transcendentals=0),
        compiler_params=limit(50),
        name="looks",
    )(shifts, *packs, master, counts, TABLES["pick"])


def _final_kernel(box_ref, left_ref, right_ref, scale_ref, o_ref):
    row = lax.broadcasted_iota(jnp.int32, (16, 256), 0)
    for c in range(2):
        at = slice(256 * c, 256 * c + 256)
        x = box_ref[:, at]
        x = x + jnp.where(row == 0, left_ref[1:2, at], 0.0)
        x = x + jnp.where(row == 15, right_ref[0:1, at], 0.0)
        o_ref[c] = x * scale_ref[...]


def final(box, left, right, scale):
    return pl.pallas_call(
        _final_kernel,
        out_shape=jax.ShapeDtypeStruct((2, 16, 256), F32),
        compiler_params=limit(4),
        name="final",
    )(box, left, right, scale)


def to_worker(x):
    return lax.ppermute(x, ALL, [(b, worker(b)) for b in range(128)])


def halo(to_right, to_left):
    up = [(worker(b), worker(b + 1)) for b in range(127)]
    down = [(j, i) for i, j in up]
    return lax.ppermute(to_right, ALL, up), lax.ppermute(to_left, ALL, down)


def local(master_raw, slave_raw, range_ref, az_ref, az_shift, rg_shift, valid_lines):
    hf = range_ref.reshape(2, NS, NQ, NP).transpose(3, 2, 0, 1).reshape(NP * NQ, 2, NS)
    hf = jnp.pad(hf * (1.0 / RANGE), ((0, 0), (0, 0), (0, 3)))
    h = az_ref.reshape(2, 128, 16).transpose(0, 2, 1) * (1.0 / LINES)

    def columns_of(ranged):
        return lax.all_to_all(ranged, ALL, 0, 0, tiled=True)

    flat = lax.axis_index(ALL)
    counts = lax.dynamic_slice(jnp.pad(valid_lines, 1), (flat * 2,), (4,))
    wide = jnp.concatenate([counts[:1], jnp.repeat(counts[1:3], BR // LOOK), counts[3:]])
    rows = LINES // LOOK
    groups = lax.broadcasted_iota(jnp.int32, (18, rows + 2), 1) - 1
    pixels = jnp.clip(wide[:, None] - LOOK * groups, 0, LOOK) * LOOK
    pixels = jnp.where((groups >= 0) & (groups < rows), pixels, 0).astype(F32)
    box_pixels = sum(pixels[j : j + 16, i : i + rows] for i in range(3) for j in range(3))
    scale = 1.0 / jnp.sqrt(jnp.maximum(box_pixels, 1.0))
    block = block_of(lax.axis_index("az"), lax.axis_index("rg"))
    own = lax.dynamic_slice(valid_lines, (block * 2,), (2,))
    col_counts = jnp.repeat(own, BR)[None, :]
    shifts = to_worker(jnp.concatenate([az_shift.reshape(8), rg_shift.reshape(8)]))

    slave = pre(slave_raw)
    slave = lax.all_to_all(slave, "rg", 0, 0, tiled=True)
    me = lax.axis_index("rg").astype(jnp.int32)[None]
    pieces = pre_shifts(me, master_raw)
    master = [
        lax.ppermute(piece, "rg", [(r, shifted(r, shift)) for r in range(NP)])
        if any(shift)
        else piece
        for shift, piece in zip(SHIFTS, pieces)
    ]
    slave = range_compress(_range_kernel, [HBM], [slave], hf)
    slave = columns_of(slave)
    matrices = prep(h)
    master = range_compress(_range_shift_kernel, [SMEM] + [HBM] * NP, [me, *master], hf)
    master = columns_of(master)
    low, high = slave_azimuth(slave, matrices)
    from_left, from_right = halo(high, low)
    master = master_azimuth(master, matrices)
    box, side = looks(shifts, (from_left, low, high, from_right), master, col_counts)

    box = lax.ppermute(box, ALL, [(worker(b), b) for b in range(128)])
    left = lax.ppermute(side, ALL, [(worker(b), b + 1) for b in range(127)])
    right = lax.ppermute(side, ALL, [(worker(b + 1), b) for b in range(127)])
    return final(box, left, right, scale).transpose(0, 2, 1)


def solution(mesh):
    return jax.shard_map(
        local,
        mesh=mesh,
        in_specs=(
            P(None, "az", "rg"),
            P(None, "az", "rg"),
            P(),
            P(),
            P(None, ALL),
            P(None, ALL),
            P(),
        ),
        out_specs=P(None, None, ALL),
        check_vma=False,
    )
```

```python
import math

import jax
import jax.numpy as jnp
import numpy as np
from jax import lax
from jax.experimental import pallas as pl
from jax.experimental.pallas import tpu as pltpu
from jax.sharding import PartitionSpec as P


LINES = 2048
RANGE = 20000
LOOK = 8
BA = 512
BR = 64
ASH = 32
RSH = 64
NBA = 4
ALL = ("az", "rg")
NP = 16
NQ = 10
NS = 125
F32 = jnp.float32
BF16 = jnp.bfloat16


SHIFTS = sorted(
    ((dx, dz) for dx in range(4) for dz in range(4)),
    key=lambda s: min(s[0], 4 - s[0]) + min(s[1], 4 - s[1]),
)


def shifted(r, shift):
    return ((r // 4 + shift[1]) % 4) * 4 + (r % 4 + shift[0]) % 4


def _rot(v, angle):
    c, s = math.cos(angle), math.sin(angle)
    turns = angle / (math.pi / 4)
    eighth = round(turns)
    x, y = v
    if abs(turns - eighth) < 1e-9:
        e = eighth % 8
        if e == 0:
            return v
        if e == 2:
            return (-y, x)
        if e == 4:
            return (-x, -y)
        if e == 6:
            return (y, -x)
        h = math.sqrt(0.5)
        if e == 1:
            return ((x - y) * h, (x + y) * h)
        if e == 3:
            return (-(x + y) * h, (x - y) * h)
        if e == 5:
            return ((y - x) * h, -(x + y) * h)
        return ((x + y) * h, (y - x) * h)
    return (x * c - y * s, x * s + y * c)


def _add(a, b):
    return (a[0] + b[0], a[1] + b[1])


def _sub(a, b):
    return (a[0] - b[0], a[1] - b[1])


def _dft2(v, sign):
    return [_add(v[0], v[1]), _sub(v[0], v[1])]


def _dft4(v, sign):
    a, b = _add(v[0], v[2]), _sub(v[0], v[2])
    c, d = _add(v[1], v[3]), _sub(v[1], v[3])
    if sign < 0:
        return [_add(a, c), (b[0] + d[1], b[1] - d[0]), _sub(a, c), (b[0] - d[1], b[1] + d[0])]
    return [_add(a, c), (b[0] - d[1], b[1] + d[0]), _sub(a, c), (b[0] + d[1], b[1] - d[0])]


def _dft5(v, sign):
    c1, c2 = math.cos(2 * math.pi / 5), math.cos(4 * math.pi / 5)
    s1, s2 = sign * math.sin(2 * math.pi / 5), sign * math.sin(4 * math.pi / 5)
    a1, b1 = _add(v[1], v[4]), _sub(v[1], v[4])
    a2, b2 = _add(v[2], v[3]), _sub(v[2], v[3])
    x0 = v[0]
    y0 = (x0[0] + a1[0] + a2[0], x0[1] + a1[1] + a2[1])
    p1 = tuple(x0[i] + c1 * a1[i] + c2 * a2[i] for i in range(2))
    p2 = tuple(x0[i] + c2 * a1[i] + c1 * a2[i] for i in range(2))
    q1 = tuple(s1 * b1[i] + s2 * b2[i] for i in range(2))
    q2 = tuple(s2 * b1[i] - s1 * b2[i] for i in range(2))
    return [
        y0,
        (p1[0] - q1[1], p1[1] + q1[0]),
        (p2[0] - q2[1], p2[1] + q2[0]),
        (p2[0] + q2[1], p2[1] - q2[0]),
        (p1[0] + q1[1], p1[1] - q1[0]),
    ]


def _dft_two(v, n1, n2, first, second, sign):
    n = n1 * n2
    out = [None] * n
    mid = []
    for b in range(n2):
        col = first([v[n2 * a + b] for a in range(n1)], sign)
        mid.append([_rot(col[k], sign * 2 * math.pi * ((b * k) % n) / n) for k in range(n1)])
    for k1 in range(n1):
        row = second([mid[b][k1] for b in range(n2)], sign)
        for k2 in range(n2):
            out[k1 + n1 * k2] = row[k2]
    return out


def dft16(v, sign):
    return _dft_two(v, 4, 4, _dft4, _dft4, sign)


def dft10(v, sign):
    return _dft_two(v, 2, 5, _dft2, _dft5, sign)


def cmul(a, b):
    return (a[0] * b[0] - a[1] * b[1], a[0] * b[1] + a[1] * b[0])


def split(x):
    hi = x.astype(BF16)
    return hi, (x - hi.astype(F32)).astype(BF16)


def dot(a, b):
    return jnp.dot(a, b, preferred_element_type=F32)


def worker(block):
    y, rest = divmod(block, 32)
    c, rest = divmod(rest, 16)
    z, x = divmod(rest, 4)
    pair, core = divmod(x, 2)
    turn = (pair + z) % 2
    return (y * 2 + core) * 16 + (3 - z if c else z) * 4 + (3 - turn if c else turn)


def block_of(az, rg):
    y, core = az // 2, az % 2
    z, x = rg // 4, rg % 4
    c = x // 2
    z = z + c * (3 - 2 * z)
    turn = x + c * (3 - 2 * x)
    return y * 32 + c * 16 + z * 4 + 2 * ((turn + z) % 2) + core


def _np_split(x):
    x = np.asarray(x, np.float32)
    hi = x.astype(BF16)
    return hi, (x - hi.astype(np.float32)).astype(BF16)


def _tables():
    t = {}
    two = 2 * np.pi
    q2 = np.arange(128)
    keep = (q2 < NS)[None, :]
    ang = -two * ((np.arange(NQ)[:, None] * q2[None, :]) % 1250) / 1250
    t["twb"] = np.stack([np.cos(ang) * keep, np.sin(ang) * keep], 1).astype(np.float32)
    n = np.arange(NQ)[None, :, None] * NS + q2[None, None, :]
    ang = two * ((np.arange(NP)[:, None, None] * n) % RANGE) / RANGE
    t["twc"] = np.stack([np.cos(ang), np.sin(ang)], 2).reshape(NP * NQ, 2, 128).astype(np.float32)
    ang = two * ((q2[:, None] * q2[None, :]) % NS) / NS
    both = keep & keep.T
    c, s = np.cos(ang) * both, np.sin(ang) * both
    t["fh"], t["fl"] = _np_split(np.block([[c, -s], [s, c]]))
    t["gh"], t["gl"] = _np_split(np.block([[c, s], [-s, c]]))
    k2 = np.arange(128)
    back = (-np.arange(128)) % 128
    ang = two * ((k2[:, None] * back[None, :]) % 128) / 128
    t["dft"] = np.stack([np.cos(ang), np.sin(ang)]).astype(np.float32)
    ang = two * (np.arange(16)[:, None] * back[None, :]) / LINES
    t["turn"] = np.stack([np.cos(ang), np.sin(ang)]).astype(np.float32)
    ang = np.broadcast_to(-two * np.arange(16)[:, None] / 16, (16, 128))
    t["wrap"] = np.stack([np.cos(ang), np.sin(ang)], 1).astype(np.float32)
    lane = np.arange(128)
    pick = np.zeros((24, 128), np.float32)
    for o in range(16):
        pick[o] = np.abs(lane // LOOK - o) <= 1
    pick[16] = lane < LOOK
    pick[17] = lane >= 128 - LOOK
    t["pick"] = pick
    return t


TABLES = _tables()


HBM = pl.BlockSpec(memory_space=pltpu.HBM)
VMEM = pl.BlockSpec(memory_space=pltpu.VMEM)
SMEM = pl.BlockSpec(memory_space=pltpu.SMEM)


AZIMUTH_MIB = 48
MASTER_MIB = 52


def limit(mib):
    return pltpu.CompilerParams(vmem_limit_bytes=mib << 20)


def _raw_rows(raw):
    raw = raw.transpose(2, 0, 1).reshape(1250, 2, 2, 128)
    return raw.transpose(0, 2, 1, 3).reshape(5000, 128)


def _read_lines(x_hbm, x_ref, t_ref, sem, done):
    def load(q):
        rows = pl.ds(1000 * q, 1000)
        return pltpu.make_async_copy(x_hbm.at[rows], x_ref.at[rows], sem.at[q])

    for q in range(5):
        load(q).start()
    for q in range(NQ):
        if q % 2 == 0:
            load(q // 2).wait()
        for half in range(2):
            for c in range(2):
                v = x_ref[pl.ds(500 * q + 2 * half + c, NS, stride=4), :]
                v = jnp.concatenate([v, jnp.zeros((128 - NS, 128), F32)], axis=0).T
                for k in range(8):
                    t_ref[8 * half + k, q, c] = v[16 * k : 16 * k + 16]
        done(q)


def _pre_kernel(x_hbm, o_hbm, x_ref, t_ref, sem):
    def store(q):
        at = pl.ds(2 * (q // 2), 2)
        return pltpu.make_async_copy(t_ref.at[:, at], o_hbm.at[:, at], sem.at[5 + q // 2])

    _read_lines(x_hbm, x_ref, t_ref, sem, lambda q: store(q).start() if q % 2 else None)
    for q in range(0, NQ, 2):
        store(q).wait()


def _pre_shift_kernel(me_ref, x_hbm, *refs):
    outs, (x_ref, t_ref, sem) = refs[:NP], refs[NP:]
    _read_lines(x_hbm, x_ref, t_ref, sem, lambda q: None)
    me = me_ref[0]
    stores = [
        pltpu.make_async_copy(t_ref.at[shifted(me, shift)], o_hbm, sem.at[5 + k])
        for k, (shift, o_hbm) in enumerate(zip(SHIFTS, outs))
    ]
    for store in stores:
        store.start()
    for store in stores:
        store.wait()


PRE_SCRATCH = [
    pltpu.VMEM((5000, 128), F32),
    pltpu.VMEM((NP, NQ, 2, 16, 128), F32),
    pltpu.SemaphoreType.DMA((5 + NP,)),
]


def pre(raw):
    return pl.pallas_call(
        _pre_kernel,
        in_specs=[HBM],
        out_specs=HBM,
        out_shape=jax.ShapeDtypeStruct((NP, NQ, 2, 16, 128), F32),
        scratch_shapes=PRE_SCRATCH,
        cost_estimate=pl.CostEstimate(flops=10**8, bytes_accessed=10**7, transcendentals=0),
        name="pre",
    )(_raw_rows(raw))


def pre_shifts(me, raw):
    return pl.pallas_call(
        _pre_shift_kernel,
        in_specs=[SMEM, HBM],
        out_specs=[HBM] * NP,
        out_shape=[jax.ShapeDtypeStruct((NQ, 2, 16, 128), F32)] * NP,
        scratch_shapes=PRE_SCRATCH,
        cost_estimate=pl.CostEstimate(flops=10**8, bytes_accessed=10**7, transcendentals=0),
        name="pre_shifts",
    )(me, _raw_rows(raw))


def _range_body(ready, tables, o_hbm, d_ref, x_ref, o_ref, out_sem):
    twb_ref, hf_ref, fh_ref, fl_ref, gh_ref, gl_ref, twc_ref = tables
    lane = lax.broadcasted_iota(jnp.int32, (16, 128), 1)

    def outer(q, carry):
        ready(q)
        for g in range(2):
            rows = slice(8 * g, 8 * g + 8)
            v = [(x_ref[p, q, 0, rows, :], x_ref[p, q, 1, rows, :]) for p in range(NP)]
            v = dft16(v, -1)
            for k in range(NP):
                at = k * NQ + q
                r, i = cmul(v[k], (twc_ref[at, 0:1, :], -twc_ref[at, 1:2, :]))
                d_ref[at, 0, rows, :] = r
                d_ref[at, 1, rows, :] = i
        return carry

    lax.fori_loop(0, NQ, outer, 0, unroll=2)
    ready(None)

    def middle(kp, carry):
        v = [(d_ref[kp * NQ + q, 0], d_ref[kp * NQ + q, 1]) for q in range(NQ)]
        v = dft10(v, -1)
        rows = []
        for k in range(NQ):
            r, i = cmul(v[k], (twb_ref[k, 0:1, :], twb_ref[k, 1:2, :]))
            rows.append(jnp.concatenate([r, i], axis=1))
        hi, lo = split(jnp.concatenate(rows, axis=0))
        y = dot(hi, fh_ref[...]) + dot(lo, fh_ref[...]) + dot(hi, fl_ref[...])
        rows = []
        for k in range(NQ):
            val = (y[16 * k : 16 * k + 16, :128], y[16 * k : 16 * k + 16, 128:])
            r, i = cmul(val, (hf_ref[kp * NQ + k, 0:1, :], hf_ref[kp * NQ + k, 1:2, :]))
            rows.append(jnp.concatenate([r, i], axis=1))
        hi, lo = split(jnp.concatenate(rows, axis=0))
        y = dot(hi, gh_ref[...]) + dot(lo, gh_ref[...]) + dot(hi, gl_ref[...])
        v = []
        for k in range(NQ):
            val = (y[16 * k : 16 * k + 16, :128], y[16 * k : 16 * k + 16, 128:])
            v.append(cmul(val, (twb_ref[k, 0:1, :], -twb_ref[k, 1:2, :])))
        v = dft10(v, 1)
        for q in range(NQ):
            at = kp * NQ + q
            r, i = cmul(v[q], (twc_ref[at, 0:1, :], twc_ref[at, 1:2, :]))
            d_ref[at, 0] = r
            d_ref[at, 1] = i
        return carry

    lax.fori_loop(0, NP, middle, 0, unroll=8)

    def inner(q, carry):
        for g in range(2):
            rows = slice(8 * g, 8 * g + 8)
            v = [(d_ref[k * NQ + q, 0, rows, :], d_ref[k * NQ + q, 1, rows, :]) for k in range(NP)]
            v = dft16(v, 1)
            for p in range(14):
                d_ref[p * NQ + q, 0, rows, :] = v[p][0]
                d_ref[p * NQ + q, 1, rows, :] = v[p][1]
        return carry

    lax.fori_loop(0, NQ, inner, 0, unroll=2)

    def store(part):
        at = pl.ds(32 * part, 32)
        return pltpu.make_async_copy(o_ref.at[at], o_hbm.at[at], out_sem.at[part])

    for d in range(128):
        n, a = divmod(128 * d, NS)
        for c in range(2):
            val = d_ref[n, c]
            if a:
                val = pltpu.roll(val, 128 - a, 1)
            start = NS - a
            while start < 128:
                n2 = (128 * d + start) // NS
                nxt = d_ref[n2, c]
                nxt = pltpu.roll(nxt, start % 128, 1)
                val = jnp.where(lane < start, val, nxt)
                start += NS
            o_ref[worker(d), c] = val
        if d % 32 == 31:
            store(d // 32).start()
    for part in range(4):
        store(part).wait()


def _tables_in(table_hbm, tables, sem):
    copies = [
        pltpu.make_async_copy(src, dst, sem.at[k]) for k, (src, dst) in enumerate(zip(table_hbm, tables))
    ]
    for copy in copies[::-1]:
        copy.start()
    return copies


def _range_kernel(x_hbm, *refs):
    table_hbm, o_hbm, tables, (d_ref, x_ref, o_ref, out_sem, in_sem, sem) = refs[:7], refs[7], refs[8:15], refs[15:]

    def load(q):
        return pltpu.make_async_copy(x_hbm.at[:, q], x_ref.at[:, q], in_sem.at[q])

    def ready(q):
        if q is None:
            for copy in copies[:6]:
                copy.wait()
        else:
            load(q).wait()

    copies = _tables_in(table_hbm, tables, sem)
    for q in range(NQ):
        load(q).start()
    copies[6].wait()
    _range_body(ready, tables, o_hbm, d_ref, x_ref, o_ref, out_sem)


def _range_shift_kernel(me_ref, *refs):
    parts, refs = refs[:NP], refs[NP:]
    table_hbm, o_hbm, tables, (d_ref, x_ref, o_ref, out_sem, in_sem, sem) = refs[:7], refs[7], refs[8:15], refs[15:]
    me = me_ref[0]
    loads = [
        pltpu.make_async_copy(
            part, x_ref.at[shifted(me, (4 - shift[0], 4 - shift[1]))], in_sem.at[k]
        )
        for k, (shift, part) in enumerate(zip(SHIFTS, parts))
    ]

    def ready(q):
        if q is None:
            for copy in copies[:6]:
                copy.wait()

    copies = _tables_in(table_hbm, tables, sem)
    for load in loads:
        load.start()
    for load in loads:
        load.wait()
    copies[6].wait()
    _range_body(ready, tables, o_hbm, d_ref, x_ref, o_ref, out_sem)


def range_compress(kernel, specs, operands, hf):
    t = TABLES
    tables = (t["twb"], hf, t["fh"], t["fl"], t["gh"], t["gl"], t["twc"])
    return pl.pallas_call(
        kernel,
        in_specs=specs + [HBM] * 7,
        out_specs=HBM,
        out_shape=jax.ShapeDtypeStruct((128, 2, 16, 128), F32),
        scratch_shapes=[pltpu.VMEM(x.shape, x.dtype) for x in tables]
        + [
            pltpu.VMEM((NP * NQ, 2, 16, 128), F32),
            pltpu.VMEM((NP, NQ, 2, 16, 128), F32),
            pltpu.VMEM((128, 2, 16, 128), F32),
            pltpu.SemaphoreType.DMA((4,)),
            pltpu.SemaphoreType.DMA((NP,)),
            pltpu.SemaphoreType.DMA((7,)),
        ],
        cost_estimate=pl.CostEstimate(flops=10**10, bytes_accessed=6 * 10**6, transcendentals=0),
    )(*operands, *tables)


def _dot_t(a, b):
    return lax.dot_general(
        a, b, (((1,), (1,)), ((), ())), precision=lax.Precision.HIGHEST, preferred_element_type=F32
    )


def _prep_kernel(h_ref, dft_ref, turn_ref, wrap_ref, a_ref, g_ref):
    def mul(a, b):
        return jnp.dot(a, b, precision=lax.Precision.HIGHEST, preferred_element_type=F32)

    hr, hi = h_ref[0], h_ref[1]
    dr, di = dft_ref[0], dft_ref[1]
    g = (mul(hr, dr) - mul(hi, di), mul(hr, di) + mul(hi, dr))
    r, i = cmul(g, (turn_ref[0], turn_ref[1]))
    g_ref[:, 0, :] = r
    g_ref[:, 1, :] = i
    row = lax.broadcasted_iota(jnp.int32, (128, 128), 0)
    lane = lax.broadcasted_iota(jnp.int32, (128, 128), 1)
    over = lane > row

    def body(k, carry):
        m = []
        for c in range(2):
            line = jnp.broadcast_to(g_ref[k, c : c + 1, :], (128, 128))
            m.append(pltpu.roll(line, 0, 1, stride=1, stride_axis=0))
        turned = cmul(m, (wrap_ref[k, 0:1, :], wrap_ref[k, 1:2, :]))
        re = jnp.where(over, turned[0], m[0])
        im = jnp.where(over, turned[1], m[1])
        for part, block in enumerate((re, -im)):
            cols = slice(128 * part, 128 * part + 128)
            high, low = split(block)
            a_ref[k, 0:128, cols] = high
            a_ref[k, 128:256, cols] = low
        return carry

    lax.fori_loop(0, 16, body, 0, unroll=2)


def prep(h):
    t = TABLES
    return pl.pallas_call(
        _prep_kernel,
        out_shape=jax.ShapeDtypeStruct((16, 256, 256), BF16),
        scratch_shapes=[pltpu.VMEM((16, 2, 128), F32)],
        cost_estimate=pl.CostEstimate(flops=2 * 10**9, bytes_accessed=5 * 10**6, transcendentals=0),
        name="prep",
    )(h, t["dft"], t["turn"], t["wrap"])


def _azimuth_front(x_hbm, a_hbm, e_ref, a_ref, sem, x_ref=None):
    def load(s):
        return pltpu.make_async_copy(x_hbm.at[:, s], x_ref.at[:, s], sem.at[s])

    matrices = pltpu.make_async_copy(a_hbm, a_ref, sem.at[8])
    staged = x_ref is not None
    if staged:
        for s in range(8):
            load(s).start()
    else:
        x_ref = x_hbm
    matrices.start()

    def first(s, carry):
        if staged:
            load(s).wait()
        for g in range(2):
            rows = slice(8 * g, 8 * g + 8)
            v = [(x_ref[a, s, 0, rows, :], x_ref[a, s, 1, rows, :]) for a in range(16)]
            v = dft16(v, -1)
            for k in range(16):
                for c in range(2):
                    at = pl.multiple_of(c * 128 + s * 16 + g * 8, 8)
                    e_ref[k, pl.ds(at, 8), :] = v[k][c]
        return carry

    lax.fori_loop(0, 8, first, 0, unroll=2)
    matrices.wait()

    def second(k, carry):
        re_hi, re_lo = split(e_ref[k, 0:128, :])
        im_hi, im_lo = split(e_ref[k, 128:256, :])

        def turned(re, im):
            straight = jnp.concatenate([re, im], axis=0)
            return jnp.concatenate([straight, jnp.concatenate([im, -re], axis=0)], axis=1)

        y = dot(a_ref[k], turned(re_hi, im_hi))
        y = y[:128] + y[128:] + dot(a_ref[k, 0:128, :], turned(re_lo, im_lo))
        e_ref[k, 0:128, :] = y[:, :128]
        e_ref[k, 128:256, :] = y[:, 128:]
        return carry

    lax.fori_loop(0, 16, second, 0, unroll=4)


AZIMUTH_SCRATCH = [
    pltpu.VMEM((16, 256, 128), F32),
    pltpu.VMEM((16, 256, 256), BF16),
    pltpu.SemaphoreType.DMA((13,)),
]
STAGED_SCRATCH = AZIMUTH_SCRATCH + [pltpu.VMEM((16, 8, 2, 16, 128), F32)]


def _azimuth_rows(e_ref, g):
    at = [pl.multiple_of(c * 128 + g * 8, 8) for c in range(2)]
    v = [(e_ref[k, pl.ds(at[0], 8), :], e_ref[k, pl.ds(at[1], 8), :]) for k in range(16)]
    return dft16(v, 1)


def _slave_kernel(x_ref, a_hbm, left_hbm, right_hbm, left_ref, right_ref, *scratch):
    _azimuth_front(x_ref, a_hbm, *scratch)
    e_ref, sem = scratch[0], scratch[2]
    low = lax.broadcasted_iota(jnp.int32, (8, 128), 1) < 64
    zero = jnp.zeros((ASH, 128), F32)
    for ref in (left_ref, right_ref):
        ref[0:ASH, :] = zero
        ref[ASH + LINES :, :] = zero

    def third(g, carry):
        v = _azimuth_rows(e_ref, g)
        for a in range(16):
            rows = pl.ds(pl.multiple_of(a * 128 + g * 8 + ASH, 8), 8)
            r, i = v[a]
            left_ref[rows, :] = jnp.where(low, r, pltpu.roll(i, 64, 1))
            right_ref[rows, :] = jnp.where(low, pltpu.roll(r, 64, 1), i)
        return carry

    lax.fori_loop(0, 16, third, 0, unroll=2)
    copies = [
        pltpu.make_async_copy(right_ref, right_hbm, sem.at[10]),
        pltpu.make_async_copy(left_ref, left_hbm, sem.at[9]),
    ]
    for copy in copies:
        copy.start()
    for copy in copies:
        copy.wait()


def slave_azimuth(x, a):
    side = jax.ShapeDtypeStruct((LINES + 2 * ASH, 128), F32)
    return pl.pallas_call(
        _slave_kernel,
        in_specs=[VMEM, HBM],
        out_specs=(HBM, HBM),
        out_shape=(side, side),
        scratch_shapes=[pltpu.VMEM(side.shape, F32)] * 2 + AZIMUTH_SCRATCH,
        cost_estimate=pl.CostEstimate(flops=5 * 10**9, bytes_accessed=10**7, transcendentals=0),
        compiler_params=limit(AZIMUTH_MIB),
        name="slave_azimuth",
    )(x.reshape(16, 8, 2, 16, 128), a)


def _master_kernel(x_hbm, a_hbm, o_hbm, o_ref, *scratch):
    _azimuth_front(x_hbm, a_hbm, *scratch)
    e_ref, sem = scratch[0], scratch[2]

    def third(g, carry):
        v = _azimuth_rows(e_ref, g)
        for a in range(16):
            rows = pl.ds(pl.multiple_of(a * 128 + g * 8, 8), 8)
            o_ref[0, rows, :] = v[a][0]
            o_ref[1, rows, :] = v[a][1]
        return carry

    lax.fori_loop(0, 16, third, 0, unroll=2)
    copy = pltpu.make_async_copy(o_ref, o_hbm, sem.at[9])
    copy.start()
    copy.wait()


def master_azimuth(x, a):
    return pl.pallas_call(
        _master_kernel,
        in_specs=[HBM, HBM],
        out_specs=HBM,
        out_shape=jax.ShapeDtypeStruct((2, LINES, 128), F32),
        scratch_shapes=[pltpu.VMEM((2, LINES, 128), F32)] + STAGED_SCRATCH,
        cost_estimate=pl.CostEstimate(flops=5 * 10**9, bytes_accessed=10**7, transcendentals=0),
        compiler_params=limit(MASTER_MIB),
        name="master_azimuth",
    )(x.reshape(16, 8, 2, 16, 128), a)


def _looks_kernel(shift_ref, *refs):
    packs, (m_hbm, n_ref, pick_ref, box_ref, side_ref) = refs[:4], refs[4:9]
    w_ref, m_ref, total_ref, sem = refs[9:]
    lane = lax.broadcasted_iota(jnp.int32, (64, 128), 1)
    line = lax.broadcasted_iota(jnp.int32, (64, 128), 0)
    low = lane < 64
    count = n_ref[...]

    def load(block):
        rows = pl.ds(0, BA + 2 * ASH) if block == 0 else pl.ds(block * BA + 2 * ASH, BA)
        mine = pl.ds(block * BA, BA)
        return [
            pltpu.make_async_copy(pack.at[rows], w_ref.at[k, rows], sem.at[5 * block + k])
            for k, pack in enumerate(packs)
        ] + [pltpu.make_async_copy(m_hbm.at[:, mine], m_ref.at[:, mine], sem.at[5 * block + 4])]

    for block in range(NBA):
        for copy in load(block):
            copy.start()
    for block in range(NBA):
        for copy in load(block):
            copy.wait()

        def move(t, carry):
            parts = []
            for r in range(2):
                shift = shift_ref[8 + 2 * block + r] + RSH
                first = shift // 64 + r
                second = jnp.minimum(first + 1, 3)
                s = lax.rem(shift, 64)
                rows = pl.ds(block * BA + t * 64 + ASH + shift_ref[2 * block + r], 64)
                parts.append(
                    jnp.where(
                        (lane & 63) + s < 64,
                        pltpu.roll(w_ref[first, rows, :], lax.rem(128 - s, 128), 1),
                        pltpu.roll(w_ref[second, rows, :], 64 - s, 1),
                    )
                )
            sr = jnp.where(low, parts[0], pltpu.roll(parts[1], 64, 1))
            si = jnp.where(low, pltpu.roll(parts[0], 64, 1), parts[1])
            at = pl.multiple_of(block * BA + t * 64, 64)
            r, i = m_ref[0, pl.ds(at, 64), :], m_ref[1, pl.ds(at, 64), :]
            keep = line + at < count
            cross = (r * sr + i * si, i * sr - r * si)
            for c in range(2):
                cells = jnp.where(keep, cross[c], 0.0).reshape(8, LOOK, 128).sum(axis=1)
                total_ref[pl.ds(pl.multiple_of(c * 256 + (block * 8 + t) * 8, 8), 8), :] = cells
            return carry

        lax.fori_loop(0, BA // 64, move, 0, unroll=4)
    y = _dot_t(pick_ref[...], total_ref[...])
    cell = lax.broadcasted_iota(jnp.int32, (24, 512), 1) % 256
    y = (
        y
        + jnp.where(cell == 0, 0.0, pltpu.roll(y, 1, 1))
        + jnp.where(cell == 255, 0.0, pltpu.roll(y, 511, 1))
    )
    box_ref[...] = y[:16]
    side_ref[...] = y[16:]


def looks(shifts, packs, master, counts):
    return pl.pallas_call(
        _looks_kernel,
        in_specs=[SMEM] + [HBM] * 5 + [VMEM] * 2,
        out_shape=(
            jax.ShapeDtypeStruct((16, 512), F32),
            jax.ShapeDtypeStruct((8, 512), F32),
        ),
        scratch_shapes=[
            pltpu.VMEM((4, LINES + 2 * ASH, 128), F32),
            pltpu.VMEM((2, LINES, 128), F32),
            pltpu.VMEM((512, 128), F32),
            pltpu.SemaphoreType.DMA((20,)),
        ],
        cost_estimate=pl.CostEstimate(flops=5 * 10**9, bytes_accessed=10**7, transcendentals=0),
        compiler_params=limit(50),
        name="looks",
    )(shifts, *packs, master, counts, TABLES["pick"])


def _merge_kernel(core_ref, box_ref, side_ref, o_ref):
    row = lax.broadcasted_iota(jnp.int32, (16, 512), 0)
    first = core_ref[0] == 0
    facing = jnp.where(first, side_ref[0:1, :], side_ref[1:2, :])
    o_ref[...] = box_ref[...] + jnp.where(row == jnp.where(first, 15, 0), facing, 0.0)


def merge(core, box, side):
    return pl.pallas_call(
        _merge_kernel,
        in_specs=[SMEM, VMEM, VMEM],
        out_shape=jax.ShapeDtypeStruct((16, 512), F32),
        compiler_params=limit(4),
        name="merge",
    )(core, box, side)


def _final_kernel(odd_ref, box_ref, outer_ref, scale_ref, o_ref):
    row = lax.broadcasted_iota(jnp.int32, (16, 256), 0)
    odd = odd_ref[0] == 1
    at = jnp.where(odd, 15, 0)
    for c in range(2):
        cells = slice(256 * c, 256 * c + 256)
        outer = jnp.where(odd, outer_ref[0:1, cells], outer_ref[1:2, cells])
        o_ref[c] = (box_ref[:, cells] + jnp.where(row == at, outer, 0.0)) * scale_ref[...]


def final(odd, box, outer, scale):
    return pl.pallas_call(
        _final_kernel,
        in_specs=[SMEM, VMEM, VMEM, VMEM],
        out_shape=jax.ShapeDtypeStruct((2, 16, 256), F32),
        compiler_params=limit(4),
        name="final",
    )(odd, box, outer, scale)


def to_worker(x):
    return lax.ppermute(x, ALL, [(b, worker(b)) for b in range(128)])


def halo(to_right, to_left):
    up = [(worker(b), worker(b + 1)) for b in range(127)]
    down = [(j, i) for i, j in up]
    return lax.ppermute(to_right, ALL, up), lax.ppermute(to_left, ALL, down)


def local(master_raw, slave_raw, range_ref, az_ref, az_shift, rg_shift, valid_lines):
    hf = range_ref.reshape(2, NS, NQ, NP).transpose(3, 2, 0, 1).reshape(NP * NQ, 2, NS)
    hf = jnp.pad(hf * (1.0 / RANGE), ((0, 0), (0, 0), (0, 3)))
    h = az_ref.reshape(2, 128, 16).transpose(0, 2, 1) * (1.0 / LINES)

    def columns_of(ranged):
        return lax.all_to_all(ranged, ALL, 0, 0, tiled=True)

    flat = lax.axis_index(ALL)
    counts = lax.dynamic_slice(jnp.pad(valid_lines, 1), (flat * 2,), (4,))
    wide = jnp.concatenate([counts[:1], jnp.repeat(counts[1:3], BR // LOOK), counts[3:]])
    rows = LINES // LOOK
    groups = lax.broadcasted_iota(jnp.int32, (18, rows + 2), 1) - 1
    pixels = jnp.clip(wide[:, None] - LOOK * groups, 0, LOOK) * LOOK
    pixels = jnp.where((groups >= 0) & (groups < rows), pixels, 0).astype(F32)
    box_pixels = sum(pixels[j : j + 16, i : i + rows] for i in range(3) for j in range(3))
    scale = 1.0 / jnp.sqrt(jnp.maximum(box_pixels, 1.0))
    block = block_of(lax.axis_index("az"), lax.axis_index("rg"))
    own = lax.dynamic_slice(valid_lines, (block * 2,), (2,))
    col_counts = jnp.repeat(own, BR)[None, :]
    shifts = to_worker(jnp.concatenate([az_shift.reshape(8), rg_shift.reshape(8)]))

    slave = pre(slave_raw)
    slave = lax.all_to_all(slave, "rg", 0, 0, tiled=True)
    me = lax.axis_index("rg").astype(jnp.int32)[None]
    pieces = pre_shifts(me, master_raw)
    master = [
        lax.ppermute(piece, "rg", [(r, shifted(r, shift)) for r in range(NP)])
        if any(shift)
        else piece
        for shift, piece in zip(SHIFTS, pieces)
    ]
    slave = range_compress(_range_kernel, [HBM], [slave], hf)
    slave = columns_of(slave)
    matrices = prep(h)
    master = range_compress(_range_shift_kernel, [SMEM] + [HBM] * NP, [me, *master], hf)
    master = columns_of(master)
    low, high = slave_azimuth(slave, matrices)
    from_left, from_right = halo(high, low)
    master = master_azimuth(master, matrices)
    box, side = looks(shifts, (from_left, low, high, from_right), master, col_counts)

    core = (lax.axis_index("az") % 2).astype(jnp.int32)[None]
    odd = (lax.axis_index("rg") % 2).astype(jnp.int32)[None]
    facing = lax.ppermute(side, ALL, [(worker(b), worker(b ^ 1)) for b in range(128)])
    outer = lax.ppermute(
        side,
        ALL,
        [(worker(b - 1), b) for b in range(2, 128, 2)]
        + [(worker(b + 1), b) for b in range(1, 126, 2)],
    )
    box = merge(core, box, facing)
    box = lax.ppermute(box, ALL, [(worker(b), b) for b in range(128)])
    return final(odd, box, outer, scale).transpose(0, 2, 1)


def solution(mesh):
    return jax.shard_map(
        local,
        mesh=mesh,
        in_specs=(
            P(None, "az", "rg"),
            P(None, "az", "rg"),
            P(),
            P(),
            P(None, ALL),
            P(None, ALL),
            P(),
        ),
        out_specs=P(None, None, ALL),
        check_vma=False,
    )
```

```python
import math

import jax
import jax.numpy as jnp
import numpy as np
from jax import lax
from jax.experimental import pallas as pl
from jax.experimental.pallas import tpu as pltpu
from jax.sharding import PartitionSpec as P


LINES = 2048
RANGE = 20000
LOOK = 8
BA = 512
BR = 64
ASH = 32
RSH = 64
NBA = 4
ALL = ("az", "rg")
NP = 16
NQ = 10
NS = 125
F32 = jnp.float32
BF16 = jnp.bfloat16


SHIFTS = [
    (0, 0), (1, 0), (0, 1), (3, 0), (0, 3), (2, 0), (0, 2), (1, 1), (3, 3),
    (1, 3), (3, 1), (2, 1), (1, 2), (2, 3), (3, 2), (2, 2),
]


def shifted(r, shift):
    return ((r // 4 + shift[1]) % 4) * 4 + (r % 4 + shift[0]) % 4


def _rot(v, angle):
    c, s = math.cos(angle), math.sin(angle)
    turns = angle / (math.pi / 4)
    eighth = round(turns)
    x, y = v
    if abs(turns - eighth) < 1e-9:
        e = eighth % 8
        if e == 0:
            return v
        if e == 2:
            return (-y, x)
        if e == 4:
            return (-x, -y)
        if e == 6:
            return (y, -x)
        h = math.sqrt(0.5)
        if e == 1:
            return ((x - y) * h, (x + y) * h)
        if e == 3:
            return (-(x + y) * h, (x - y) * h)
        if e == 5:
            return ((y - x) * h, -(x + y) * h)
        return ((x + y) * h, (y - x) * h)
    return (x * c - y * s, x * s + y * c)


def _add(a, b):
    return (a[0] + b[0], a[1] + b[1])


def _sub(a, b):
    return (a[0] - b[0], a[1] - b[1])


def _dft2(v, sign):
    return [_add(v[0], v[1]), _sub(v[0], v[1])]


def _dft4(v, sign):
    a, b = _add(v[0], v[2]), _sub(v[0], v[2])
    c, d = _add(v[1], v[3]), _sub(v[1], v[3])
    if sign < 0:
        return [_add(a, c), (b[0] + d[1], b[1] - d[0]), _sub(a, c), (b[0] - d[1], b[1] + d[0])]
    return [_add(a, c), (b[0] - d[1], b[1] + d[0]), _sub(a, c), (b[0] + d[1], b[1] - d[0])]


def _dft5(v, sign):
    c1, c2 = math.cos(2 * math.pi / 5), math.cos(4 * math.pi / 5)
    s1, s2 = sign * math.sin(2 * math.pi / 5), sign * math.sin(4 * math.pi / 5)
    a1, b1 = _add(v[1], v[4]), _sub(v[1], v[4])
    a2, b2 = _add(v[2], v[3]), _sub(v[2], v[3])
    x0 = v[0]
    y0 = (x0[0] + a1[0] + a2[0], x0[1] + a1[1] + a2[1])
    p1 = tuple(x0[i] + c1 * a1[i] + c2 * a2[i] for i in range(2))
    p2 = tuple(x0[i] + c2 * a1[i] + c1 * a2[i] for i in range(2))
    q1 = tuple(s1 * b1[i] + s2 * b2[i] for i in range(2))
    q2 = tuple(s2 * b1[i] - s1 * b2[i] for i in range(2))
    return [
        y0,
        (p1[0] - q1[1], p1[1] + q1[0]),
        (p2[0] - q2[1], p2[1] + q2[0]),
        (p2[0] + q2[1], p2[1] - q2[0]),
        (p1[0] + q1[1], p1[1] - q1[0]),
    ]


def _dft_two(v, n1, n2, first, second, sign):
    n = n1 * n2
    out = [None] * n
    mid = []
    for b in range(n2):
        col = first([v[n2 * a + b] for a in range(n1)], sign)
        mid.append([_rot(col[k], sign * 2 * math.pi * ((b * k) % n) / n) for k in range(n1)])
    for k1 in range(n1):
        row = second([mid[b][k1] for b in range(n2)], sign)
        for k2 in range(n2):
            out[k1 + n1 * k2] = row[k2]
    return out


def dft16(v, sign):
    return _dft_two(v, 4, 4, _dft4, _dft4, sign)


def dft10(v, sign):
    return _dft_two(v, 2, 5, _dft2, _dft5, sign)


def cmul(a, b):
    return (a[0] * b[0] - a[1] * b[1], a[0] * b[1] + a[1] * b[0])


def split(x):
    hi = x.astype(BF16)
    return hi, (x - hi.astype(F32)).astype(BF16)


def dot(a, b):
    return jnp.dot(a, b, preferred_element_type=F32)


def worker(block):
    y, rest = divmod(block, 32)
    c, rest = divmod(rest, 16)
    z, x = divmod(rest, 4)
    pair, core = divmod(x, 2)
    turn = (pair + z) % 2
    return (y * 2 + core) * 16 + (3 - z if c else z) * 4 + (3 - turn if c else turn)


def block_of(az, rg):
    y, core = az // 2, az % 2
    z, x = rg // 4, rg % 4
    c = x // 2
    z = z + c * (3 - 2 * z)
    turn = x + c * (3 - 2 * x)
    return y * 32 + c * 16 + z * 4 + 2 * ((turn + z) % 2) + core


def _np_split(x):
    x = np.asarray(x, np.float32)
    hi = x.astype(BF16)
    return hi, (x - hi.astype(np.float32)).astype(BF16)


def _tables():
    t = {}
    two = 2 * np.pi
    q2 = np.arange(128)
    keep = (q2 < NS)[None, :]
    ang = -two * ((np.arange(NQ)[:, None] * q2[None, :]) % 1250) / 1250
    t["twb"] = np.stack([np.cos(ang) * keep, np.sin(ang) * keep], 1).astype(np.float32)
    n = np.arange(NQ)[None, :, None] * NS + q2[None, None, :]
    ang = two * ((np.arange(NP)[:, None, None] * n) % RANGE) / RANGE
    t["twc"] = np.stack([np.cos(ang), np.sin(ang)], 2).reshape(NP * NQ, 2, 128).astype(np.float32)
    ang = two * ((q2[:, None] * q2[None, :]) % NS) / NS
    both = keep & keep.T
    c, s = np.cos(ang) * both, np.sin(ang) * both
    t["fh"], t["fl"] = _np_split(np.block([[c, -s], [s, c]]))
    t["gh"], t["gl"] = _np_split(np.block([[c, s], [-s, c]]))
    k2 = np.arange(128)
    back = (-np.arange(128)) % 128
    ang = two * ((k2[:, None] * back[None, :]) % 128) / 128
    t["dft"] = np.stack([np.cos(ang), np.sin(ang)]).astype(np.float32)
    ang = two * (np.arange(16)[:, None] * back[None, :]) / LINES
    t["turn"] = np.stack([np.cos(ang), np.sin(ang)]).astype(np.float32)
    ang = np.broadcast_to(-two * np.arange(16)[:, None] / 16, (16, 128))
    t["wrap"] = np.stack([np.cos(ang), np.sin(ang)], 1).astype(np.float32)
    lane = np.arange(128)
    pick = np.zeros((24, 128), np.float32)
    for o in range(16):
        pick[o] = np.abs(lane // LOOK - o) <= 1
    pick[16] = lane < LOOK
    pick[17] = lane >= 128 - LOOK
    t["pick"] = pick
    return t


TABLES = _tables()


HBM = pl.BlockSpec(memory_space=pltpu.HBM)
VMEM = pl.BlockSpec(memory_space=pltpu.VMEM)
SMEM = pl.BlockSpec(memory_space=pltpu.SMEM)


AZIMUTH_MIB = 48
MASTER_MIB = 52


def limit(mib):
    return pltpu.CompilerParams(vmem_limit_bytes=mib << 20)


def _raw_rows(raw):
    raw = raw.transpose(2, 0, 1).reshape(1250, 2, 2, 128)
    return raw.transpose(0, 2, 1, 3).reshape(5000, 128)


def _read_lines(x_hbm, x_ref, t_ref, sem, done):
    def load(q):
        rows = pl.ds(1000 * q, 1000)
        return pltpu.make_async_copy(x_hbm.at[rows], x_ref.at[rows], sem.at[q])

    for q in range(5):
        load(q).start()
    for q in range(NQ):
        if q % 2 == 0:
            load(q // 2).wait()
        for half in range(2):
            for c in range(2):
                v = x_ref[pl.ds(500 * q + 2 * half + c, NS, stride=4), :]
                v = jnp.concatenate([v, jnp.zeros((128 - NS, 128), F32)], axis=0).T
                for k in range(8):
                    t_ref[8 * half + k, q, c] = v[16 * k : 16 * k + 16]
        done(q)


def _pre_kernel(x_hbm, o_hbm, x_ref, t_ref, sem):
    def store(q):
        at = pl.ds(2 * (q // 2), 2)
        return pltpu.make_async_copy(t_ref.at[:, at], o_hbm.at[:, at], sem.at[5 + q // 2])

    _read_lines(x_hbm, x_ref, t_ref, sem, lambda q: store(q).start() if q % 2 else None)
    for q in range(0, NQ, 2):
        store(q).wait()


def _pre_shift_kernel(me_ref, x_hbm, *refs):
    outs, (x_ref, t_ref, sem) = refs[:NP], refs[NP:]
    _read_lines(x_hbm, x_ref, t_ref, sem, lambda q: None)
    me = me_ref[0]
    stores = [
        pltpu.make_async_copy(t_ref.at[shifted(me, shift)], o_hbm, sem.at[5 + k])
        for k, (shift, o_hbm) in enumerate(zip(SHIFTS, outs))
    ]
    for store in stores:
        store.start()
    for store in stores:
        store.wait()


PRE_SCRATCH = [
    pltpu.VMEM((5016, 128), F32),
    pltpu.VMEM((NP, NQ, 2, 16, 128), F32),
    pltpu.SemaphoreType.DMA((5 + NP,)),
]


def pre(raw):
    return pl.pallas_call(
        _pre_kernel,
        in_specs=[HBM],
        out_specs=HBM,
        out_shape=jax.ShapeDtypeStruct((NP, NQ, 2, 16, 128), F32),
        scratch_shapes=PRE_SCRATCH,
        cost_estimate=pl.CostEstimate(flops=10**8, bytes_accessed=10**7, transcendentals=0),
        name="pre",
    )(_raw_rows(raw))


def pre_shifts(me, raw):
    return pl.pallas_call(
        _pre_shift_kernel,
        in_specs=[SMEM, HBM],
        out_specs=[HBM] * NP,
        out_shape=[jax.ShapeDtypeStruct((NQ, 2, 16, 128), F32)] * NP,
        scratch_shapes=PRE_SCRATCH,
        cost_estimate=pl.CostEstimate(flops=10**8, bytes_accessed=10**7, transcendentals=0),
        name="pre_shifts",
    )(me, _raw_rows(raw))


def _range_body(ready, tables, o_hbm, d_ref, x_ref, o_ref, out_sem):
    twb_ref, hf_ref, fh_ref, fl_ref, gh_ref, gl_ref, twc_ref = tables
    lane = lax.broadcasted_iota(jnp.int32, (16, 128), 1)

    def outer(q, carry):
        ready(q)
        for g in range(2):
            rows = slice(8 * g, 8 * g + 8)
            v = [(x_ref[p, q, 0, rows, :], x_ref[p, q, 1, rows, :]) for p in range(NP)]
            v = dft16(v, -1)
            for k in range(NP):
                at = k * NQ + q
                r, i = cmul(v[k], (twc_ref[at, 0:1, :], -twc_ref[at, 1:2, :]))
                d_ref[at, 0, rows, :] = r
                d_ref[at, 1, rows, :] = i
        return carry

    lax.fori_loop(0, NQ, outer, 0, unroll=2)
    ready(None)

    def middle(kp, carry):
        v = [(d_ref[kp * NQ + q, 0], d_ref[kp * NQ + q, 1]) for q in range(NQ)]
        v = dft10(v, -1)
        rows = []
        for k in range(NQ):
            r, i = cmul(v[k], (twb_ref[k, 0:1, :], twb_ref[k, 1:2, :]))
            rows.append(jnp.concatenate([r, i], axis=1))
        hi, lo = split(jnp.concatenate(rows, axis=0))
        y = dot(hi, fh_ref[...]) + dot(lo, fh_ref[...]) + dot(hi, fl_ref[...])
        rows = []
        for k in range(NQ):
            val = (y[16 * k : 16 * k + 16, :128], y[16 * k : 16 * k + 16, 128:])
            r, i = cmul(val, (hf_ref[kp * NQ + k, 0:1, :], hf_ref[kp * NQ + k, 1:2, :]))
            rows.append(jnp.concatenate([r, i], axis=1))
        hi, lo = split(jnp.concatenate(rows, axis=0))
        y = dot(hi, gh_ref[...]) + dot(lo, gh_ref[...]) + dot(hi, gl_ref[...])
        v = []
        for k in range(NQ):
            val = (y[16 * k : 16 * k + 16, :128], y[16 * k : 16 * k + 16, 128:])
            v.append(cmul(val, (twb_ref[k, 0:1, :], -twb_ref[k, 1:2, :])))
        v = dft10(v, 1)
        for q in range(NQ):
            at = kp * NQ + q
            r, i = cmul(v[q], (twc_ref[at, 0:1, :], twc_ref[at, 1:2, :]))
            d_ref[at, 0] = r
            d_ref[at, 1] = i
        return carry

    lax.fori_loop(0, NP, middle, 0, unroll=16)

    def inner(q, carry):
        for g in range(2):
            rows = slice(8 * g, 8 * g + 8)
            v = [(d_ref[k * NQ + q, 0, rows, :], d_ref[k * NQ + q, 1, rows, :]) for k in range(NP)]
            v = dft16(v, 1)
            for p in range(14):
                d_ref[p * NQ + q, 0, rows, :] = v[p][0]
                d_ref[p * NQ + q, 1, rows, :] = v[p][1]
        return carry

    lax.fori_loop(0, NQ, inner, 0, unroll=2)

    def store(part):
        at = (pl.ds(2 * (part // 2), 2), slice(None), part % 2)
        return pltpu.make_async_copy(o_ref.at[at], o_hbm.at[at], out_sem.at[part])

    for d in range(128):
        n, a = divmod(128 * d, NS)
        for c in range(2):
            val = d_ref[n, c]
            if a:
                val = pltpu.roll(val, 128 - a, 1)
            start = NS - a
            while start < 128:
                n2 = (128 * d + start) // NS
                nxt = d_ref[n2, c]
                nxt = pltpu.roll(nxt, start % 128, 1)
                val = jnp.where(lane < start, val, nxt)
                start += NS
            az, rg = divmod(worker(d), 16)
            o_ref[az, rg // 4, rg % 4 // 2, rg % 2, c] = val
        if d % 16 == 15:
            store(d // 16).start()
    for part in range(8):
        store(part).wait()


def _tables_in(table_hbm, tables, sem):
    copies = [
        pltpu.make_async_copy(src, dst, sem.at[k]) for k, (src, dst) in enumerate(zip(table_hbm, tables))
    ]
    for copy in copies[::-1]:
        copy.start()
    return copies


def _range_kernel(x_hbm, *refs):
    table_hbm, o_hbm, tables, (d_ref, x_ref, o_ref, out_sem, in_sem, sem) = refs[:7], refs[7], refs[8:15], refs[15:]

    def load(q):
        return pltpu.make_async_copy(x_hbm.at[:, q], x_ref.at[:, q], in_sem.at[q])

    def ready(q):
        if q is None:
            for copy in copies[:6]:
                copy.wait()
        else:
            load(q).wait()

    copies = _tables_in(table_hbm, tables, sem)
    for q in range(NQ):
        load(q).start()
    copies[6].wait()
    _range_body(ready, tables, o_hbm, d_ref, x_ref, o_ref, out_sem)


def _range_shift_kernel(me_ref, *refs):
    parts, refs = refs[:NP], refs[NP:]
    table_hbm, o_hbm, tables, (d_ref, x_ref, o_ref, out_sem, in_sem, sem) = refs[:7], refs[7], refs[8:15], refs[15:]
    me = me_ref[0]
    loads = [
        pltpu.make_async_copy(
            part, x_ref.at[shifted(me, (4 - shift[0], 4 - shift[1]))], in_sem.at[k]
        )
        for k, (shift, part) in enumerate(zip(SHIFTS, parts))
    ]

    def ready(q):
        if q is None:
            for copy in copies[:6]:
                copy.wait()

    copies = _tables_in(table_hbm, tables, sem)
    for load in loads:
        load.start()
    for load in loads:
        load.wait()
    copies[6].wait()
    _range_body(ready, tables, o_hbm, d_ref, x_ref, o_ref, out_sem)


def range_compress(kernel, specs, operands, hf):
    t = TABLES
    tables = (t["twb"], hf, t["fh"], t["fl"], t["gh"], t["gl"], t["twc"])
    return pl.pallas_call(
        kernel,
        in_specs=specs + [HBM] * 7,
        out_specs=HBM,
        out_shape=jax.ShapeDtypeStruct((8, 4, 2, 2, 2, 16, 128), F32),
        scratch_shapes=[pltpu.VMEM(x.shape, x.dtype) for x in tables]
        + [
            pltpu.VMEM((NP * NQ, 2, 16, 128), F32),
            pltpu.VMEM((NP, NQ, 2, 16, 128), F32),
            pltpu.VMEM((8, 4, 2, 2, 2, 16, 128), F32),
            pltpu.SemaphoreType.DMA((8,)),
            pltpu.SemaphoreType.DMA((NP,)),
            pltpu.SemaphoreType.DMA((7,)),
        ],
        cost_estimate=pl.CostEstimate(flops=10**10, bytes_accessed=6 * 10**6, transcendentals=0),
    )(*operands, *tables).reshape(128, 2, 16, 128)


def _dot_t(a, b):
    return lax.dot_general(
        a, b, (((1,), (1,)), ((), ())), precision=lax.Precision.HIGHEST, preferred_element_type=F32
    )


def _prep_kernel(h_ref, dft_ref, turn_ref, wrap_ref, a_ref, g_ref):
    def mul(a, b):
        return jnp.dot(a, b, precision=lax.Precision.HIGHEST, preferred_element_type=F32)

    hr, hi = h_ref[0], h_ref[1]
    dr, di = dft_ref[0], dft_ref[1]
    g = (mul(hr, dr) - mul(hi, di), mul(hr, di) + mul(hi, dr))
    r, i = cmul(g, (turn_ref[0], turn_ref[1]))
    g_ref[:, 0, :] = r
    g_ref[:, 1, :] = i
    row = lax.broadcasted_iota(jnp.int32, (128, 128), 0)
    lane = lax.broadcasted_iota(jnp.int32, (128, 128), 1)
    over = lane > row

    def body(k, carry):
        m = []
        for c in range(2):
            line = jnp.broadcast_to(g_ref[k, c : c + 1, :], (128, 128))
            m.append(pltpu.roll(line, 0, 1, stride=1, stride_axis=0))
        turned = cmul(m, (wrap_ref[k, 0:1, :], wrap_ref[k, 1:2, :]))
        re = jnp.where(over, turned[0], m[0])
        im = jnp.where(over, turned[1], m[1])
        for part, block in enumerate((re, -im)):
            cols = slice(128 * part, 128 * part + 128)
            high, low = split(block)
            a_ref[k, 0:128, cols] = high
            a_ref[k, 128:256, cols] = low
        return carry

    lax.fori_loop(0, 16, body, 0, unroll=2)


def prep(h):
    t = TABLES
    return pl.pallas_call(
        _prep_kernel,
        out_shape=jax.ShapeDtypeStruct((16, 256, 256), BF16),
        scratch_shapes=[pltpu.VMEM((16, 2, 128), F32)],
        cost_estimate=pl.CostEstimate(flops=2 * 10**9, bytes_accessed=5 * 10**6, transcendentals=0),
        name="prep",
    )(h, t["dft"], t["turn"], t["wrap"])


def _azimuth_front(x_hbm, a_hbm, e_ref, a_ref, sem, x_ref=None):
    def load(s):
        return pltpu.make_async_copy(x_hbm.at[:, s], x_ref.at[:, s], sem.at[s])

    matrices = pltpu.make_async_copy(a_hbm, a_ref, sem.at[8])
    staged = x_ref is not None
    if staged:
        for s in range(8):
            load(s).start()
    else:
        x_ref = x_hbm
    matrices.start()

    def first(s, carry):
        if staged:
            load(s).wait()
        for g in range(2):
            rows = slice(8 * g, 8 * g + 8)
            v = [(x_ref[a, s, 0, rows, :], x_ref[a, s, 1, rows, :]) for a in range(16)]
            v = dft16(v, -1)
            for k in range(16):
                for c in range(2):
                    at = pl.multiple_of(c * 128 + s * 16 + g * 8, 8)
                    e_ref[k, pl.ds(at, 8), :] = v[k][c]
        return carry

    lax.fori_loop(0, 8, first, 0, unroll=2)
    matrices.wait()

    def second(k, carry):
        re_hi, re_lo = split(e_ref[k, 0:128, :])
        im_hi, im_lo = split(e_ref[k, 128:256, :])

        def turned(re, im):
            straight = jnp.concatenate([re, im], axis=0)
            return jnp.concatenate([straight, jnp.concatenate([im, -re], axis=0)], axis=1)

        y = dot(a_ref[k], turned(re_hi, im_hi))
        y = y[:128] + y[128:] + dot(a_ref[k, 0:128, :], turned(re_lo, im_lo))
        e_ref[k, 0:128, :] = y[:, :128]
        e_ref[k, 128:256, :] = y[:, 128:]
        return carry

    lax.fori_loop(0, 16, second, 0, unroll=4)


AZIMUTH_SCRATCH = [
    pltpu.VMEM((16, 256, 128), F32),
    pltpu.VMEM((16, 256, 256), BF16),
    pltpu.SemaphoreType.DMA((13,)),
]
STAGED_SCRATCH = AZIMUTH_SCRATCH + [pltpu.VMEM((16, 8, 2, 16, 128), F32)]


def _azimuth_rows(e_ref, g):
    at = [pl.multiple_of(c * 128 + g * 8, 8) for c in range(2)]
    v = [(e_ref[k, pl.ds(at[0], 8), :], e_ref[k, pl.ds(at[1], 8), :]) for k in range(16)]
    return dft16(v, 1)


def _slave_kernel(x_ref, a_hbm, left_hbm, right_hbm, left_ref, right_ref, *scratch):
    _azimuth_front(x_ref, a_hbm, *scratch)
    e_ref, sem = scratch[0], scratch[2]
    low = lax.broadcasted_iota(jnp.int32, (8, 128), 1) < 64
    zero = jnp.zeros((ASH, 128), F32)
    for ref in (left_ref, right_ref):
        ref[0:ASH, :] = zero
        ref[ASH + LINES :, :] = zero

    def third(g, carry):
        v = _azimuth_rows(e_ref, g)
        for a in range(16):
            rows = pl.ds(pl.multiple_of(a * 128 + g * 8 + ASH, 8), 8)
            r, i = v[a]
            left_ref[rows, :] = jnp.where(low, r, pltpu.roll(i, 64, 1))
            right_ref[rows, :] = jnp.where(low, pltpu.roll(r, 64, 1), i)
        return carry

    lax.fori_loop(0, 16, third, 0, unroll=2)
    copies = [
        pltpu.make_async_copy(right_ref, right_hbm, sem.at[10]),
        pltpu.make_async_copy(left_ref, left_hbm, sem.at[9]),
    ]
    for copy in copies:
        copy.start()
    for copy in copies:
        copy.wait()


def slave_azimuth(x, a):
    side = jax.ShapeDtypeStruct((LINES + 2 * ASH, 128), F32)
    return pl.pallas_call(
        _slave_kernel,
        in_specs=[VMEM, HBM],
        out_specs=(HBM, HBM),
        out_shape=(side, side),
        scratch_shapes=[pltpu.VMEM(side.shape, F32)] * 2 + AZIMUTH_SCRATCH,
        cost_estimate=pl.CostEstimate(flops=5 * 10**9, bytes_accessed=10**7, transcendentals=0),
        compiler_params=limit(AZIMUTH_MIB),
        name="slave_azimuth",
    )(x.reshape(16, 8, 2, 16, 128), a)


def _master_kernel(x_hbm, a_hbm, o_hbm, o_ref, *scratch):
    _azimuth_front(x_hbm, a_hbm, *scratch)
    e_ref, sem = scratch[0], scratch[2]

    def third(g, carry):
        v = _azimuth_rows(e_ref, g)
        for a in range(16):
            rows = pl.ds(pl.multiple_of(a * 128 + g * 8, 8), 8)
            o_ref[0, rows, :] = v[a][0]
            o_ref[1, rows, :] = v[a][1]
        return carry

    lax.fori_loop(0, 16, third, 0, unroll=2)
    copy = pltpu.make_async_copy(o_ref, o_hbm, sem.at[9])
    copy.start()
    copy.wait()


def master_azimuth(x, a):
    return pl.pallas_call(
        _master_kernel,
        in_specs=[HBM, HBM],
        out_specs=HBM,
        out_shape=jax.ShapeDtypeStruct((2, LINES, 128), F32),
        scratch_shapes=[pltpu.VMEM((2, LINES, 128), F32)] + STAGED_SCRATCH,
        cost_estimate=pl.CostEstimate(flops=5 * 10**9, bytes_accessed=10**7, transcendentals=0),
        compiler_params=limit(MASTER_MIB),
        name="master_azimuth",
    )(x.reshape(16, 8, 2, 16, 128), a)


def _looks_kernel(shift_ref, *refs):
    packs, (m_hbm, n_ref, pick_ref, box_ref, side_ref) = refs[:4], refs[4:9]
    w_ref, m_ref, total_ref, sem = refs[9:]
    lane = lax.broadcasted_iota(jnp.int32, (64, 128), 1)
    line = lax.broadcasted_iota(jnp.int32, (64, 128), 0)
    low = lane < 64
    count = n_ref[...]

    def load(block):
        rows = pl.ds(0, BA + 2 * ASH) if block == 0 else pl.ds(block * BA + 2 * ASH, BA)
        mine = pl.ds(block * BA, BA)
        return [
            pltpu.make_async_copy(pack.at[rows], w_ref.at[k, rows], sem.at[5 * block + k])
            for k, pack in enumerate(packs)
        ] + [pltpu.make_async_copy(m_hbm.at[:, mine], m_ref.at[:, mine], sem.at[5 * block + 4])]

    for block in range(NBA):
        for copy in load(block):
            copy.start()
    for block in range(NBA):
        for copy in load(block):
            copy.wait()

        def move(t, carry):
            parts = []
            for r in range(2):
                shift = shift_ref[8 + 2 * block + r] + RSH
                first = shift // 64 + r
                second = jnp.minimum(first + 1, 3)
                s = lax.rem(shift, 64)
                rows = pl.ds(block * BA + t * 64 + ASH + shift_ref[2 * block + r], 64)
                parts.append(
                    jnp.where(
                        (lane & 63) + s < 64,
                        pltpu.roll(w_ref[first, rows, :], lax.rem(128 - s, 128), 1),
                        pltpu.roll(w_ref[second, rows, :], 64 - s, 1),
                    )
                )
            sr = jnp.where(low, parts[0], pltpu.roll(parts[1], 64, 1))
            si = jnp.where(low, pltpu.roll(parts[0], 64, 1), parts[1])
            at = pl.multiple_of(block * BA + t * 64, 64)
            r, i = m_ref[0, pl.ds(at, 64), :], m_ref[1, pl.ds(at, 64), :]
            keep = line + at < count
            cross = (r * sr + i * si, i * sr - r * si)
            for c in range(2):
                cells = jnp.where(keep, cross[c], 0.0).reshape(8, LOOK, 128).sum(axis=1)
                total_ref[pl.ds(pl.multiple_of(c * 256 + (block * 8 + t) * 8, 8), 8), :] = cells
            return carry

        lax.fori_loop(0, BA // 64, move, 0, unroll=4)
    y = _dot_t(pick_ref[...], total_ref[...])
    cell = lax.broadcasted_iota(jnp.int32, (24, 512), 1) % 256
    y = (
        y
        + jnp.where(cell == 0, 0.0, pltpu.roll(y, 1, 1))
        + jnp.where(cell == 255, 0.0, pltpu.roll(y, 511, 1))
    )
    box_ref[...] = y[:16]
    side_ref[...] = y[16:]


def looks(shifts, packs, master, counts):
    return pl.pallas_call(
        _looks_kernel,
        in_specs=[SMEM] + [HBM] * 5 + [VMEM] * 2,
        out_shape=(
            jax.ShapeDtypeStruct((16, 512), F32),
            jax.ShapeDtypeStruct((8, 512), F32),
        ),
        scratch_shapes=[
            pltpu.VMEM((4, LINES + 2 * ASH + 16, 128), F32),
            pltpu.VMEM((2, LINES, 128), F32),
            pltpu.VMEM((512, 128), F32),
            pltpu.SemaphoreType.DMA((20,)),
        ],
        cost_estimate=pl.CostEstimate(flops=5 * 10**9, bytes_accessed=10**7, transcendentals=0),
        compiler_params=limit(50),
        name="looks",
    )(shifts, *packs, master, counts, TABLES["pick"])


def _merge_kernel(core_ref, box_ref, side_ref, o_ref):
    row = lax.broadcasted_iota(jnp.int32, (16, 512), 0)
    first = core_ref[0] == 0
    facing = jnp.where(first, side_ref[0:1, :], side_ref[1:2, :])
    o_ref[...] = box_ref[...] + jnp.where(row == jnp.where(first, 15, 0), facing, 0.0)


def merge(core, box, side):
    return pl.pallas_call(
        _merge_kernel,
        in_specs=[SMEM, VMEM, VMEM],
        out_shape=jax.ShapeDtypeStruct((16, 512), F32),
        compiler_params=limit(4),
        name="merge",
    )(core, box, side)


def _final_kernel(odd_ref, box_ref, outer_ref, scale_ref, o_ref):
    row = lax.broadcasted_iota(jnp.int32, (16, 256), 0)
    odd = odd_ref[0] == 1
    at = jnp.where(odd, 15, 0)
    for c in range(2):
        cells = slice(256 * c, 256 * c + 256)
        outer = jnp.where(odd, outer_ref[0:1, cells], outer_ref[1:2, cells])
        o_ref[c] = (box_ref[:, cells] + jnp.where(row == at, outer, 0.0)) * scale_ref[...]


def final(odd, box, outer, scale):
    return pl.pallas_call(
        _final_kernel,
        in_specs=[SMEM, VMEM, VMEM, VMEM],
        out_shape=jax.ShapeDtypeStruct((2, 16, 256), F32),
        compiler_params=limit(4),
        name="final",
    )(odd, box, outer, scale)


def to_worker(x):
    return lax.ppermute(x, ALL, [(b, worker(b)) for b in range(128)])


def halo(to_right, to_left):
    up = [(worker(b), worker(b + 1)) for b in range(127)]
    down = [(j, i) for i, j in up]
    return lax.ppermute(to_right, ALL, up), lax.ppermute(to_left, ALL, down)


def local(master_raw, slave_raw, range_ref, az_ref, az_shift, rg_shift, valid_lines):
    hf = range_ref.reshape(2, NS, NQ, NP).transpose(3, 2, 0, 1).reshape(NP * NQ, 2, NS)
    hf = jnp.pad(hf * (1.0 / RANGE), ((0, 0), (0, 0), (0, 3)))
    h = az_ref.reshape(2, 128, 16).transpose(0, 2, 1) * (1.0 / LINES)

    def columns_of(ranged):
        return lax.all_to_all(ranged, ALL, 0, 0, tiled=True)

    flat = lax.axis_index(ALL)
    counts = lax.dynamic_slice(jnp.pad(valid_lines, 1), (flat * 2,), (4,))
    wide = jnp.concatenate([counts[:1], jnp.repeat(counts[1:3], BR // LOOK), counts[3:]])
    rows = LINES // LOOK
    groups = lax.broadcasted_iota(jnp.int32, (18, rows + 2), 1) - 1
    pixels = jnp.clip(wide[:, None] - LOOK * groups, 0, LOOK) * LOOK
    pixels = jnp.where((groups >= 0) & (groups < rows), pixels, 0).astype(F32)
    box_pixels = sum(pixels[j : j + 16, i : i + rows] for i in range(3) for j in range(3))
    scale = 1.0 / jnp.sqrt(jnp.maximum(box_pixels, 1.0))
    block = block_of(lax.axis_index("az"), lax.axis_index("rg"))
    own = lax.dynamic_slice(valid_lines, (block * 2,), (2,))
    col_counts = jnp.repeat(own, BR)[None, :]
    shifts = to_worker(jnp.concatenate([az_shift.reshape(8), rg_shift.reshape(8)]))

    slave = pre(slave_raw)
    slave = lax.all_to_all(slave, "rg", 0, 0, tiled=True)
    me = lax.axis_index("rg").astype(jnp.int32)[None]
    pieces = pre_shifts(me, master_raw)
    master = [
        lax.ppermute(piece, "rg", [(r, shifted(r, shift)) for r in range(NP)])
        if any(shift)
        else piece
        for shift, piece in zip(SHIFTS, pieces)
    ]
    slave = range_compress(_range_kernel, [HBM], [slave], hf)
    slave = columns_of(slave)
    matrices = prep(h)
    master = range_compress(_range_shift_kernel, [SMEM] + [HBM] * NP, [me, *master], hf)
    master = columns_of(master)
    low, high = slave_azimuth(slave, matrices)
    from_left, from_right = halo(high, low)
    master = master_azimuth(master, matrices)
    box, side = looks(shifts, (from_left, low, high, from_right), master, col_counts)

    core = (lax.axis_index("az") % 2).astype(jnp.int32)[None]
    odd = (lax.axis_index("rg") % 2).astype(jnp.int32)[None]
    facing = lax.ppermute(side, ALL, [(worker(b), worker(b ^ 1)) for b in range(128)])
    outer = lax.ppermute(
        side,
        ALL,
        [(worker(b - 1), b) for b in range(2, 128, 2)]
        + [(worker(b + 1), b) for b in range(1, 126, 2)],
    )
    box = merge(core, box, facing)
    box = lax.ppermute(box, ALL, [(worker(b), b) for b in range(128)])
    return final(odd, box, outer, scale).transpose(0, 2, 1)


def solution(mesh):
    return jax.shard_map(
        local,
        mesh=mesh,
        in_specs=(
            P(None, "az", "rg"),
            P(None, "az", "rg"),
            P(),
            P(),
            P(None, ALL),
            P(None, ALL),
            P(),
        ),
        out_specs=P(None, None, ALL),
        check_vma=False,
    )
```
